32 devices in a mesh: dp: 1 (over z), tp: 4 (over y), fsdp: 8 (over x, core).
Axes of the slice: x: 4, y: 4, z: 1, core: 2. Of those that a mesh axis runs over, the one named last changes fastest.
The devices are a block of a 4x4x8 slice.
Arguments:
- tokens: bfloat16 [8, 4096, 3072], P(('dp', 'fsdp'))
- positions: int32 [8, 4096], P(('dp', 'fsdp'))
- valid_len: int32 [8], P(('dp', 'fsdp'))
- w_query: bfloat16 [3072, 3072], P('fsdp', 'tp')
- w_key: bfloat16 [3072, 1024], P('fsdp', 'tp')
- w_value: bfloat16 [3072, 1024], P('fsdp', 'tp')
- w_out: bfloat16 [3072, 3072], P('tp', 'fsdp')
- w_gate: bfloat16 [3072, 8192], P('fsdp', 'tp')
- w_up: bfloat16 [3072, 8192], P('fsdp', 'tp')
- w_down: bfloat16 [8192, 3072], P('tp', 'fsdp')
- norm_attn: bfloat16 [3072], replicated
- norm_mlp: bfloat16 [3072], replicated
Outputs:
- output 1: bfloat16 [8, 4096, 3072], P(('dp', 'fsdp'))
- output 2: bfloat16 [8, 4096, 8, 128], P(('dp', 'fsdp'), None, 'tp')
- output 3: bfloat16 [8, 4096, 8, 128], P(('dp', 'fsdp'), None, 'tp')
All inputs are finite; a program needn't handle non-finite values.
Results may differ from the reference program's by a relative error of at most 0.0131316.
Values are sent between devices in bfloat16 or wider.
A program may use at most 768 MiB of HBM per device.

```python
import math
import jax
import jax.numpy as jnp
from jax import lax

MODEL_DIM = 3072
Q_HEADS = 24
KV_HEADS = 8
HEAD_DIM = 128
FFN_DIM = 8192
SEQ_LEN = 4096
BATCH_SIZE = 8

GROUP_SIZE = Q_HEADS // KV_HEADS
Q_BLOCK = min(SEQ_LEN, 256)
ROPE_THETA = 500000.0
NORM_EPS = 1e-5
SCORE_SCALE = HEAD_DIM ** -0.5
Q_GAIN = math.sqrt(max(math.log(SEQ_LEN) - 2.5, 1.0))


def setup_inputs(seed: int = 0, part: int = 0) -> dict:
    part_key = jax.random.fold_in(jax.random.key(seed), part)
    key_tok, key_pos, key_len = jax.random.split(part_key, 3)
    w_keys = jax.random.split(jax.random.key(seed + 1), 9)

    def draw_matrix(sub_key, mat_shape, scale_by):
        return (jax.random.normal(sub_key, mat_shape, jnp.float32) * scale_by).astype(jnp.bfloat16)

    tokens = jax.random.normal(key_tok, (BATCH_SIZE, SEQ_LEN, MODEL_DIM), jnp.float32).astype(jnp.bfloat16)
    starts = jax.random.randint(key_pos, (BATCH_SIZE, 1), 0, 4 * SEQ_LEN + 1, dtype=jnp.int32)
    positions = starts + jnp.arange(SEQ_LEN, dtype=jnp.int32)[None, :]
    valid_len = jax.random.randint(key_len, (BATCH_SIZE,), 1, SEQ_LEN + 1, dtype=jnp.int32).at[0].set(SEQ_LEN)
    q_width = Q_HEADS * HEAD_DIM
    kv_width = KV_HEADS * HEAD_DIM
    return {
        'tokens': tokens,
        'positions': positions,
        'valid_len': valid_len,
        'w_query': draw_matrix(w_keys[0], (MODEL_DIM, q_width), Q_GAIN * MODEL_DIM ** -0.5),
        'w_key': draw_matrix(w_keys[1], (MODEL_DIM, kv_width), MODEL_DIM ** -0.5),
        'w_value': draw_matrix(w_keys[2], (MODEL_DIM, kv_width), MODEL_DIM ** -0.5),
        'w_out': draw_matrix(w_keys[3], (q_width, MODEL_DIM), q_width ** -0.5),
        'w_gate': draw_matrix(w_keys[4], (MODEL_DIM, FFN_DIM), MODEL_DIM ** -0.5),
        'w_up': draw_matrix(w_keys[5], (MODEL_DIM, FFN_DIM), MODEL_DIM ** -0.5),
        'w_down': draw_matrix(w_keys[6], (FFN_DIM, MODEL_DIM), FFN_DIM ** -0.5),
        'norm_attn': (1.0 + 0.4 * jax.random.normal(w_keys[7], (MODEL_DIM,), jnp.float32)).astype(jnp.bfloat16),
        'norm_mlp': (1.0 + 0.4 * jax.random.normal(w_keys[8], (MODEL_DIM,), jnp.float32)).astype(jnp.bfloat16),
    }


def rope_freqs():
    half_idx = jnp.arange(HEAD_DIM // 2, dtype=jnp.float32)
    inv_freq = jnp.power(ROPE_THETA, -2.0 * half_idx / HEAD_DIM)
    wave_len = 2.0 * math.pi / inv_freq
    smooth = (8192.0 / wave_len - 1.0) / 3.0
    blended = (1.0 - smooth) * inv_freq / 8.0 + smooth * inv_freq
    return jnp.where(wave_len < 2048.0, inv_freq, jnp.where(wave_len > 8192.0, inv_freq / 8.0, blended))


def rms_norm(values, gain_vec):
    vals_f32 = values.astype(jnp.float32)
    inv_rms = lax.rsqrt(jnp.mean(vals_f32 * vals_f32, axis=-1, keepdims=True) + NORM_EPS)
    return (vals_f32 * inv_rms * gain_vec.astype(jnp.float32)).astype(jnp.bfloat16)


def rotate(proj_val, cos_t, sin_t):
    half_dim = proj_val.shape[-1] // 2
    lead_half = proj_val[..., :half_dim]
    tail_half = proj_val[..., half_dim:]
    return jnp.concatenate([lead_half * cos_t - tail_half * sin_t, tail_half * cos_t + lead_half * sin_t], axis=-1)


def reference(tokens, positions, valid_len, w_query, w_key, w_value, w_out, w_gate, w_up, w_down, norm_attn, norm_mlp):
    inv_freqs = rope_freqs()
    key_idx = jnp.arange(SEQ_LEN)
    n_blocks = SEQ_LEN // Q_BLOCK

    def one_request(request_data):
        x_req, pos_req, req_len = request_data
        angles = pos_req.astype(jnp.float32)[:, None] * inv_freqs[None, :]
        cos_t = jnp.cos(angles)[:, None, :]
        sin_t = jnp.sin(angles)[:, None, :]
        h_in = rms_norm(x_req, norm_attn)
        q_proj = jnp.dot(h_in, w_query, preferred_element_type=jnp.float32).reshape(SEQ_LEN, Q_HEADS, HEAD_DIM)
        k_proj = jnp.dot(h_in, w_key, preferred_element_type=jnp.float32).reshape(SEQ_LEN, KV_HEADS, HEAD_DIM)
        v_req = jnp.dot(h_in, w_value, preferred_element_type=jnp.float32).astype(jnp.bfloat16).reshape(SEQ_LEN, KV_HEADS, HEAD_DIM)
        q_rot = rotate(q_proj, cos_t, sin_t).astype(jnp.bfloat16)
        k_rot = rotate(k_proj, cos_t, sin_t).astype(jnp.bfloat16)
        q_blocks = q_rot.reshape(n_blocks, Q_BLOCK, KV_HEADS, GROUP_SIZE, HEAD_DIM)
        k_f32 = k_rot.astype(jnp.float32)
        v_f32 = v_req.astype(jnp.float32)

        def one_block(block_data):
            q_blk, first_row = block_data
            scores = jnp.einsum('qkgd,skd->kgqs', q_blk.astype(jnp.float32), k_f32) * SCORE_SCALE
            q_idx = first_row + jnp.arange(Q_BLOCK)
            allowed = (key_idx[None, :] <= q_idx[:, None]) & (key_idx[None, :] < req_len)
            scores = jnp.where(allowed, scores, -jnp.inf)
            attn_prob = jax.nn.softmax(scores, axis=-1).astype(jnp.bfloat16).astype(jnp.float32)
            return jnp.einsum('kgqs,skd->qkgd', attn_prob, v_f32).astype(jnp.bfloat16)

        blocks = lax.map(one_block, (q_blocks, jnp.arange(n_blocks) * Q_BLOCK))
        attn_out = blocks.reshape(SEQ_LEN, Q_HEADS * HEAD_DIM)
        y_attn = jnp.dot(attn_out, w_out, preferred_element_type=jnp.float32)
        resid_mid = (x_req.astype(jnp.float32) + y_attn).astype(jnp.bfloat16)
        h_mlp = rms_norm(resid_mid, norm_mlp)
        gate_val = jnp.dot(h_mlp, w_gate, preferred_element_type=jnp.float32)
        up_val = jnp.dot(h_mlp, w_up, preferred_element_type=jnp.float32)
        hidden_act = (jax.nn.silu(gate_val) * up_val).astype(jnp.bfloat16)
        down_val = jnp.dot(hidden_act, w_down, preferred_element_type=jnp.float32)
        out_req = (resid_mid.astype(jnp.float32) + down_val).astype(jnp.bfloat16)
        return out_req, k_rot, v_req

    hidden_out, key_cache, value_cache = lax.map(one_request, (tokens, positions, valid_len))
    return hidden_out, key_cache, value_cache
```

```python
import functools
import math
import jax
import jax.numpy as jnp
from jax import lax
from jax.experimental import pallas as pl
from jax.experimental.pallas import tpu as pltpu
from jax.sharding import PartitionSpec as P

HEAD_DIM = 128
ROPE_THETA = 500000.0
NORM_EPS = 1e-5
EXP2_SCALE = HEAD_DIM ** -0.5 * math.log2(math.e)
N_CALLS = 2
VMEM_LIMIT = 60 * 1024 * 1024


def rope_freqs():
    half_idx = jnp.arange(HEAD_DIM // 2, dtype=jnp.float32)
    inv_freq = jnp.power(ROPE_THETA, -2.0 * half_idx / HEAD_DIM)
    wave_len = 2.0 * math.pi / inv_freq
    smooth = (8192.0 / wave_len - 1.0) / 3.0
    blended = (1.0 - smooth) * inv_freq / 8.0 + smooth * inv_freq
    return jnp.where(wave_len < 2048.0, inv_freq, jnp.where(wave_len > 8192.0, inv_freq / 8.0, blended))


def params(**kw):
    return pltpu.CompilerParams(vmem_limit_bytes=VMEM_LIMIT, **kw)


def cost(flops, nbytes):
    return pl.CostEstimate(flops=flops, bytes_accessed=nbytes, transcendentals=0)


def norm_rows(vals_f32, gain):
    inv = lax.rsqrt(jnp.mean(vals_f32 * vals_f32, axis=-1, keepdims=True) + NORM_EPS)
    return (vals_f32 * inv * gain).astype(jnp.bfloat16)


def qkv_kernel(n_q, n_kv, x_ref, g_ref, w_ref, cos_ref, sin_ref, q_ref, k_ref, v_ref):
    h = norm_rows(x_ref[...].astype(jnp.float32), g_ref[...].astype(jnp.float32))
    cos_t, sin_t = cos_ref[...], sin_ref[...]
    for g in range(n_kv):
        per = n_q // n_kv
        for kind in range(2):
            if kind == 0:
                lo, cnt = g * per, per
            else:
                lo, cnt = n_q + g, 1
            y = jnp.dot(h, w_ref[:, lo * HEAD_DIM:(lo + cnt) * HEAD_DIM], preferred_element_type=jnp.float32)
            for i in range(cnt):
                a = y[:, i * HEAD_DIM:(i + 1) * HEAD_DIM]
                r = (a * cos_t + pltpu.roll(a, HEAD_DIM // 2, 1) * sin_t).astype(jnp.bfloat16)
                if kind == 0:
                    q_ref[lo + i] = r
                else:
                    k_ref[:, g * HEAD_DIM:(g + 1) * HEAD_DIM] = r
    base = (n_q + n_kv) * HEAD_DIM
    v_ref[...] = jnp.dot(h, w_ref[:, base:base + n_kv * HEAD_DIM], preferred_element_type=jnp.float32).astype(jnp.bfloat16)


def qkv_call(x, gain, w, cos_t, sin_t, n_q, n_kv):
    s, d = x.shape
    bm = min(512, s)
    n = w.shape[1]
    row = lambda i: (i, 0)
    return pl.pallas_call(
        functools.partial(qkv_kernel, n_q, n_kv),
        grid=(s // bm,),
        in_specs=[pl.BlockSpec((bm, d), row), pl.BlockSpec((1, d), lambda i: (0, 0)), pl.BlockSpec((d, n), lambda i: (0, 0)),
                  pl.BlockSpec((bm, HEAD_DIM), row), pl.BlockSpec((bm, HEAD_DIM), row)],
        out_specs=[pl.BlockSpec((n_q, bm, HEAD_DIM), lambda i: (0, i, 0)),
                   pl.BlockSpec((bm, n_kv * HEAD_DIM), row), pl.BlockSpec((bm, n_kv * HEAD_DIM), row)],
        out_shape=[jax.ShapeDtypeStruct((n_q, s, HEAD_DIM), jnp.bfloat16),
                   jax.ShapeDtypeStruct((s, n_kv * HEAD_DIM), jnp.bfloat16),
                   jax.ShapeDtypeStruct((s, n_kv * HEAD_DIM), jnp.bfloat16)],
        compiler_params=params(),
        cost_estimate=cost(2 * s * d * n, 2 * s * d + 2 * d * n + 2 * s * n),
        name="qkv",
    )(x, gain, w, cos_t, sin_t)


def att_kernel(bq, bk, per, first, len_ref, q_ref, k_ref, v_ref, o_ref, m_ref, l_ref, acc_ref):
    row0 = first + pl.program_id(1) * bq
    valid = len_ref[0]
    m_ref[...] = jnp.full_like(m_ref, -jnp.inf)
    l_ref[...] = jnp.zeros_like(l_ref)
    acc_ref[...] = jnp.zeros_like(acc_ref)
    reps = bk // HEAD_DIM

    def step(j, masked):
        k0 = pl.multiple_of(j * bk, bk)
        k_blk = k_ref[pl.ds(k0, bk), :]
        v_blk = v_ref[pl.ds(k0, bk), :]
        if masked:
            kid = k0 + lax.broadcasted_iota(jnp.int32, (bq, bk), 1)
            qid = row0 + lax.broadcasted_iota(jnp.int32, (bq, bk), 0)
            allowed = (kid <= qid) & (kid < valid)
        for h in range(per):
            sc = lax.dot_general(q_ref[h], k_blk, (((1,), (1,)), ((), ())), preferred_element_type=jnp.float32)
            if masked:
                sc = jnp.where(allowed, sc, -jnp.inf)
            m_old = m_ref[h]
            m_new = jnp.maximum(m_old, jnp.max(sc, axis=1, keepdims=True))
            p = jnp.exp2((sc - jnp.tile(m_new, (1, reps))) * EXP2_SCALE)
            alpha = jnp.exp2((m_old - m_new) * EXP2_SCALE)
            l_ref[h] = l_ref[h] * alpha + jnp.sum(p, axis=1, keepdims=True)
            acc_ref[h] = acc_ref[h] * alpha + jnp.dot(p.astype(jnp.bfloat16), v_blk, preferred_element_type=jnp.float32)
            m_ref[h] = m_new

    n_full = jnp.minimum((row0 + 1) // bk, valid // bk)
    n_end = jnp.minimum((row0 + bq + bk - 1) // bk, (valid + bk - 1) // bk)

    def full(j, _):
        step(j, False)
        return 0

    def part(j, _):
        step(j, True)
        return 0

    lax.fori_loop(0, n_full, full, 0)
    lax.fori_loop(n_full, n_end, part, 0)
    for h in range(per):
        o_ref[:, h * HEAD_DIM:(h + 1) * HEAD_DIM] = (acc_ref[h] / l_ref[h]).astype(jnp.bfloat16)


def att_call(q, k, v, valid_len, call):
    n_q, s, _ = q.shape
    n_kv = k.shape[1] // HEAD_DIM
    per = n_q // n_kv
    rows = s // N_CALLS
    bq = min(256, rows)
    bk = min(512, s)
    first = call * rows
    off = first // bq
    frac = (2 * call + 1) / N_CALLS ** 2
    kernel = functools.partial(att_kernel, bq, bk, per, first)
    args = [valid_len, q, k, v]
    in_specs = [pl.BlockSpec(memory_space=pltpu.SMEM),
                pl.BlockSpec((per, bq, HEAD_DIM), lambda g, i: (g, off + i, 0)),
                pl.BlockSpec((s, HEAD_DIM), lambda g, i: (0, g)),
                pl.BlockSpec((s, HEAD_DIM), lambda g, i: (0, g))]
    return pl.pallas_call(
        kernel,
        grid=(n_kv, rows // bq),
        in_specs=in_specs,
        out_specs=pl.BlockSpec((bq, per * HEAD_DIM), lambda g, i: (i, g)),
        out_shape=jax.ShapeDtypeStruct((rows, n_q * HEAD_DIM), jnp.bfloat16),
        scratch_shapes=[pltpu.VMEM((per, bq, HEAD_DIM), jnp.float32)] * 3,
        compiler_params=params(),
        cost_estimate=cost(int(8 * frac * n_q * s * s * HEAD_DIM), 4 * n_q * s * HEAD_DIM),
        name="attention",
    )(*args)


def out_kernel(n_src, bn, idx_ref, *refs):
    o_refs = refs[:n_src]
    w_ref, x_ref, g_ref, r_ref, u_ref, y_ref = refs[n_src:]
    d = x_ref.shape[1]

    @pl.loop(0, d // bn)
    def _(n):
        acc = None
        for s in range(n_src):
            col = pl.multiple_of(idx_ref[1 + s] * d + n * bn, bn)
            part = jnp.dot(o_refs[s][...], w_ref[:, pl.ds(col, bn)], preferred_element_type=jnp.float32)
            acc = part if acc is None else acc + part
        col = pl.multiple_of(n * bn, bn)
        y_ref[:, pl.ds(col, bn)] = (x_ref[:, pl.ds(col, bn)].astype(jnp.float32) + acc).astype(jnp.bfloat16)

    r_ref[...] = y_ref[...]
    u_ref[...] = norm_rows(y_ref[...].astype(jnp.float32), g_ref[...].astype(jnp.float32))


def out_call(idx, o_pieces, w, x, gain, sub, n_tp):
    n_src = len(o_pieces)
    rows, ko = o_pieces[0].shape
    d = x.shape[1]
    bn = min(512, d)
    row = lambda i, idx: (i, 0)
    fixed = lambda i, idx: (0, 0)
    return pl.pallas_call(
        functools.partial(out_kernel, n_src, bn),
        grid_spec=pltpu.PrefetchScalarGridSpec(
            num_scalar_prefetch=1,
            grid=(rows // sub,),
            in_specs=[pl.BlockSpec((sub, ko), row)] * n_src + [
                pl.BlockSpec(w.shape, fixed, pipeline_mode=pl.Buffered(1)),
                pl.BlockSpec((sub, d), lambda i, idx: (i * n_tp + idx[0], 0)),
                pl.BlockSpec((1, d), fixed)],
            out_specs=[pl.BlockSpec((sub, d), row), pl.BlockSpec((sub, d), row)],
            scratch_shapes=[pltpu.VMEM((sub, d), jnp.bfloat16)]),
        out_shape=[jax.ShapeDtypeStruct((rows, d), jnp.bfloat16)] * 2,
        compiler_params=params(),
        cost_estimate=cost(2 * rows * d * ko * n_src, 2 * w.size + 8 * rows * d),
        name="w_out",
    )(idx, *o_pieces, w, x, gain)


def gu_kernel(bm, u_ref, g_ref, up_ref, a_ref):
    rows = u_ref.shape[0]

    @pl.loop(0, rows // bm)
    def _(m):
        r = pl.ds(pl.multiple_of(m * bm, bm), bm)
        u = u_ref[r, :]
        gate = jnp.dot(u, g_ref[0], preferred_element_type=jnp.float32)
        up = jnp.dot(u, up_ref[0], preferred_element_type=jnp.float32)
        a_ref[r, :] = (jax.nn.silu(gate) * up).astype(jnp.bfloat16)


def gu_call(u, w):
    rows, d = u.shape
    n_src, _, two = w.shape
    half = two // 2
    bn = min(512, half)
    nb = half // bn
    bm = min(256, rows)
    return pl.pallas_call(
        functools.partial(gu_kernel, bm),
        grid=(n_src, nb),
        in_specs=[pl.BlockSpec((rows, d), lambda j, n: (0, 0), pipeline_mode=pl.Buffered(1)),
                  pl.BlockSpec((1, d, bn), lambda j, n: (j, 0, n)),
                  pl.BlockSpec((1, d, bn), lambda j, n: (j, 0, nb + n))],
        out_specs=pl.BlockSpec((rows, bn), lambda j, n: (0, j * nb + n)),
        out_shape=jax.ShapeDtypeStruct((rows, n_src * half), jnp.bfloat16),
        compiler_params=params(),
        cost_estimate=cost(2 * rows * d * n_src * two, 2 * w.size + 2 * rows * d + 2 * rows * n_src * half),
        name="gate_up",
    )(u, w, w)


def down_kernel(bm, parts, *refs):
    a_refs = refs[:parts]
    w_ref, r_ref, o_ref, acc_ref = refs[parts:]
    j = pl.program_id(1)
    kp = a_refs[0].shape[1]
    rows = acc_ref.shape[0]

    @pl.when(j == 0)
    def _():
        acc_ref[...] = r_ref[...].astype(jnp.float32)

    @pl.loop(0, rows // bm)
    def _(m):
        r = pl.ds(pl.multiple_of(m * bm, bm), bm)
        acc = acc_ref[r, :]
        for p in range(parts):
            acc = acc + jnp.dot(a_refs[p][r, :], w_ref[p * kp:(p + 1) * kp, :], preferred_element_type=jnp.float32)
        acc_ref[r, :] = acc

    @pl.when(j == pl.num_programs(1) - 1)
    def _():
        o_ref[...] = acc_ref[...].astype(jnp.bfloat16)


def down_call(a_parts, w, resid, n_src, chunk, n_chunks):
    rows, d = resid.shape
    rows //= n_chunks
    parts = len(a_parts)
    kj = w.shape[0]
    kp = kj // parts
    bn = min(1024, d)
    nb = d // bn
    bm = min(256, rows)
    return pl.pallas_call(
        functools.partial(down_kernel, bm, parts),
        grid=(nb, n_src),
        in_specs=[pl.BlockSpec((rows, kp), lambda n, j: (chunk, j))] * parts + [
            pl.BlockSpec((kj, bn), lambda n, j: (0, j * nb + n)),
            pl.BlockSpec((rows, bn), lambda n, j: (chunk, n))],
        out_specs=pl.BlockSpec((rows, bn), lambda n, j: (0, n)),
        out_shape=jax.ShapeDtypeStruct((rows, d), jnp.bfloat16),
        scratch_shapes=[pltpu.VMEM((rows, bn), jnp.float32)],
        compiler_params=params(),
        cost_estimate=cost(2 * rows * d * kj * n_src, 2 * w.size + 4 * rows * d),
        name="down",
    )(*a_parts, w, resid)


def solution(mesh):
    batch_axes = ('dp', 'fsdp')
    n_tp = mesh.shape['tp']
    n_fs = mesh.shape['fsdp']
    in_specs = (P(batch_axes, None, None), P(batch_axes, None), P(batch_axes),
                P('fsdp', 'tp'), P('fsdp', 'tp'), P('fsdp', 'tp'), P('tp', 'fsdp'),
                P('fsdp', 'tp'), P('fsdp', 'tp'), P('tp', 'fsdp'), P(None), P(None))
    out_specs = (P(batch_axes, None, None), P(batch_axes, None, 'tp', None), P(batch_axes, None, 'tp', None))

    def local_layer(tokens, positions, valid_len, w_query, w_key, w_value, w_out, w_gate, w_up, w_down, norm_attn, norm_mlp):
        _, seq, d = tokens.shape
        x = tokens.reshape(seq, d)
        n_q = w_query.shape[1] // HEAD_DIM
        n_kv = w_key.shape[1] // HEAD_DIM
        sub = seq // (n_tp * N_CALLS)
        me = lax.axis_index('tp')
        both = ('tp', 'fsdp')

        w_qkv = lax.all_gather(jnp.concatenate([w_query, w_key, w_value], axis=1), 'fsdp', axis=0, tiled=True)
        full_o = lax.all_gather(w_out, both, axis=1, tiled=True)
        fl = w_gate.shape[1]
        gu_parts = []
        for p in range(2):
            cut = slice(p * fl // 2, (p + 1) * fl // 2)
            local = jnp.concatenate([w_gate[:, cut], w_up[:, cut]], axis=1)
            gu_parts.append(lax.all_gather(local, both, axis=0, tiled=True).reshape(n_tp, d, fl))
        full_d = lax.all_gather(w_down, both, axis=1, tiled=True)

        angles = positions.reshape(seq, 1).astype(jnp.float32) * rope_freqs()[None, :]
        cos_h, sin_h = jnp.cos(angles), jnp.sin(angles)
        cos_t = jnp.concatenate([cos_h, cos_h], axis=1)
        sin_t = jnp.concatenate([-sin_h, sin_h], axis=1)
        q, k, v = qkv_call(x, norm_attn.reshape(1, d), w_qkv, cos_t, sin_t, n_q, n_kv)

        pieces = [[] for _ in range(n_tp)]
        for call in range(N_CALLS):
            o = att_call(q, k, v, valid_len, call)
            for s in range(n_tp):
                blk = lax.dynamic_slice_in_dim(o, (me + s) % n_tp * sub, sub, axis=0)
                if s:
                    blk = lax.ppermute(blk, 'tp', [(i, (i + s) % n_tp) for i in range(n_tp)])
                pieces[s].append(blk)
        o_pieces = [jnp.concatenate(p, axis=0) for p in pieces]
        idx = jnp.stack([me] + [(me - s) % n_tp for s in range(n_tp)]).astype(jnp.int32)
        resid, u = out_call(idx, o_pieces, full_o, x, norm_mlp.reshape(1, d), sub, n_tp)

        a_parts = [gu_call(u, w) for w in gu_parts]
        outs = []
        for c in range(N_CALLS):
            part = down_call(a_parts, full_d, resid, n_tp, c, N_CALLS)
            outs.append(lax.all_gather(part, 'tp', axis=0, tiled=True))
        hidden = jnp.concatenate(outs, axis=0).reshape(1, seq, d)
        return hidden, k.reshape(1, seq, n_kv, HEAD_DIM), v.reshape(1, seq, n_kv, HEAD_DIM)

    return jax.shard_map(local_layer, mesh=mesh, in_specs=in_specs, out_specs=out_specs, check_vma=False)
```

```python
import functools
import math
import jax
import jax.numpy as jnp
from jax import lax
from jax.experimental import pallas as pl
from jax.experimental.pallas import tpu as pltpu
from jax.sharding import Mesh, PartitionSpec as P


HEAD_DIM = 128
ROPE_THETA = 500000.0
NORM_EPS = 1e-5
EXP2_SCALE = HEAD_DIM ** -0.5 * math.log2(math.e)
N_CALLS = 2
VMEM_LIMIT = 67043328


def rope_freqs():
    half_idx = jnp.arange(HEAD_DIM // 2, dtype=jnp.float32)
    inv_freq = jnp.power(ROPE_THETA, -2.0 * half_idx / HEAD_DIM)
    wave_len = 2.0 * math.pi / inv_freq
    smooth = (8192.0 / wave_len - 1.0) / 3.0
    blended = (1.0 - smooth) * inv_freq / 8.0 + smooth * inv_freq
    return jnp.where(wave_len < 2048.0, inv_freq, jnp.where(wave_len > 8192.0, inv_freq / 8.0, blended))


def params(**kw):
    return pltpu.CompilerParams(vmem_limit_bytes=VMEM_LIMIT, **kw)


def cost(flops, nbytes):
    return pl.CostEstimate(flops=flops, bytes_accessed=nbytes, transcendentals=0)


def norm_rows(vals_f32, gain):
    inv = lax.rsqrt(jnp.mean(vals_f32 * vals_f32, axis=-1, keepdims=True) + NORM_EPS)
    return (vals_f32 * inv * gain).astype(jnp.bfloat16)


def qkv_kernel(n_q, n_kv, x_ref, g_ref, w_ref, cos_ref, sin_ref, q_ref, k_ref, v_ref):
    h = norm_rows(x_ref[...].astype(jnp.float32), g_ref[...].astype(jnp.float32))
    cos_t, sin_t = cos_ref[...], sin_ref[...]
    for g in range(n_kv):
        per = n_q // n_kv
        for kind in range(2):
            if kind == 0:
                lo, cnt = g * per, per
            else:
                lo, cnt = n_q + g, 1
            y = jnp.dot(h, w_ref[:, lo * HEAD_DIM:(lo + cnt) * HEAD_DIM], preferred_element_type=jnp.float32)
            for i in range(cnt):
                a = y[:, i * HEAD_DIM:(i + 1) * HEAD_DIM]
                r = (a * cos_t + pltpu.roll(a, HEAD_DIM // 2, 1) * sin_t).astype(jnp.bfloat16)
                if kind == 0:
                    q_ref[lo + i] = r
                else:
                    k_ref[:, g * HEAD_DIM:(g + 1) * HEAD_DIM] = r
    base = (n_q + n_kv) * HEAD_DIM
    v_ref[...] = jnp.dot(h, w_ref[:, base:base + n_kv * HEAD_DIM], preferred_element_type=jnp.float32).astype(jnp.bfloat16)


def qkv_call(x, gain, w, cos_t, sin_t, n_q, n_kv):
    s, d = x.shape
    bm = min(512, s)
    n = w.shape[1]
    row = lambda i: (i, 0)
    return pl.pallas_call(
        functools.partial(qkv_kernel, n_q, n_kv),
        grid=(s // bm,),
        in_specs=[pl.BlockSpec((bm, d), row), pl.BlockSpec((1, d), lambda i: (0, 0)), pl.BlockSpec((d, n), lambda i: (0, 0)),
                  pl.BlockSpec((bm, HEAD_DIM), row), pl.BlockSpec((bm, HEAD_DIM), row)],
        out_specs=[pl.BlockSpec((n_q, bm, HEAD_DIM), lambda i: (0, i, 0)),
                   pl.BlockSpec((bm, n_kv * HEAD_DIM), row), pl.BlockSpec((bm, n_kv * HEAD_DIM), row)],
        out_shape=[jax.ShapeDtypeStruct((n_q, s, HEAD_DIM), jnp.bfloat16),
                   jax.ShapeDtypeStruct((s, n_kv * HEAD_DIM), jnp.bfloat16),
                   jax.ShapeDtypeStruct((s, n_kv * HEAD_DIM), jnp.bfloat16)],
        compiler_params=params(),
        cost_estimate=cost(2 * s * d * n, 2 * s * d + 2 * d * n + 2 * s * n),
        name="qkv",
    )(x, gain, w, cos_t, sin_t)


def att_kernel(bq, bk, per, first, len_ref, q_ref, k_ref, v_ref, o_ref, m_ref, l_ref, acc_ref):
    row0 = first + pl.program_id(1) * bq
    valid = len_ref[0]
    m_ref[...] = jnp.full_like(m_ref, -jnp.inf)
    l_ref[...] = jnp.zeros_like(l_ref)
    acc_ref[...] = jnp.zeros_like(acc_ref)
    reps = bk // HEAD_DIM

    def step(j, masked):
        k0 = pl.multiple_of(j * bk, bk)
        k_blk = k_ref[pl.ds(k0, bk), :]
        v_blk = v_ref[pl.ds(k0, bk), :]
        if masked:
            kid = k0 + lax.broadcasted_iota(jnp.int32, (bq, bk), 1)
            qid = row0 + lax.broadcasted_iota(jnp.int32, (bq, bk), 0)
            allowed = (kid <= qid) & (kid < valid)
        for h in range(per):
            sc = lax.dot_general(q_ref[h], k_blk, (((1,), (1,)), ((), ())), preferred_element_type=jnp.float32)
            if masked:
                sc = jnp.where(allowed, sc, -jnp.inf)
            m_old = m_ref[h]
            m_new = jnp.maximum(m_old, jnp.max(sc, axis=1, keepdims=True))
            p = jnp.exp2((sc - jnp.tile(m_new, (1, reps))) * EXP2_SCALE)
            alpha = jnp.exp2((m_old - m_new) * EXP2_SCALE)
            l_ref[h] = l_ref[h] * alpha + jnp.sum(p, axis=1, keepdims=True)
            acc_ref[h] = acc_ref[h] * alpha + jnp.dot(p.astype(jnp.bfloat16), v_blk, preferred_element_type=jnp.float32)
            m_ref[h] = m_new

    n_full = jnp.minimum((row0 + 1) // bk, valid // bk)
    n_end = jnp.minimum((row0 + bq + bk - 1) // bk, (valid + bk - 1) // bk)

    def full(j, _):
        step(j, False)
        return 0

    def part(j, _):
        step(j, True)
        return 0

    lax.fori_loop(0, n_full, full, 0)
    lax.fori_loop(n_full, n_end, part, 0)
    for h in range(per):
        o_ref[:, h * HEAD_DIM:(h + 1) * HEAD_DIM] = (acc_ref[h] / l_ref[h]).astype(jnp.bfloat16)


def att_call(q, k, v, valid_len, call):
    n_q, s, _ = q.shape
    n_kv = k.shape[1] // HEAD_DIM
    per = n_q // n_kv
    rows = s // N_CALLS
    bq = min(256, rows)
    bk = min(512, s)
    first = call * rows
    off = first // bq
    frac = (2 * call + 1) / N_CALLS ** 2
    kernel = functools.partial(att_kernel, bq, bk, per, first)
    args = [valid_len, q, k, v]
    in_specs = [pl.BlockSpec(memory_space=pltpu.SMEM),
                pl.BlockSpec((per, bq, HEAD_DIM), lambda g, i: (g, off + i, 0)),
                pl.BlockSpec((s, HEAD_DIM), lambda g, i: (0, g)),
                pl.BlockSpec((s, HEAD_DIM), lambda g, i: (0, g))]
    return pl.pallas_call(
        kernel,
        grid=(n_kv, rows // bq),
        in_specs=in_specs,
        out_specs=pl.BlockSpec((bq, per * HEAD_DIM), lambda g, i: (i, g)),
        out_shape=jax.ShapeDtypeStruct((rows, n_q * HEAD_DIM), jnp.bfloat16),
        scratch_shapes=[pltpu.VMEM((per, bq, HEAD_DIM), jnp.float32)] * 3,
        compiler_params=params(),
        cost_estimate=cost(int(8 * frac * n_q * s * s * HEAD_DIM), 4 * n_q * s * HEAD_DIM),
        name="attention",
    )(*args)


def out_kernel(n_src, bn, idx_ref, *refs):
    o_refs = refs[:n_src]
    w_ref, x_ref, g_ref, r_ref, u_ref, y_ref = refs[n_src:]
    d = x_ref.shape[1]

    @pl.loop(0, d // bn)
    def _(n):
        acc = None
        for s in range(n_src):
            col = pl.multiple_of(idx_ref[1 + s] * d + n * bn, bn)
            part = jnp.dot(o_refs[s][...], w_ref[:, pl.ds(col, bn)], preferred_element_type=jnp.float32)
            acc = part if acc is None else acc + part
        col = pl.multiple_of(n * bn, bn)
        y_ref[:, pl.ds(col, bn)] = (x_ref[:, pl.ds(col, bn)].astype(jnp.float32) + acc).astype(jnp.bfloat16)

    r_ref[...] = y_ref[...]
    u_ref[...] = norm_rows(y_ref[...].astype(jnp.float32), g_ref[...].astype(jnp.float32))


def out_call(idx, o_pieces, w, x, gain, sub, n_tp):
    n_src = len(o_pieces)
    rows, ko = o_pieces[0].shape
    d = x.shape[1]
    bn = min(512, d)
    row = lambda i, idx: (i, 0)
    fixed = lambda i, idx: (0, 0)
    return pl.pallas_call(
        functools.partial(out_kernel, n_src, bn),
        grid_spec=pltpu.PrefetchScalarGridSpec(
            num_scalar_prefetch=1,
            grid=(rows // sub,),
            in_specs=[pl.BlockSpec((sub, ko), row)] * n_src + [
                pl.BlockSpec(w.shape, fixed, pipeline_mode=pl.Buffered(1)),
                pl.BlockSpec((sub, d), lambda i, idx: (i * n_tp + idx[0], 0)),
                pl.BlockSpec((1, d), fixed)],
            out_specs=[pl.BlockSpec((sub, d), row), pl.BlockSpec((sub, d), row)],
            scratch_shapes=[pltpu.VMEM((sub, d), jnp.bfloat16)]),
        out_shape=[jax.ShapeDtypeStruct((rows, d), jnp.bfloat16)] * 2,
        compiler_params=params(),
        cost_estimate=cost(2 * rows * d * ko * n_src, 2 * w.size + 8 * rows * d),
        name="w_out",
    )(idx, *o_pieces, w, x, gain)


def gu_kernel(bm, u_ref, g_ref, up_ref, a_ref):
    rows = u_ref.shape[0]

    @pl.loop(0, rows // bm)
    def _(m):
        r = pl.ds(pl.multiple_of(m * bm, bm), bm)
        u = u_ref[r, :]
        gate = jnp.dot(u, g_ref[0], preferred_element_type=jnp.float32)
        up = jnp.dot(u, up_ref[0], preferred_element_type=jnp.float32)
        a_ref[r, :] = (jax.nn.silu(gate) * up).astype(jnp.bfloat16)


def gu_call(u, w):
    rows, d = u.shape
    n_src, _, two = w.shape
    half = two // 2
    bn = min(512, half)
    nb = half // bn
    bm = min(256, rows)
    return pl.pallas_call(
        functools.partial(gu_kernel, bm),
        grid=(n_src, nb),
        in_specs=[pl.BlockSpec((rows, d), lambda j, n: (0, 0), pipeline_mode=pl.Buffered(1)),
                  pl.BlockSpec((1, d, bn), lambda j, n: (j, 0, n)),
                  pl.BlockSpec((1, d, bn), lambda j, n: (j, 0, nb + n))],
        out_specs=pl.BlockSpec((rows, bn), lambda j, n: (0, j * nb + n)),
        out_shape=jax.ShapeDtypeStruct((rows, n_src * half), jnp.bfloat16),
        compiler_params=params(),
        cost_estimate=cost(2 * rows * d * n_src * two, 2 * w.size + 2 * rows * d + 2 * rows * n_src * half),
        name="gate_up",
    )(u, w, w)


def down_kernel(bm, parts, own, *refs):
    a_refs = refs[:parts]
    w_ref = refs[parts]
    rest = refs[parts + 1:]
    acc_ref = rest[-1]
    j = pl.program_id(1)
    kp = a_refs[0].shape[1]
    rows = acc_ref.shape[0]
    half = rows // 2

    @pl.when(j == 0)
    def _():
        if own:
            for h in range(2):
                r = slice(h * half, (h + 1) * half)
                acc_ref[r, :] = rest[0][r, :].astype(jnp.float32) + rest[1 + h][...].astype(jnp.float32)
        else:
            acc_ref[...] = jnp.zeros_like(acc_ref)

    @pl.loop(0, rows // bm)
    def _(m):
        r = pl.ds(pl.multiple_of(m * bm, bm), bm)
        acc = acc_ref[r, :]
        for p in range(parts):
            acc = acc + jnp.dot(a_refs[p][r, :], w_ref[p * kp:(p + 1) * kp, :], preferred_element_type=jnp.float32)
        acc_ref[r, :] = acc

    @pl.when(j == pl.num_programs(1) - 1)
    def _():
        if own:
            rest[3][...] = acc_ref[...].astype(jnp.bfloat16)
        else:
            for h in range(2):
                rest[h][...] = acc_ref[h * half:(h + 1) * half, :].astype(jnp.bfloat16)


def down_call(a_parts, w, rows, chunk, resid=None, partials=()):
    kj = w.shape[0]
    parts = len(a_parts)
    kp = kj // parts
    n_src = a_parts[0].shape[1] // kp
    d = w.shape[1] // n_src
    own = resid is not None
    bn = min(1024, d)
    nb = d // bn
    bm = min(256, rows)
    args = [*a_parts, w]
    in_specs = [pl.BlockSpec((rows, kp), lambda n, j: (chunk, j))] * parts + [pl.BlockSpec((kj, bn), lambda n, j: (0, j * nb + n))]
    col = lambda n, j: (0, n)
    if own:
        args += [resid, *partials]
        in_specs += [pl.BlockSpec((rows, bn), lambda n, j: (chunk, n))] + [pl.BlockSpec((rows // 2, bn), col)] * 2
        out_specs = pl.BlockSpec((rows, bn), col)
        out_shape = jax.ShapeDtypeStruct((rows, d), jnp.bfloat16)
    else:
        out_specs = [pl.BlockSpec((rows // 2, bn), col)] * 2
        out_shape = [jax.ShapeDtypeStruct((rows // 2, d), jnp.bfloat16)] * 2
    return pl.pallas_call(
        functools.partial(down_kernel, bm, parts, own),
        grid=(nb, n_src),
        in_specs=in_specs,
        out_specs=out_specs,
        out_shape=out_shape,
        scratch_shapes=[pltpu.VMEM((rows, bn), jnp.float32)],
        compiler_params=params(),
        cost_estimate=cost(2 * rows * d * kj * n_src, 2 * w.size + 4 * rows * d),
        name="down",
    )(*args)


def after(val, *deps):
    return lax.optimization_barrier((val, *deps))[0]


def solution(mesh):
    n_tp = mesh.shape['tp']
    n_fs = mesh.shape['fsdp']
    mesh2 = Mesh(mesh.devices.reshape(mesh.shape['dp'], n_tp // 2, 2, n_fs), ('dp', 'ta', 'tb', 'fsdp'))
    tp = ('ta', 'tb')
    batch_axes = ('dp', 'fsdp')
    in_specs = (P(batch_axes, None, None), P(batch_axes, None), P(batch_axes),
                P('fsdp', tp), P('fsdp', tp), P('fsdp', tp), P(tp, 'fsdp'),
                P('fsdp', tp), P('fsdp', tp), P(tp, 'fsdp'), P(None), P(None))
    out_specs = (P(batch_axes, None, None), P(batch_axes, None, tp, None), P(batch_axes, None, tp, None))

    def shift(val, s):
        return lax.ppermute(val, tp, [(i, (i + s) % n_tp) for i in range(n_tp)])

    def local_layer(tokens, positions, valid_len, w_query, w_key, w_value, w_out, w_gate, w_up, w_down, norm_attn, norm_mlp):
        _, seq, d = tokens.shape
        x = tokens.reshape(seq, d)
        n_q = w_query.shape[1] // HEAD_DIM
        n_kv = w_key.shape[1] // HEAD_DIM
        sub = seq // (n_tp * N_CALLS)
        me = lax.axis_index(tp)

        w_qkv = lax.all_gather(jnp.concatenate([w_query, w_key, w_value], axis=1), 'fsdp', axis=0, tiled=True)
        full_o = lax.all_gather(w_out, ('ta', 'tb', 'fsdp'), axis=1, tiled=True)
        fl = w_gate.shape[1]
        gu_parts = []
        for p in range(2):
            cut = slice(p * fl // 2, (p + 1) * fl // 2)
            local = jnp.concatenate([w_gate[:, cut], w_up[:, cut]], axis=1)
            gu_parts.append(lax.all_gather(local, ('ta', 'fsdp'), axis=0, tiled=True).reshape(n_tp // 2, d, fl))
        full_d = lax.all_gather(w_down, ('ta', 'fsdp'), axis=1, tiled=True)

        angles = positions.reshape(seq, 1).astype(jnp.float32) * rope_freqs()[None, :]
        cos_h, sin_h = jnp.cos(angles), jnp.sin(angles)
        cos_t = jnp.concatenate([cos_h, cos_h], axis=1)
        sin_t = jnp.concatenate([-sin_h, sin_h], axis=1)
        q, k, v = qkv_call(x, norm_attn.reshape(1, d), w_qkv, cos_t, sin_t, n_q, n_kv)

        pieces = [[] for _ in range(n_tp)]
        for call in range(N_CALLS):
            o = att_call(after(q, *[p[0] for p in pieces[:call]]), k, v, valid_len, call)
            for s in range(n_tp):
                blk = lax.dynamic_slice_in_dim(o, (me + s) % n_tp * sub, sub, axis=0)
                if s:
                    blk = shift(blk, s)
                pieces[s].append(blk)
        o_pieces = [jnp.concatenate(p, axis=0) for p in pieces]
        idx = jnp.stack([me] + [(me - s) % n_tp for s in range(n_tp)]).astype(jnp.int32)
        resid, u = out_call(idx, o_pieces, full_o, x, norm_mlp.reshape(1, d), sub, n_tp)

        u4 = u.reshape(N_CALLS, 2, sub // 2, d)
        u_prev = shift(u4[:, 0], 1)
        u_next = shift(u4[:, 1], -1)
        a_own = [gu_call(u, gu_parts[0])]
        a_own.append(gu_call(after(u, a_own[0]), gu_parts[1]))
        u_prev, u_next = lax.optimization_barrier((u_prev, u_next, a_own[1]))[:2]
        u_recv = jnp.stack([u_prev, u_next], axis=1).reshape(u.shape)
        a_recv = [gu_call(u_recv, gu_parts[0])]
        a_recv.append(gu_call(after(u_recv, a_recv[0]), gu_parts[1]))
        partials = []
        order = a_recv[1]
        for c in range(N_CALLS):
            p_prev, p_next = down_call([after(a_recv[0], order), a_recv[1]], full_d, sub, c)
            order = p_prev
            b_next = shift(p_prev, -1)
            b_prev = shift(p_next, 1)
            partials.append((b_next, b_prev))
        outs = []
        for c in range(N_CALLS):
            mine = down_call([after(a_own[0], order), a_own[1]], full_d, sub, c, resid, partials[c])
            order = mine
            outs.append(lax.all_gather(after(mine, *outs), tp, axis=0, tiled=True))
        hidden = jnp.concatenate(outs, axis=0).reshape(1, seq, d)
        return hidden, k.reshape(1, seq, n_kv, HEAD_DIM), v.reshape(1, seq, n_kv, HEAD_DIM)

    return jax.shard_map(local_layer, mesh=mesh2, in_specs=in_specs, out_specs=out_specs, check_vma=False)
```

```python
import functools
import math
import jax
import jax.numpy as jnp
from jax import lax
from jax.experimental import pallas as pl
from jax.experimental.pallas import tpu as pltpu
from jax.sharding import Mesh, PartitionSpec as P


HEAD_DIM = 128
ROPE_THETA = 500000.0
NORM_EPS = 1e-5
EXP2_SCALE = HEAD_DIM ** -0.5 * math.log2(math.e)
N_CALLS = 2
VMEM_LIMIT = 67043328


def rope_freqs():
    half_idx = jnp.arange(HEAD_DIM // 2, dtype=jnp.float32)
    inv_freq = jnp.power(ROPE_THETA, -2.0 * half_idx / HEAD_DIM)
    wave_len = 2.0 * math.pi / inv_freq
    smooth = (8192.0 / wave_len - 1.0) / 3.0
    blended = (1.0 - smooth) * inv_freq / 8.0 + smooth * inv_freq
    return jnp.where(wave_len < 2048.0, inv_freq, jnp.where(wave_len > 8192.0, inv_freq / 8.0, blended))


def params(**kw):
    return pltpu.CompilerParams(vmem_limit_bytes=VMEM_LIMIT, **kw)


def cost(flops, nbytes):
    return pl.CostEstimate(flops=flops, bytes_accessed=nbytes, transcendentals=0)


def norm_rows(vals_f32, gain):
    inv = lax.rsqrt(jnp.mean(vals_f32 * vals_f32, axis=-1, keepdims=True) + NORM_EPS)
    return (vals_f32 * inv * gain).astype(jnp.bfloat16)


def norm_kernel(x_ref, g_ref, h_ref):
    h_ref[...] = norm_rows(x_ref[...].astype(jnp.float32), g_ref[...].astype(jnp.float32))


def norm_call(x, gain):
    s, d = x.shape
    bm = min(256, s)
    return pl.pallas_call(
        norm_kernel,
        grid=(s // bm,),
        in_specs=[pl.BlockSpec((bm, d), lambda i: (i, 0)), pl.BlockSpec((1, d), lambda i: (0, 0))],
        out_specs=pl.BlockSpec((bm, d), lambda i: (i, 0)),
        out_shape=jax.ShapeDtypeStruct((s, d), jnp.bfloat16),
        compiler_params=params(),
        cost_estimate=cost(8 * s * d, 4 * s * d),
        name="norm",
    )(x, gain)


def qkv_kernel(n_q, n_kv, h_ref, w_ref, cos_ref, sin_ref, q_ref, k_ref, v_ref, vt_ref):
    h = h_ref[...]
    cos_t, sin_t = cos_ref[...], sin_ref[...]
    n_heads = n_q + 2 * n_kv
    for lo in range(0, n_heads, 2):
        y = jnp.dot(h, w_ref[:, lo * HEAD_DIM:(lo + 2) * HEAD_DIM], preferred_element_type=jnp.float32)
        for i in range(lo, lo + 2):
            a = y[:, (i - lo) * HEAD_DIM:(i - lo + 1) * HEAD_DIM]
            if i >= n_q + n_kv:
                cols = slice((i - n_q - n_kv) * HEAD_DIM, (i - n_q - n_kv + 1) * HEAD_DIM)
                v_ref[:, cols] = a.astype(jnp.bfloat16)
                vt_ref[cols, :] = a.T.astype(jnp.bfloat16)
                continue
            r = (a * cos_t + pltpu.roll(a, HEAD_DIM // 2, 1) * sin_t).astype(jnp.bfloat16)
            if i < n_q:
                q_ref[i] = r
            else:
                k_ref[:, (i - n_q) * HEAD_DIM:(i - n_q + 1) * HEAD_DIM] = r


def qkv_call(h, w, cos_t, sin_t, n_q, n_kv):
    s, d = h.shape
    bm = min(512, s)
    n = w.shape[1]
    row = lambda i: (i, 0)
    return pl.pallas_call(
        functools.partial(qkv_kernel, n_q, n_kv),
        grid=(s // bm,),
        in_specs=[pl.BlockSpec((bm, d), row), pl.BlockSpec((d, n), lambda i: (0, 0), pipeline_mode=pl.Buffered(1)),
                  pl.BlockSpec((bm, HEAD_DIM), row), pl.BlockSpec((bm, HEAD_DIM), row)],
        out_specs=[pl.BlockSpec((n_q, bm, HEAD_DIM), lambda i: (0, i, 0)),
                   pl.BlockSpec((bm, n_kv * HEAD_DIM), row), pl.BlockSpec((bm, n_kv * HEAD_DIM), row),
                   pl.BlockSpec((n_kv * HEAD_DIM, bm), lambda i: (0, i))],
        out_shape=[jax.ShapeDtypeStruct((n_q, s, HEAD_DIM), jnp.bfloat16),
                   jax.ShapeDtypeStruct((s, n_kv * HEAD_DIM), jnp.bfloat16),
                   jax.ShapeDtypeStruct((s, n_kv * HEAD_DIM), jnp.bfloat16),
                   jax.ShapeDtypeStruct((n_kv * HEAD_DIM, s), jnp.bfloat16)],
        compiler_params=params(),
        cost_estimate=cost(2 * s * d * n, 2 * s * d + 2 * d * n + 2 * s * n),
        name="qkv",
    )(h, w, cos_t, sin_t)


def att_kernel(bq, bk, per, first, len_ref, q_ref, k_ref, vt_ref, o_ref, s_ref, p_ref, m_ref, l_ref, alpha_ref, acc_ref):
    row0 = first + pl.program_id(1) * bq
    valid = len_ref[0]
    last = k_ref.shape[0] // bk - 1
    m_ref[...] = jnp.full_like(m_ref, -jnp.inf)
    l_ref[...] = jnp.zeros_like(l_ref)
    alpha_ref[...] = jnp.zeros_like(alpha_ref)
    acc_ref[...] = jnp.zeros_like(acc_ref)
    p_ref[...] = jnp.zeros_like(p_ref)

    def scores(j, h):
        k_blk = k_ref[pl.ds(pl.multiple_of(j * bk, bk), bk), :]
        s_ref[h] = lax.dot_general(k_blk, q_ref[h], (((1,), (1,)), ((), ())), preferred_element_type=jnp.float32)

    def values(j, h):
        vt_blk = vt_ref[:, pl.ds(pl.multiple_of(j * bk, bk), bk)]
        acc_ref[h] = acc_ref[h] * alpha_ref[h] + jnp.dot(vt_blk, p_ref[h], preferred_element_type=jnp.float32)

    tall = min(32, bk)

    def softmax(j, h, masked):
        m_old = m_ref[h]
        m8 = None
        for c in range(bk // tall):
            r = slice(c * tall, (c + 1) * tall)
            sc = s_ref[h, r, :]
            if masked:
                kid = j * bk + c * tall + lax.broadcasted_iota(jnp.int32, (tall, bq), 0)
                qid = row0 + lax.broadcasted_iota(jnp.int32, (tall, bq), 1)
                sc = jnp.where((kid <= qid) & (kid < valid), sc, -jnp.inf)
                s_ref[h, r, :] = sc
            top = jnp.max(sc.reshape(tall // 8, 8, bq), axis=0)
            m8 = top if m8 is None else jnp.maximum(m8, top)
        m_new = jnp.maximum(m_old, jnp.max(m8, axis=0, keepdims=True))
        m_rows = jnp.broadcast_to(m_new, (8, bq))[None]
        l8 = None
        for c in range(bk // tall):
            r = slice(c * tall, (c + 1) * tall)
            p = jnp.exp2((s_ref[h, r, :].reshape(tall // 8, 8, bq) - m_rows) * EXP2_SCALE)
            tot = jnp.sum(p, axis=0)
            l8 = tot if l8 is None else l8 + tot
            p_ref[h, r, :] = p.reshape(tall, bq).astype(jnp.bfloat16)
        alpha = jnp.exp2((m_old - m_new) * EXP2_SCALE)
        l_ref[h] = l_ref[h] * alpha + jnp.sum(l8, axis=0, keepdims=True)
        alpha_ref[h] = alpha
        m_ref[h] = m_new

    def step(j, masked):
        for h in range(per):
            values(jnp.maximum(j - 1, 0), h)
            softmax(j, h, masked)
            scores(jnp.minimum(j + 1, last), h)

    n_full = jnp.minimum((row0 + 1) // bk, valid // bk)
    n_end = jnp.minimum((row0 + bq + bk - 1) // bk, (valid + bk - 1) // bk)

    def full(j, _):
        step(j, False)
        return 0

    def part(j, _):
        step(j, True)
        return 0

    for h in range(per):
        scores(0, h)
    lax.fori_loop(0, n_full, full, 0)
    lax.fori_loop(n_full, n_end, part, 0)
    for h in range(per):
        values(n_end - 1, h)
        o_ref[:, h * HEAD_DIM:(h + 1) * HEAD_DIM] = (acc_ref[h] / l_ref[h]).T.astype(jnp.bfloat16)


def att_call(q, k, vt, valid_len, call):
    n_q, s, _ = q.shape
    n_kv = k.shape[1] // HEAD_DIM
    per = n_q // n_kv
    rows = s // N_CALLS
    bq = min(512, rows)
    bk = min(512, s)
    first = call * rows
    off = first // bq
    frac = (2 * call + 1) / N_CALLS ** 2
    return pl.pallas_call(
        functools.partial(att_kernel, bq, bk, per, first),
        grid=(n_kv, rows // bq),
        in_specs=[pl.BlockSpec(memory_space=pltpu.SMEM),
                  pl.BlockSpec((per, bq, HEAD_DIM), lambda g, i: (g, off + i, 0)),
                  pl.BlockSpec((s, HEAD_DIM), lambda g, i: (0, g)),
                  pl.BlockSpec((HEAD_DIM, s), lambda g, i: (g, 0))],
        out_specs=pl.BlockSpec((bq, per * HEAD_DIM), lambda g, i: (i, g)),
        out_shape=jax.ShapeDtypeStruct((rows, n_q * HEAD_DIM), jnp.bfloat16),
        scratch_shapes=[pltpu.VMEM((per, bk, bq), jnp.float32), pltpu.VMEM((per, bk, bq), jnp.bfloat16)]
        + [pltpu.VMEM((per, 1, bq), jnp.float32)] * 3 + [pltpu.VMEM((per, HEAD_DIM, bq), jnp.float32)],
        compiler_params=params(),
        cost_estimate=cost(int(8 * frac * n_q * s * s * HEAD_DIM), 4 * n_q * s * HEAD_DIM),
        name="attention",
    )(valid_len, q, k, vt)


def out_kernel(n_src, bn, idx_ref, *refs):
    o_refs = refs[:n_src]
    w_ref, x_ref, g_ref, r_ref, u_ref, y_ref = refs[n_src:]
    d = x_ref.shape[1]

    @pl.loop(0, d // bn)
    def _(n):
        acc = None
        for s in range(n_src):
            col = pl.multiple_of(idx_ref[1 + s] * d + n * bn, bn)
            part = jnp.dot(o_refs[s][...], w_ref[:, pl.ds(col, bn)], preferred_element_type=jnp.float32)
            acc = part if acc is None else acc + part
        col = pl.multiple_of(n * bn, bn)
        y_ref[:, pl.ds(col, bn)] = (x_ref[:, pl.ds(col, bn)].astype(jnp.float32) + acc).astype(jnp.bfloat16)

    r_ref[...] = y_ref[...]
    u_ref[...] = norm_rows(y_ref[...].astype(jnp.float32), g_ref[...].astype(jnp.float32))


def out_call(idx, o_pieces, w, x, gain, sub, n_tp):
    n_src = len(o_pieces)
    rows, ko = o_pieces[0].shape
    d = x.shape[1]
    bn = min(512, d)
    row = lambda i, idx: (i, 0)
    fixed = lambda i, idx: (0, 0)
    return pl.pallas_call(
        functools.partial(out_kernel, n_src, bn),
        grid_spec=pltpu.PrefetchScalarGridSpec(
            num_scalar_prefetch=1,
            grid=(rows // sub,),
            in_specs=[pl.BlockSpec((sub, ko), row)] * n_src + [
                pl.BlockSpec(w.shape, fixed, pipeline_mode=pl.Buffered(1)),
                pl.BlockSpec((sub, d), lambda i, idx: (i * n_tp + idx[0], 0)),
                pl.BlockSpec((1, d), fixed)],
            out_specs=[pl.BlockSpec((sub, d), row), pl.BlockSpec((sub, d), row)],
            scratch_shapes=[pltpu.VMEM((sub, d), jnp.bfloat16)]),
        out_shape=[jax.ShapeDtypeStruct((rows, d), jnp.bfloat16)] * 2,
        compiler_params=params(),
        cost_estimate=cost(2 * rows * d * ko * n_src, 2 * w.size + 8 * rows * d),
        name="w_out",
    )(idx, *o_pieces, w, x, gain)


def gu_kernel(bm, u_ref, g_ref, up_ref, a_ref):
    rows = u_ref.shape[0]

    @pl.loop(0, rows // bm)
    def _(m):
        r = pl.ds(pl.multiple_of(m * bm, bm), bm)
        u = u_ref[r, :]
        gate = jnp.dot(u, g_ref[...], preferred_element_type=jnp.float32)
        up = jnp.dot(u, up_ref[...], preferred_element_type=jnp.float32)
        a_ref[r, :] = (jax.nn.silu(gate) * up).astype(jnp.bfloat16)


def gu_call(u, w, n_src):
    rows, d = u.shape
    half = w.shape[1] // (2 * n_src)
    bn = min(512, half)
    nb = half // bn
    bm = min(256, rows)
    return pl.pallas_call(
        functools.partial(gu_kernel, bm),
        grid=(n_src, nb),
        in_specs=[pl.BlockSpec((rows, d), lambda j, n: (0, 0), pipeline_mode=pl.Buffered(1)),
                  pl.BlockSpec((d, bn), lambda j, n: (0, 2 * j * nb + n)),
                  pl.BlockSpec((d, bn), lambda j, n: (0, (2 * j + 1) * nb + n))],
        out_specs=pl.BlockSpec((rows, bn), lambda j, n: (0, j * nb + n)),
        out_shape=jax.ShapeDtypeStruct((rows, n_src * half), jnp.bfloat16),
        compiler_params=params(),
        cost_estimate=cost(4 * rows * d * n_src * half, 2 * w.size + 2 * rows * d + 2 * rows * n_src * half),
        name="gate_up",
    )(u, w, w)


def down_kernel(bm, parts, own, *refs):
    a_refs = refs[:parts]
    w_ref = refs[parts]
    rest = refs[parts + 1:]
    acc_ref = rest[-1]
    j = pl.program_id(1)
    kp = a_refs[0].shape[1]
    rows = acc_ref.shape[0]
    half = rows // 2

    @pl.when(j == 0)
    def _():
        if own:
            for h in range(2):
                r = slice(h * half, (h + 1) * half)
                acc_ref[r, :] = rest[0][r, :].astype(jnp.float32) + rest[1 + h][...].astype(jnp.float32)
        else:
            acc_ref[...] = jnp.zeros_like(acc_ref)

    @pl.loop(0, rows // bm)
    def _(m):
        r = pl.ds(pl.multiple_of(m * bm, bm), bm)
        acc = acc_ref[r, :]
        for p in range(parts):
            acc = acc + jnp.dot(a_refs[p][r, :], w_ref[p * kp:(p + 1) * kp, :], preferred_element_type=jnp.float32)
        acc_ref[r, :] = acc

    @pl.when(j == pl.num_programs(1) - 1)
    def _():
        if own:
            rest[3][...] = acc_ref[...].astype(jnp.bfloat16)
        else:
            for h in range(2):
                rest[h][...] = acc_ref[h * half:(h + 1) * half, :].astype(jnp.bfloat16)


def down_call(a_parts, w, n_src, rows, chunk, resid=None, partials=()):
    d = w.shape[1]
    parts = len(a_parts)
    kj = w.shape[0] // n_src
    kp = kj // parts
    own = resid is not None
    bn = min(1024, d)
    nb = d // bn
    bm = min(256, rows)
    args = [*a_parts, w]
    in_specs = [pl.BlockSpec((rows, kp), lambda n, j: (chunk, j))] * parts + [pl.BlockSpec((kj, bn), lambda n, j: (j, n))]
    col = lambda n, j: (0, n)
    if own:
        args += [resid, *partials]
        in_specs += [pl.BlockSpec((rows, bn), lambda n, j: (chunk, n))] + [pl.BlockSpec((rows // 2, bn), col)] * 2
        out_specs = pl.BlockSpec((rows, bn), col)
        out_shape = jax.ShapeDtypeStruct((rows, d), jnp.bfloat16)
    else:
        out_specs = [pl.BlockSpec((rows // 2, bn), col)] * 2
        out_shape = [jax.ShapeDtypeStruct((rows // 2, d), jnp.bfloat16)] * 2
    return pl.pallas_call(
        functools.partial(down_kernel, bm, parts, own),
        grid=(nb, n_src),
        in_specs=in_specs,
        out_specs=out_specs,
        out_shape=out_shape,
        scratch_shapes=[pltpu.VMEM((rows, bn), jnp.float32)],
        compiler_params=params(),
        cost_estimate=cost(2 * rows * d * kj * n_src, 2 * w.size + 4 * rows * d),
        name="down",
    )(*args)


def after(val, *deps):
    return lax.optimization_barrier((val, *deps))[0]


def solution(mesh):
    n_tp = mesh.shape['tp']
    n_fs = mesh.shape['fsdp']
    mesh2 = Mesh(mesh.devices.reshape(mesh.shape['dp'], n_tp // 2, 2, n_fs), ('dp', 'ta', 'tb', 'fsdp'))
    tp = ('ta', 'tb')
    batch_axes = ('dp', 'fsdp')
    in_specs = (P(batch_axes, None, None), P(batch_axes, None), P(batch_axes),
                P('fsdp', tp), P('fsdp', tp), P('fsdp', tp), P(tp, 'fsdp'),
                P('fsdp', tp), P('fsdp', tp), P(tp, 'fsdp'), P(None), P(None))
    out_specs = (P(batch_axes, None, None), P(batch_axes, None, tp, None), P(batch_axes, None, tp, None))

    def shift(val, s):
        return lax.ppermute(val, tp, [(i, (i + s) % n_tp) for i in range(n_tp)])

    def local_layer(tokens, positions, valid_len, w_query, w_key, w_value, w_out, w_gate, w_up, w_down, norm_attn, norm_mlp):
        _, seq, d = tokens.shape
        x = tokens.reshape(seq, d)
        n_q = w_query.shape[1] // HEAD_DIM
        n_kv = w_key.shape[1] // HEAD_DIM
        sub = seq // (n_tp * N_CALLS)
        me = lax.axis_index(tp)

        w_qkv = lax.all_gather(jnp.concatenate([w_query, w_key, w_value], axis=1), 'fsdp', axis=0, tiled=True)
        full_o = lax.all_gather(w_out, ('ta', 'tb', 'fsdp'), axis=1, tiled=True)
        fl = w_gate.shape[1]
        n_src = 2
        swaps = []
        for p in range(2):
            cut = slice(p * fl // 2, (p + 1) * fl // 2)
            local = jnp.concatenate([w_gate[:, cut], w_up[:, cut]], axis=1)
            swaps.append((local, shift(local, 2)))
        swaps.append((w_down, shift(w_down, 2)))

        def joined(p, axis, *deps):
            return jnp.concatenate([after(swaps[p][0], *deps), swaps[p][1]], axis=axis)

        angles = positions.reshape(seq, 1).astype(jnp.float32) * rope_freqs()[None, :]
        cos_h, sin_h = jnp.cos(angles), jnp.sin(angles)
        cos_t = jnp.concatenate([cos_h, cos_h], axis=1)
        sin_t = jnp.concatenate([-sin_h, sin_h], axis=1)
        h = norm_call(x, norm_attn.reshape(1, d))
        q, k, v, vt = qkv_call(h, w_qkv, cos_t, sin_t, n_q, n_kv)

        pieces = [[] for _ in range(n_tp)]
        gu_parts = []
        o = q
        for call in range(N_CALLS):
            gu_parts.append(joined(call, 1, o))
            o = att_call(after(q, gu_parts[call], o), k, vt, valid_len, call)
            for s in range(n_tp):
                blk = lax.dynamic_slice_in_dim(o, (me + s) % n_tp * sub, sub, axis=0)
                if s:
                    blk = shift(blk, s)
                pieces[s].append(blk)
        d_part = joined(2, 0, o)
        gu_full = [lax.all_gather(w, 'fsdp', axis=0, tiled=True) for w in gu_parts]
        full_d = lax.all_gather(d_part, 'fsdp', axis=1, tiled=True)
        o_pieces = [jnp.concatenate(p, axis=0) for p in pieces]
        o_pieces[0] = after(o_pieces[0], d_part)
        idx = jnp.stack([me] + [(me - s) % n_tp for s in range(n_tp)]).astype(jnp.int32)
        resid, u = out_call(idx, o_pieces, full_o, x, norm_mlp.reshape(1, d), sub, n_tp)

        u4 = u.reshape(N_CALLS, 2, sub // 2, d)
        u_prev = shift(u4[:, 0], 1)
        u_next = shift(u4[:, 1], -1)
        a_own = [gu_call(u, gu_full[0], n_src)]
        a_own.append(gu_call(after(u, a_own[0]), gu_full[1], n_src))
        u_prev, u_next = lax.optimization_barrier((u_prev, u_next, a_own[1]))[:2]
        u_recv = jnp.stack([u_prev, u_next], axis=1).reshape(u.shape)
        a_recv = [gu_call(u_recv, gu_full[0], n_src)]
        a_recv.append(gu_call(after(u_recv, a_recv[0]), gu_full[1], n_src))
        partials = []
        order = a_recv[1]
        for c in range(N_CALLS):
            p_prev, p_next = down_call([after(a_recv[0], order), a_recv[1]], full_d, n_src, sub, c)
            order = p_prev
            b_next = shift(p_prev, -1)
            b_prev = shift(p_next, 1)
            partials.append((b_next, b_prev))
        outs = []
        for c in range(N_CALLS):
            mine = down_call([after(a_own[0], order), a_own[1]], full_d, n_src, sub, c, resid, partials[c])
            order = mine
            outs.append(lax.all_gather(after(mine, *outs), tp, axis=0, tiled=True))
        hidden = jnp.concatenate(outs, axis=0).reshape(1, seq, d)
        return hidden, k.reshape(1, seq, n_kv, HEAD_DIM), v.reshape(1, seq, n_kv, HEAD_DIM)

    return jax.shard_map(local_layer, mesh=mesh2, in_specs=in_specs, out_specs=out_specs, check_vma=False)
```

```python
import functools
import math
import jax
import jax.numpy as jnp
from jax import lax
from jax.experimental import pallas as pl
from jax.experimental.pallas import tpu as pltpu
from jax.sharding import Mesh, PartitionSpec as P


HEAD_DIM = 128
ROPE_THETA = 500000.0
NORM_EPS = 1e-5
EXP2_SCALE = HEAD_DIM ** -0.5 * math.log2(math.e)
N_CALLS = 2
VMEM_LIMIT = 67043328


def rope_freqs():
    half_idx = jnp.arange(HEAD_DIM // 2, dtype=jnp.float32)
    inv_freq = jnp.power(ROPE_THETA, -2.0 * half_idx / HEAD_DIM)
    wave_len = 2.0 * math.pi / inv_freq
    smooth = (8192.0 / wave_len - 1.0) / 3.0
    blended = (1.0 - smooth) * inv_freq / 8.0 + smooth * inv_freq
    return jnp.where(wave_len < 2048.0, inv_freq, jnp.where(wave_len > 8192.0, inv_freq / 8.0, blended))


def params(**kw):
    return pltpu.CompilerParams(vmem_limit_bytes=VMEM_LIMIT, **kw)


def cost(flops, nbytes):
    return pl.CostEstimate(flops=flops, bytes_accessed=nbytes, transcendentals=0)


def norm_rows(vals_f32, gain):
    inv = lax.rsqrt(jnp.mean(vals_f32 * vals_f32, axis=-1, keepdims=True) + NORM_EPS)
    return (vals_f32 * inv * gain).astype(jnp.bfloat16)


def norm_kernel(x_ref, g_ref, h_ref):
    h_ref[...] = norm_rows(x_ref[...].astype(jnp.float32), g_ref[...].astype(jnp.float32))


def norm_call(x, gain):
    s, d = x.shape
    bm = min(256, s)
    return pl.pallas_call(
        norm_kernel,
        grid=(s // bm,),
        in_specs=[pl.BlockSpec((bm, d), lambda i: (i, 0)), pl.BlockSpec((1, d), lambda i: (0, 0))],
        out_specs=pl.BlockSpec((bm, d), lambda i: (i, 0)),
        out_shape=jax.ShapeDtypeStruct((s, d), jnp.bfloat16),
        compiler_params=params(),
        cost_estimate=cost(8 * s * d, 4 * s * d),
        name="norm",
    )(x, gain)


def qkv_kernel(n_q, n_kv, h_ref, w_ref, cos_ref, sin_ref, q_ref, k_ref, v_ref, vt_ref):
    h = h_ref[...]
    cos_t, sin_t = cos_ref[...], sin_ref[...]
    n_heads = n_q + 2 * n_kv
    for lo in range(0, n_heads, 2):
        y = jnp.dot(h, w_ref[:, lo * HEAD_DIM:(lo + 2) * HEAD_DIM], preferred_element_type=jnp.float32)
        for i in range(lo, lo + 2):
            a = y[:, (i - lo) * HEAD_DIM:(i - lo + 1) * HEAD_DIM]
            if i >= n_q + n_kv:
                cols = slice((i - n_q - n_kv) * HEAD_DIM, (i - n_q - n_kv + 1) * HEAD_DIM)
                v_ref[:, cols] = a.astype(jnp.bfloat16)
                vt_ref[cols, :] = a.T.astype(jnp.bfloat16)
                continue
            r = (a * cos_t + pltpu.roll(a, HEAD_DIM // 2, 1) * sin_t).astype(jnp.bfloat16)
            if i < n_q:
                q_ref[i] = r
            else:
                k_ref[:, (i - n_q) * HEAD_DIM:(i - n_q + 1) * HEAD_DIM] = r


def qkv_call(h, w, cos_t, sin_t, n_q, n_kv):
    s, d = h.shape
    bm = min(512, s)
    n = w.shape[1]
    row = lambda i: (i, 0)
    return pl.pallas_call(
        functools.partial(qkv_kernel, n_q, n_kv),
        grid=(s // bm,),
        in_specs=[pl.BlockSpec((bm, d), row), pl.BlockSpec((d, n), lambda i: (0, 0), pipeline_mode=pl.Buffered(1)),
                  pl.BlockSpec((bm, HEAD_DIM), row), pl.BlockSpec((bm, HEAD_DIM), row)],
        out_specs=[pl.BlockSpec((n_q, bm, HEAD_DIM), lambda i: (0, i, 0)),
                   pl.BlockSpec((bm, n_kv * HEAD_DIM), row), pl.BlockSpec((bm, n_kv * HEAD_DIM), row),
                   pl.BlockSpec((n_kv * HEAD_DIM, bm), lambda i: (0, i))],
        out_shape=[jax.ShapeDtypeStruct((n_q, s, HEAD_DIM), jnp.bfloat16),
                   jax.ShapeDtypeStruct((s, n_kv * HEAD_DIM), jnp.bfloat16),
                   jax.ShapeDtypeStruct((s, n_kv * HEAD_DIM), jnp.bfloat16),
                   jax.ShapeDtypeStruct((n_kv * HEAD_DIM, s), jnp.bfloat16)],
        compiler_params=params(),
        cost_estimate=cost(2 * s * d * n, 2 * s * d + 2 * d * n + 2 * s * n),
        name="qkv",
    )(h, w, cos_t, sin_t)


def att_kernel(bq, bk, per, first, len_ref, q_ref, k_ref, vt_ref, o_ref, s_ref, p_ref, m_ref, l_ref, alpha_ref, acc_ref):
    row0 = first + pl.program_id(1) * bq
    valid = len_ref[0]
    last = k_ref.shape[0] // bk - 1
    m_ref[...] = jnp.full_like(m_ref, -jnp.inf)
    l_ref[...] = jnp.zeros_like(l_ref)
    alpha_ref[...] = jnp.zeros_like(alpha_ref)
    acc_ref[...] = jnp.zeros_like(acc_ref)
    p_ref[...] = jnp.zeros_like(p_ref)

    def scores(j, h):
        k_blk = k_ref[pl.ds(pl.multiple_of(j * bk, bk), bk), :]
        s_ref[h] = lax.dot_general(k_blk, q_ref[h], (((1,), (1,)), ((), ())), preferred_element_type=jnp.float32)

    def values(j, h):
        vt_blk = vt_ref[:, pl.ds(pl.multiple_of(j * bk, bk), bk)]
        acc_ref[h] = acc_ref[h] * alpha_ref[h] + jnp.dot(vt_blk, p_ref[h], preferred_element_type=jnp.float32)

    tall = min(32, bk)

    def softmax(j, h, masked):
        m_old = m_ref[h]
        m8 = None
        for c in range(bk // tall):
            r = slice(c * tall, (c + 1) * tall)
            sc = s_ref[h, r, :]
            if masked:
                kid = j * bk + c * tall + lax.broadcasted_iota(jnp.int32, (tall, bq), 0)
                qid = row0 + lax.broadcasted_iota(jnp.int32, (tall, bq), 1)
                sc = jnp.where((kid <= qid) & (kid < valid), sc, -jnp.inf)
                s_ref[h, r, :] = sc
            top = jnp.max(sc.reshape(tall // 8, 8, bq), axis=0)
            m8 = top if m8 is None else jnp.maximum(m8, top)
        m_new = jnp.maximum(m_old, jnp.max(m8, axis=0, keepdims=True))
        m_rows = jnp.broadcast_to(m_new, (8, bq))[None]
        l8 = None
        for c in range(bk // tall):
            r = slice(c * tall, (c + 1) * tall)
            p = jnp.exp2((s_ref[h, r, :].reshape(tall // 8, 8, bq) - m_rows) * EXP2_SCALE)
            tot = jnp.sum(p, axis=0)
            l8 = tot if l8 is None else l8 + tot
            p_ref[h, r, :] = p.reshape(tall, bq).astype(jnp.bfloat16)
        alpha = jnp.exp2((m_old - m_new) * EXP2_SCALE)
        l_ref[h] = l_ref[h] * alpha + jnp.sum(l8, axis=0, keepdims=True)
        alpha_ref[h] = alpha
        m_ref[h] = m_new

    def step(j, masked):
        for h in range(per):
            values(jnp.maximum(j - 1, 0), h)
            softmax(j, h, masked)
            scores(jnp.minimum(j + 1, last), h)

    n_full = jnp.minimum((row0 + 1) // bk, valid // bk)
    n_end = jnp.minimum((row0 + bq + bk - 1) // bk, (valid + bk - 1) // bk)

    def full(j, _):
        step(j, False)
        return 0

    def part(j, _):
        step(j, True)
        return 0

    for h in range(per):
        scores(0, h)
    lax.fori_loop(0, n_full, full, 0)
    lax.fori_loop(n_full, n_end, part, 0)
    for h in range(per):
        values(n_end - 1, h)
        o_ref[:, h * HEAD_DIM:(h + 1) * HEAD_DIM] = (acc_ref[h] / l_ref[h]).T.astype(jnp.bfloat16)


def att_call(q, k, vt, valid_len, call):
    n_q, s, _ = q.shape
    n_kv = k.shape[1] // HEAD_DIM
    per = n_q // n_kv
    rows = s // N_CALLS
    bq = min(512, rows)
    bk = min(512, s)
    first = call * rows
    off = first // bq
    frac = (2 * call + 1) / N_CALLS ** 2
    return pl.pallas_call(
        functools.partial(att_kernel, bq, bk, per, first),
        grid=(n_kv, rows // bq),
        in_specs=[pl.BlockSpec(memory_space=pltpu.SMEM),
                  pl.BlockSpec((per, bq, HEAD_DIM), lambda g, i: (g, off + i, 0)),
                  pl.BlockSpec((s, HEAD_DIM), lambda g, i: (0, g)),
                  pl.BlockSpec((HEAD_DIM, s), lambda g, i: (g, 0))],
        out_specs=pl.BlockSpec((bq, per * HEAD_DIM), lambda g, i: (i, g)),
        out_shape=jax.ShapeDtypeStruct((rows, n_q * HEAD_DIM), jnp.bfloat16),
        scratch_shapes=[pltpu.VMEM((per, bk, bq), jnp.float32), pltpu.VMEM((per, bk, bq), jnp.bfloat16)]
        + [pltpu.VMEM((per, 1, bq), jnp.float32)] * 3 + [pltpu.VMEM((per, HEAD_DIM, bq), jnp.float32)],
        compiler_params=params(),
        cost_estimate=cost(int(8 * frac * n_q * s * s * HEAD_DIM), 4 * n_q * s * HEAD_DIM),
        name="attention",
    )(valid_len, q, k, vt)


def out_kernel(n_src, idx_ref, *refs):
    o_refs = refs[:n_src]
    w_ref, x_ref, g_ref, r_ref, ua_ref, ub_ref, o_all, y_ref = refs[n_src:]
    ko = o_refs[0].shape[1]
    n = pl.program_id(0)
    bn = w_ref.shape[1]
    half = ua_ref.shape[0]

    @pl.when(n == 0)
    def _():
        for s in range(n_src):
            o_all[:, s * ko:(s + 1) * ko] = o_refs[s][...]

    acc = jnp.dot(o_all[...], w_ref[...], preferred_element_type=jnp.float32)
    col = pl.ds(pl.multiple_of(n * bn, bn), bn)
    y_ref[:, col] = (x_ref[:, col].astype(jnp.float32) + acc).astype(jnp.bfloat16)

    @pl.when(n == pl.num_programs(0) - 1)
    def _():
        r_ref[...] = y_ref[...]
        u = norm_rows(y_ref[...].astype(jnp.float32), g_ref[...].astype(jnp.float32))
        ua_ref[...] = u[:half]
        ub_ref[...] = u[half:]


def out_call(idx, o_pieces, w, x, gain):
    n_src = len(o_pieces)
    rows, ko = o_pieces[0].shape
    d = x.shape[1]
    bn = min(512, d)
    fixed = lambda n, idx: (0, 0)
    half = jax.ShapeDtypeStruct((rows // 2, d), jnp.bfloat16)
    return pl.pallas_call(
        functools.partial(out_kernel, n_src),
        grid_spec=pltpu.PrefetchScalarGridSpec(
            num_scalar_prefetch=1,
            grid=(d // bn,),
            in_specs=[pl.BlockSpec((rows, ko), fixed)] * n_src + [
                pl.BlockSpec((n_src * ko, bn), lambda n, idx: (0, n)),
                pl.BlockSpec((rows, d), lambda n, idx: (idx[0], 0)),
                pl.BlockSpec((1, d), fixed)],
            out_specs=[pl.BlockSpec((rows, d), fixed), pl.BlockSpec((rows // 2, d), fixed), pl.BlockSpec((rows // 2, d), fixed)],
            scratch_shapes=[pltpu.VMEM((rows, n_src * ko), jnp.bfloat16), pltpu.VMEM((rows, d), jnp.bfloat16)]),
        out_shape=[jax.ShapeDtypeStruct((rows, d), jnp.bfloat16), half, half],
        compiler_params=params(),
        cost_estimate=cost(2 * rows * d * ko * n_src, 2 * w.size + 8 * rows * d),
        name="w_out",
    )(idx, *o_pieces, w, x, gain)


def gu_kernel(bm, n_u, *refs):
    u_refs = refs[:n_u]
    g_ref, up_ref, a_ref, u_all, sem = refs[n_u:]
    rows = u_all.shape[0]
    piece = rows // n_u

    @pl.when((pl.program_id(0) == 0) & (pl.program_id(1) == 0))
    def _():
        copies = [pltpu.make_async_copy(u_refs[i], u_all.at[i * piece:(i + 1) * piece, :], sem.at[i]) for i in range(n_u)]
        for c in copies:
            c.start()
        for c in copies:
            c.wait()

    @pl.loop(0, rows // bm)
    def _(m):
        r = pl.ds(pl.multiple_of(m * bm, bm), bm)
        u = u_all[r, :]
        gate = jnp.dot(u, g_ref[...], preferred_element_type=jnp.float32)
        up = jnp.dot(u, up_ref[...], preferred_element_type=jnp.float32)
        a_ref[r, :] = (jax.nn.silu(gate) * up).astype(jnp.bfloat16)


def gu_call(us, w, n_src):
    n_u = len(us)
    rows, d = us[0].shape
    rows *= n_u
    half = w.shape[1] // (2 * n_src)
    bn = min(512, half)
    nb = half // bn
    bm = min(256, rows)
    return pl.pallas_call(
        functools.partial(gu_kernel, bm, n_u),
        grid=(n_src, nb),
        in_specs=[pl.BlockSpec(memory_space=pl.ANY)] * n_u + [
            pl.BlockSpec((d, bn), lambda j, n: (0, 2 * j * nb + n)),
            pl.BlockSpec((d, bn), lambda j, n: (0, (2 * j + 1) * nb + n))],
        out_specs=pl.BlockSpec((rows, bn), lambda j, n: (0, j * nb + n)),
        out_shape=jax.ShapeDtypeStruct((rows, n_src * half), jnp.bfloat16),
        scratch_shapes=[pltpu.VMEM((rows, d), jnp.bfloat16), pltpu.SemaphoreType.DMA((n_u,))],
        compiler_params=params(),
        cost_estimate=cost(4 * rows * d * n_src * half, 2 * w.size + 2 * rows * d + 2 * rows * n_src * half),
        name="gate_up",
    )(*us, w, w)


def down_kernel(bm, parts, own, n_f, blk, n_blk, *refs):
    a_refs = refs[:parts]
    w_ref = refs[parts]
    rest = refs[parts + 1:]
    acc_ref = rest[-1]
    j = pl.program_id(0)
    kp = a_refs[0].shape[1]
    rows, cols = acc_ref.shape
    lanes = cols // n_f

    @pl.when(j == 0)
    def _():
        if own:
            quarter = rows // (2 * N_CALLS)
            for c in range(N_CALLS):
                for h in range(2):
                    r = slice((2 * c + h) * quarter, (2 * c + h + 1) * quarter)
                    for f in range(n_f):
                        src = slice((f * n_blk + blk) * lanes, (f * n_blk + blk + 1) * lanes)
                        dst = slice(f * lanes, (f + 1) * lanes)
                        part = rest[N_CALLS + h][c * quarter:(c + 1) * quarter, dst].astype(jnp.float32)
                        acc_ref[r, dst] = rest[c][h * quarter:(h + 1) * quarter, src].astype(jnp.float32) + part
        else:
            acc_ref[...] = jnp.zeros_like(acc_ref)

    @pl.loop(0, rows // bm)
    def _(m):
        r = pl.ds(pl.multiple_of(m * bm, bm), bm)
        acc = acc_ref[r, :]
        for p in range(parts):
            acc = acc + jnp.dot(a_refs[p][r, :], w_ref[p * kp:(p + 1) * kp, :], preferred_element_type=jnp.float32)
        acc_ref[r, :] = acc

    @pl.when(j == pl.num_programs(0) - 1)
    def _():
        if own:
            rest[N_CALLS + 2][...] = acc_ref[...].astype(jnp.bfloat16)
        else:
            for h in range(2):
                rest[h][...] = acc_ref[h * rows // 2:(h + 1) * rows // 2, :].astype(jnp.bfloat16)


def down_call(a_parts, w, n_src, n_f, blk, n_blk, resid=None, partials=()):
    cols = w.shape[1]
    parts = len(a_parts)
    rows = a_parts[0].shape[0]
    kj = w.shape[0] // n_src
    kp = kj // parts
    own = resid is not None
    bm = min(256, rows)
    fixed = lambda j: (0, 0)
    args = [*a_parts, w]
    in_specs = [pl.BlockSpec((rows, kp), lambda j: (0, j))] * parts + [pl.BlockSpec((kj, cols), lambda j: (j, 0))]
    if own:
        args += [*resid, *partials]
        in_specs += [pl.BlockSpec(r.shape, fixed, pipeline_mode=pl.Buffered(1)) for r in (*resid, *partials)]
        out_specs = pl.BlockSpec((rows, cols), fixed)
        out_shape = jax.ShapeDtypeStruct((rows, cols), jnp.bfloat16)
    else:
        out_specs = [pl.BlockSpec((rows // 2, cols), fixed)] * 2
        out_shape = [jax.ShapeDtypeStruct((rows // 2, cols), jnp.bfloat16)] * 2
    return pl.pallas_call(
        functools.partial(down_kernel, bm, parts, own, n_f, blk, n_blk),
        grid=(n_src,),
        in_specs=in_specs,
        out_specs=out_specs,
        out_shape=out_shape,
        scratch_shapes=[pltpu.VMEM((rows, cols), jnp.float32)],
        compiler_params=params(),
        cost_estimate=cost(2 * rows * cols * kj * n_src, 2 * w.size + 4 * rows * cols),
        name="down",
    )(*args)


def place_kernel(n_in, moves, n_f, blk, n_blk, idx_ref, *refs):
    ins = refs[:n_in]
    out_ref, sem = refs[-2:]
    copies = []
    for i, src_row, rows, call, who in moves:
        lanes = ins[i].shape[1] // n_f
        row = pl.multiple_of(idx_ref[who] * rows + call * rows * (idx_ref.shape[0] - 1), rows)
        for f in range(n_f):
            copies.append(pltpu.make_async_copy(
                ins[i].at[src_row:src_row + rows, f * lanes:(f + 1) * lanes],
                out_ref.at[pl.ds(row, rows), (f * n_blk + blk) * lanes:(f * n_blk + blk + 1) * lanes],
                sem.at[len(copies)]))
    for c in copies:
        c.start()
    for c in copies:
        c.wait()


def place_call(idx, pieces, moves, shape, n_f, blk, n_blk, out):
    n_in = len(pieces)
    args = list(pieces)
    in_specs = [pl.BlockSpec(p.shape, lambda *_: (0, 0)) for p in pieces]
    aliases = {}
    if out is not None:
        args.append(out)
        in_specs.append(pl.BlockSpec(memory_space=pl.ANY))
        aliases = {n_in + 1: 0}
    return pl.pallas_call(
        functools.partial(place_kernel, n_in, moves, n_f, blk, n_blk),
        grid_spec=pltpu.PrefetchScalarGridSpec(
            num_scalar_prefetch=1, grid=(1,), in_specs=in_specs, out_specs=pl.BlockSpec(memory_space=pl.ANY),
            scratch_shapes=[pltpu.SemaphoreType.DMA((len(moves) * n_f,))]),
        out_shape=jax.ShapeDtypeStruct(shape, jnp.bfloat16),
        input_output_aliases=aliases,
        compiler_params=params(),
        cost_estimate=cost(1000000, 4 * sum(p.size for p in pieces)),
        name="place",
    )(idx, *args)


def after(val, *deps):
    return lax.optimization_barrier((val, *deps))[0]


def solution(mesh):
    n_tp = mesh.shape['tp']
    n_fs = mesh.shape['fsdp']
    mesh2 = Mesh(mesh.devices.reshape(mesh.shape['dp'], n_tp // 2, 2, n_fs), ('dp', 'ta', 'tb', 'fsdp'))
    tp = ('ta', 'tb')
    batch_axes = ('dp', 'fsdp')
    in_specs = (P(batch_axes, None, None), P(batch_axes, None), P(batch_axes),
                P('fsdp', tp), P('fsdp', tp), P('fsdp', tp), P(tp, 'fsdp'),
                P('fsdp', tp), P('fsdp', tp), P(tp, 'fsdp'), P(None), P(None))
    out_specs = (P(batch_axes, None, None), P(batch_axes, None, tp, None), P(batch_axes, None, tp, None))

    def shift(val, s):
        return lax.ppermute(val, tp, [(i, (i + s) % n_tp) for i in range(n_tp)])

    def local_layer(tokens, positions, valid_len, w_query, w_key, w_value, w_out, w_gate, w_up, w_down, norm_attn, norm_mlp):
        _, seq, d = tokens.shape
        x = tokens.reshape(seq, d)
        n_q = w_query.shape[1] // HEAD_DIM
        n_kv = w_key.shape[1] // HEAD_DIM
        sub = seq // (n_tp * N_CALLS)
        me = lax.axis_index(tp)

        w_qkv = lax.all_gather(jnp.concatenate([w_query, w_key, w_value], axis=1), 'fsdp', axis=0, tiled=True)
        rounds = []
        for s in range(1, n_tp):
            rounds.append(shift(w_out, s))
        full_o = lax.all_gather(jnp.concatenate([w_out, *rounds], axis=0), 'fsdp', axis=1, tiled=True)
        fl = w_gate.shape[1]
        n_src = 2
        swaps = []
        for p in range(2):
            cut = slice(p * fl // 2, (p + 1) * fl // 2)
            local = jnp.concatenate([w_gate[:, cut], w_up[:, cut]], axis=1)
            swaps.append((local, shift(local, 2)))
        swaps.append((w_down, shift(w_down, 2)))

        def joined(p, axis, *deps):
            return jnp.concatenate([after(swaps[p][0], *deps), swaps[p][1]], axis=axis)

        angles = positions.reshape(seq, 1).astype(jnp.float32) * rope_freqs()[None, :]
        cos_h, sin_h = jnp.cos(angles), jnp.sin(angles)
        cos_t = jnp.concatenate([cos_h, cos_h], axis=1)
        sin_t = jnp.concatenate([-sin_h, sin_h], axis=1)
        h = norm_call(x, norm_attn.reshape(1, d))
        q, k, v, vt = qkv_call(h, w_qkv, cos_t, sin_t, n_q, n_kv)

        pieces = []
        gu_parts = []
        o = q
        for call in range(N_CALLS):
            gu_parts.append(joined(call, 1, o))
            o = att_call(after(q, gu_parts[call], o), k, vt, valid_len, call)
            got = []
            for s in range(n_tp):
                blk = lax.dynamic_slice_in_dim(o, (me + s) % n_tp * sub, sub, axis=0)
                if s:
                    blk = shift(blk, s)
                got.append(blk)
            pieces.append(got)
        d_part = joined(2, 0, o)
        gu_full = [lax.all_gather(w, 'fsdp', axis=0, tiled=True) for w in gu_parts]
        n_blk = w_down.shape[1] // HEAD_DIM
        d_full = [lax.all_gather(d_part[:, b * HEAD_DIM:(b + 1) * HEAD_DIM], 'fsdp', axis=1, tiled=True) for b in range(n_blk)]

        resid, u_own, u_prev, u_next = [], [], [], []
        order = d_part
        for call in range(N_CALLS):
            got = pieces[call]
            got[0] = after(got[0], order)
            row = (call * n_tp + me).reshape(1).astype(jnp.int32)
            r, ua, ub = out_call(row, got, full_o, x, norm_mlp.reshape(1, d))
            order = r
            resid.append(r)
            u_own += [ua, ub]
            u_prev.append(shift(ua, 1))
            u_next.append(shift(ub, -1))
        u_recv = u_prev + u_next

        a_own = [gu_call(u_own, gu_full[0], n_src)]
        a_own.append(gu_call([after(u_own[0], a_own[0])] + u_own[1:], gu_full[1], n_src))
        a_recv = [gu_call([after(u_recv[0], a_own[1])] + u_recv[1:], gu_full[0], n_src)]
        a_recv.append(gu_call([after(u_recv[0], a_recv[0])] + u_recv[1:], gu_full[1], n_src))

        order = a_recv[1]
        mine, far = [], []
        for b in range(n_blk):
            p_prev, p_next = down_call([after(a_recv[0], order), a_recv[1]], d_full[b], n_src, n_fs, b, n_blk)
            b_next = shift(p_prev, -1)
            b_prev = shift(p_next, 1)
            m = down_call([after(a_own[0], p_prev), a_own[1]], d_full[b], n_src, n_fs, b, n_blk, resid, (b_next, b_prev))
            order = m
            f_prev = shift(m, 1)
            f_next = shift(m, -1)
            far_0 = shift(f_prev[:sub], 1)
            far_1 = shift(f_next[sub:], -1)
            mine.append((m, f_prev, f_next))
            far.append((far_0, far_1))
        idx = jnp.stack([(me - s) % n_tp for s in range(n_tp)] + [me]).astype(jnp.int32)
        near_moves = [(i, c * sub, sub, c, who) for i, who in ((0, 0), (1, 1), (2, n_tp - 1)) for c in range(N_CALLS)]
        far_moves = [(0, 0, sub, 0, 2), (1, 0, sub, 1, 2)]
        hidden = None
        for b in range(n_blk):
            near = list(mine[b])
            if b == 0:
                near[0] = after(near[0], order)
            hidden = place_call(idx, near, near_moves, (seq, d), n_fs, b, n_blk, hidden)
            hidden = place_call(idx, far[b], far_moves, (seq, d), n_fs, b, n_blk, hidden)
        hidden = hidden.reshape(1, seq, d)
        return hidden, k.reshape(1, seq, n_kv, HEAD_DIM), v.reshape(1, seq, n_kv, HEAD_DIM)


    return jax.shard_map(local_layer, mesh=mesh2, in_specs=in_specs, out_specs=out_specs, check_vma=False)
```

```python
import functools
import math
import jax
import jax.numpy as jnp
from jax import lax
from jax.experimental import pallas as pl
from jax.experimental.pallas import tpu as pltpu
from jax.sharding import Mesh, PartitionSpec as P


HEAD_DIM = 128
ROPE_THETA = 500000.0
NORM_EPS = 1e-5
EXP2_SCALE = HEAD_DIM ** -0.5 * math.log2(math.e)
N_CALLS = 2
VMEM_LIMIT = 67043328


def rope_freqs():
    half_idx = jnp.arange(HEAD_DIM // 2, dtype=jnp.float32)
    inv_freq = jnp.power(ROPE_THETA, -2.0 * half_idx / HEAD_DIM)
    wave_len = 2.0 * math.pi / inv_freq
    smooth = (8192.0 / wave_len - 1.0) / 3.0
    blended = (1.0 - smooth) * inv_freq / 8.0 + smooth * inv_freq
    return jnp.where(wave_len < 2048.0, inv_freq, jnp.where(wave_len > 8192.0, inv_freq / 8.0, blended))


def params(**kw):
    return pltpu.CompilerParams(vmem_limit_bytes=VMEM_LIMIT, **kw)


def cost(flops, nbytes):
    return pl.CostEstimate(flops=flops, bytes_accessed=nbytes, transcendentals=0)


def norm_rows(vals_f32, gain):
    inv = lax.rsqrt(jnp.mean(vals_f32 * vals_f32, axis=-1, keepdims=True) + NORM_EPS)
    return (vals_f32 * inv * gain).astype(jnp.bfloat16)


def norm_kernel(x_ref, g_ref, h_ref):
    h_ref[...] = norm_rows(x_ref[...].astype(jnp.float32), g_ref[...].astype(jnp.float32))


def norm_call(x, gain):
    s, d = x.shape
    bm = min(256, s)
    return pl.pallas_call(
        norm_kernel,
        grid=(s // bm,),
        in_specs=[pl.BlockSpec((bm, d), lambda i: (i, 0)), pl.BlockSpec((1, d), lambda i: (0, 0))],
        out_specs=pl.BlockSpec((bm, d), lambda i: (i, 0)),
        out_shape=jax.ShapeDtypeStruct((s, d), jnp.bfloat16),
        compiler_params=params(),
        cost_estimate=cost(8 * s * d, 4 * s * d),
        name="norm",
    )(x, gain)


def qkv_kernel(n_q, n_kv, h_ref, w_ref, cos_ref, sin_ref, q_ref, k_ref, v_ref, vt_ref):
    h = h_ref[...]
    cos_t, sin_t = cos_ref[...], sin_ref[...]
    n_heads = n_q + 2 * n_kv
    for lo in range(0, n_heads, 2):
        y = jnp.dot(h, w_ref[:, lo * HEAD_DIM:(lo + 2) * HEAD_DIM], preferred_element_type=jnp.float32)
        for i in range(lo, lo + 2):
            a = y[:, (i - lo) * HEAD_DIM:(i - lo + 1) * HEAD_DIM]
            if i >= n_q + n_kv:
                cols = slice((i - n_q - n_kv) * HEAD_DIM, (i - n_q - n_kv + 1) * HEAD_DIM)
                v_ref[:, cols] = a.astype(jnp.bfloat16)
                vt_ref[cols, :] = a.T.astype(jnp.bfloat16)
                continue
            r = (a * cos_t + pltpu.roll(a, HEAD_DIM // 2, 1) * sin_t).astype(jnp.bfloat16)
            if i < n_q:
                q_ref[i] = r
            else:
                k_ref[:, (i - n_q) * HEAD_DIM:(i - n_q + 1) * HEAD_DIM] = r


def qkv_call(h, w, cos_t, sin_t, n_q, n_kv):
    s, d = h.shape
    bm = min(512, s)
    n = w.shape[1]
    row = lambda i: (i, 0)
    return pl.pallas_call(
        functools.partial(qkv_kernel, n_q, n_kv),
        grid=(s // bm,),
        in_specs=[pl.BlockSpec((bm, d), row), pl.BlockSpec((d, n), lambda i: (0, 0), pipeline_mode=pl.Buffered(1)),
                  pl.BlockSpec((bm, HEAD_DIM), row), pl.BlockSpec((bm, HEAD_DIM), row)],
        out_specs=[pl.BlockSpec((n_q, bm, HEAD_DIM), lambda i: (0, i, 0)),
                   pl.BlockSpec((bm, n_kv * HEAD_DIM), row), pl.BlockSpec((bm, n_kv * HEAD_DIM), row),
                   pl.BlockSpec((n_kv * HEAD_DIM, bm), lambda i: (0, i))],
        out_shape=[jax.ShapeDtypeStruct((n_q, s, HEAD_DIM), jnp.bfloat16),
                   jax.ShapeDtypeStruct((s, n_kv * HEAD_DIM), jnp.bfloat16),
                   jax.ShapeDtypeStruct((s, n_kv * HEAD_DIM), jnp.bfloat16),
                   jax.ShapeDtypeStruct((n_kv * HEAD_DIM, s), jnp.bfloat16)],
        compiler_params=params(),
        cost_estimate=cost(2 * s * d * n, 2 * s * d + 2 * d * n + 2 * s * n),
        name="qkv",
    )(h, w, cos_t, sin_t)


def att_kernel(bq, bk, per, first, len_ref, q_ref, k_ref, vt_ref, o_ref, s_ref, p_ref, m_ref, l_ref, alpha_ref, acc_ref):
    row0 = first + pl.program_id(1) * bq
    valid = len_ref[0]
    last = k_ref.shape[0] // bk - 1
    m_ref[...] = jnp.full_like(m_ref, -jnp.inf)
    l_ref[...] = jnp.zeros_like(l_ref)
    alpha_ref[...] = jnp.zeros_like(alpha_ref)
    acc_ref[...] = jnp.zeros_like(acc_ref)
    p_ref[...] = jnp.zeros_like(p_ref)

    def scores(j, h):
        k_blk = k_ref[pl.ds(pl.multiple_of(j * bk, bk), bk), :]
        s_ref[h] = lax.dot_general(k_blk, q_ref[h], (((1,), (1,)), ((), ())), preferred_element_type=jnp.float32)

    def values(j, h):
        vt_blk = vt_ref[:, pl.ds(pl.multiple_of(j * bk, bk), bk)]
        acc_ref[h] = acc_ref[h] * alpha_ref[h] + jnp.dot(vt_blk, p_ref[h], preferred_element_type=jnp.float32)

    tall = min(32, bk)

    def softmax(j, h, masked):
        m_old = m_ref[h]
        m8 = None
        for c in range(bk // tall):
            r = slice(c * tall, (c + 1) * tall)
            sc = s_ref[h, r, :]
            if masked:
                kid = j * bk + c * tall + lax.broadcasted_iota(jnp.int32, (tall, bq), 0)
                qid = row0 + lax.broadcasted_iota(jnp.int32, (tall, bq), 1)
                sc = jnp.where((kid <= qid) & (kid < valid), sc, -jnp.inf)
                s_ref[h, r, :] = sc
            top = jnp.max(sc.reshape(tall // 8, 8, bq), axis=0)
            m8 = top if m8 is None else jnp.maximum(m8, top)
        m_new = jnp.maximum(m_old, jnp.max(m8, axis=0, keepdims=True))
        m_rows = jnp.broadcast_to(m_new, (8, bq))[None]
        l8 = None
        for c in range(bk // tall):
            r = slice(c * tall, (c + 1) * tall)
            p = jnp.exp2((s_ref[h, r, :].reshape(tall // 8, 8, bq) - m_rows) * EXP2_SCALE)
            tot = jnp.sum(p, axis=0)
            l8 = tot if l8 is None else l8 + tot
            p_ref[h, r, :] = p.reshape(tall, bq).astype(jnp.bfloat16)
        alpha = jnp.exp2((m_old - m_new) * EXP2_SCALE)
        l_ref[h] = l_ref[h] * alpha + jnp.sum(l8, axis=0, keepdims=True)
        alpha_ref[h] = alpha
        m_ref[h] = m_new

    def step(j, masked):
        for h in range(per):
            values(jnp.maximum(j - 1, 0), h)
            softmax(j, h, masked)
            scores(jnp.minimum(j + 1, last), h)

    n_full = jnp.minimum((row0 + 1) // bk, valid // bk)
    n_end = jnp.minimum((row0 + bq + bk - 1) // bk, (valid + bk - 1) // bk)

    def full(j, _):
        step(j, False)
        return 0

    def part(j, _):
        step(j, True)
        return 0

    for h in range(per):
        scores(0, h)
    lax.fori_loop(0, n_full, full, 0)
    lax.fori_loop(n_full, n_end, part, 0)
    for h in range(per):
        values(n_end - 1, h)
        o_ref[:, h * HEAD_DIM:(h + 1) * HEAD_DIM] = (acc_ref[h] / l_ref[h]).T.astype(jnp.bfloat16)


def att_call(q, k, vt, valid_len, call):
    n_q, s, _ = q.shape
    n_kv = k.shape[1] // HEAD_DIM
    per = n_q // n_kv
    rows = s // N_CALLS
    bq = min(512, rows)
    bk = min(512, s)
    first = call * rows
    off = first // bq
    frac = (2 * call + 1) / N_CALLS ** 2
    return pl.pallas_call(
        functools.partial(att_kernel, bq, bk, per, first),
        grid=(n_kv, rows // bq),
        in_specs=[pl.BlockSpec(memory_space=pltpu.SMEM),
                  pl.BlockSpec((per, bq, HEAD_DIM), lambda g, i: (g, off + i, 0)),
                  pl.BlockSpec((s, HEAD_DIM), lambda g, i: (0, g)),
                  pl.BlockSpec((HEAD_DIM, s), lambda g, i: (g, 0))],
        out_specs=pl.BlockSpec((bq, per * HEAD_DIM), lambda g, i: (i, g)),
        out_shape=jax.ShapeDtypeStruct((rows, n_q * HEAD_DIM), jnp.bfloat16),
        scratch_shapes=[pltpu.VMEM((per, bk, bq), jnp.float32), pltpu.VMEM((per, bk, bq), jnp.bfloat16)]
        + [pltpu.VMEM((per, 1, bq), jnp.float32)] * 3 + [pltpu.VMEM((per, HEAD_DIM, bq), jnp.float32)],
        compiler_params=params(),
        cost_estimate=cost(int(8 * frac * n_q * s * s * HEAD_DIM), 4 * n_q * s * HEAD_DIM),
        name="attention",
    )(valid_len, q, k, vt)


def out_kernel(n_src, idx_ref, *refs):
    o_refs = refs[:n_src]
    w_ref, x_ref, g_ref, r_ref, ua_ref, ub_ref, o_all, y_ref = refs[n_src:]
    ko = o_refs[0].shape[1]
    n = pl.program_id(0)
    bn = w_ref.shape[1]
    half = ua_ref.shape[0]

    @pl.when(n == 0)
    def _():
        for s in range(n_src):
            o_all[:, s * ko:(s + 1) * ko] = o_refs[s][...]

    acc = jnp.dot(o_all[...], w_ref[...], preferred_element_type=jnp.float32)
    col = pl.ds(pl.multiple_of(n * bn, bn), bn)
    y_ref[:, col] = (x_ref[:, col].astype(jnp.float32) + acc).astype(jnp.bfloat16)

    @pl.when(n == pl.num_programs(0) - 1)
    def _():
        r_ref[...] = y_ref[...]
        u = norm_rows(y_ref[...].astype(jnp.float32), g_ref[...].astype(jnp.float32))
        ua_ref[...] = u[:half]
        ub_ref[...] = u[half:]


def out_call(idx, o_pieces, w, x, gain):
    n_src = len(o_pieces)
    rows, ko = o_pieces[0].shape
    d = x.shape[1]
    bn = min(512, d)
    fixed = lambda n, idx: (0, 0)
    half = jax.ShapeDtypeStruct((rows // 2, d), jnp.bfloat16)
    return pl.pallas_call(
        functools.partial(out_kernel, n_src),
        grid_spec=pltpu.PrefetchScalarGridSpec(
            num_scalar_prefetch=1,
            grid=(d // bn,),
            in_specs=[pl.BlockSpec((rows, ko), fixed)] * n_src + [
                pl.BlockSpec((n_src * ko, bn), lambda n, idx: (0, n)),
                pl.BlockSpec((rows, d), lambda n, idx: (idx[0], 0)),
                pl.BlockSpec((1, d), fixed)],
            out_specs=[pl.BlockSpec((rows, d), fixed), pl.BlockSpec((rows // 2, d), fixed), pl.BlockSpec((rows // 2, d), fixed)],
            scratch_shapes=[pltpu.VMEM((rows, n_src * ko), jnp.bfloat16), pltpu.VMEM((rows, d), jnp.bfloat16)]),
        out_shape=[jax.ShapeDtypeStruct((rows, d), jnp.bfloat16), half, half],
        compiler_params=params(),
        cost_estimate=cost(2 * rows * d * ko * n_src, 2 * w.size + 8 * rows * d),
        name="w_out",
    )(idx, *o_pieces, w, x, gain)


def gu_kernel(bm, n_u, *refs):
    u_refs = refs[:n_u]
    g_ref, up_ref, a_ref, u_all, sem = refs[n_u:]
    rows = u_all.shape[0]
    piece = rows // n_u
    first = (pl.program_id(0) == 0) & (pl.program_id(1) == 0)
    copies = [pltpu.make_async_copy(u_refs[i], u_all.at[i * piece:(i + 1) * piece, :], sem.at[i]) for i in range(n_u)]

    @pl.when(first)
    def _():
        for c in copies:
            c.start()

    @pl.loop(0, rows // bm)
    def _(m):
        r = pl.ds(pl.multiple_of(m * bm, bm), bm)
        for i in range(n_u):
            @pl.when(first & (m == i * piece // bm))
            def _():
                copies[i].wait()
        u = u_all[r, :]
        gate = jnp.dot(u, g_ref[...], preferred_element_type=jnp.float32)
        up = jnp.dot(u, up_ref[...], preferred_element_type=jnp.float32)
        a_ref[r, :] = (jax.nn.silu(gate) * up).astype(jnp.bfloat16)


def gu_call(us, w, n_src):
    n_u = len(us)
    rows, d = us[0].shape
    rows *= n_u
    half = w.shape[1] // (2 * n_src)
    bn = math.gcd(256, half)
    nb = half // bn
    bm = min(512, rows)
    return pl.pallas_call(
        functools.partial(gu_kernel, bm, n_u),
        grid=(n_src, nb),
        in_specs=[pl.BlockSpec(memory_space=pl.ANY)] * n_u + [
            pl.BlockSpec((d, bn), lambda j, n: (0, 2 * j * nb + n)),
            pl.BlockSpec((d, bn), lambda j, n: (0, (2 * j + 1) * nb + n))],
        out_specs=pl.BlockSpec((rows, bn), lambda j, n: (0, j * nb + n)),
        out_shape=jax.ShapeDtypeStruct((rows, n_src * half), jnp.bfloat16),
        scratch_shapes=[pltpu.VMEM((rows, d), jnp.bfloat16), pltpu.SemaphoreType.DMA((n_u,))],
        compiler_params=params(),
        cost_estimate=cost(4 * rows * d * n_src * half, 2 * w.size + 2 * rows * d + 2 * rows * n_src * half),
        name="gate_up",
    )(*us, w, w)


def down_kernel(bm, parts, own, n_f, blk, n_blk, *refs):
    a_refs = refs[:parts]
    w_ref = refs[parts]
    rest = refs[parts + 1:]
    acc_ref = rest[-1]
    j = pl.program_id(0)
    rows, cols = acc_ref.shape
    lanes = cols // n_f

    @pl.when(j == 0)
    def _():
        if own:
            quarter = rows // (2 * N_CALLS)
            for c in range(N_CALLS):
                for h in range(2):
                    r = slice((2 * c + h) * quarter, (2 * c + h + 1) * quarter)
                    for f in range(n_f):
                        src = slice((f * n_blk + blk) * lanes, (f * n_blk + blk + 1) * lanes)
                        dst = slice(f * lanes, (f + 1) * lanes)
                        part = rest[N_CALLS + h][c * quarter:(c + 1) * quarter, dst].astype(jnp.float32)
                        acc_ref[r, dst] = rest[c][h * quarter:(h + 1) * quarter, src].astype(jnp.float32) + part
        else:
            acc_ref[...] = jnp.zeros_like(acc_ref)

    @pl.loop(0, rows // bm)
    def _(m):
        r = pl.ds(pl.multiple_of(m * bm, bm), bm)
        acc = acc_ref[r, :]
        k0 = 0
        for p in range(parts):
            kp = a_refs[p].shape[1]
            acc = acc + jnp.dot(a_refs[p][r, :], w_ref[k0:k0 + kp, :], preferred_element_type=jnp.float32)
            k0 += kp
        acc_ref[r, :] = acc

    @pl.when(j == pl.num_programs(0) - 1)
    def _():
        if own:
            sub = rows // N_CALLS
            for c in range(N_CALLS):
                rest[N_CALLS + 2 + c][...] = acc_ref[c * sub:(c + 1) * sub, :].astype(jnp.bfloat16)
        else:
            for h in range(2):
                rest[h][...] = acc_ref[h * rows // 2:(h + 1) * rows // 2, :].astype(jnp.bfloat16)


def down_call(a_parts, w, n_src, n_f, blk, n_blk, resid=None, partials=()):
    cols = w.shape[1]
    parts = len(a_parts)
    rows = a_parts[0].shape[0]
    kj = w.shape[0] // n_src
    own = resid is not None
    bm = min(256, rows)
    fixed = lambda j: (0, 0)
    args = [*a_parts, w]
    in_specs = [pl.BlockSpec((rows, a.shape[1] // n_src), lambda j: (0, j)) for a in a_parts] + [pl.BlockSpec((kj, cols), lambda j: (j, 0))]
    if own:
        args += [*resid, *partials]
        in_specs += [pl.BlockSpec(r.shape, fixed, pipeline_mode=pl.Buffered(1)) for r in (*resid, *partials)]
    n_out = N_CALLS if own else 2
    out_specs = [pl.BlockSpec((rows // n_out, cols), fixed)] * n_out
    out_shape = [jax.ShapeDtypeStruct((rows // n_out, cols), jnp.bfloat16)] * n_out
    return pl.pallas_call(
        functools.partial(down_kernel, bm, parts, own, n_f, blk, n_blk),
        grid=(n_src,),
        in_specs=in_specs,
        out_specs=out_specs,
        out_shape=out_shape,
        scratch_shapes=[pltpu.VMEM((rows, cols), jnp.float32)],
        compiler_params=params(),
        cost_estimate=cost(2 * rows * cols * kj * n_src, 2 * w.size + 4 * rows * cols),
        name="down",
    )(*args)


def place_kernel(n_in, moves, n_f, blk, n_blk, idx_ref, *refs):
    ins = refs[:n_in]
    out_ref, sem = refs[-2:]
    copies = []
    for i, src_row, rows, call, who in moves:
        lanes = ins[i].shape[1] // n_f
        row = pl.multiple_of(idx_ref[who] * rows + call * rows * (idx_ref.shape[0] - 1), rows)
        for f in range(n_f):
            copies.append(pltpu.make_async_copy(
                ins[i].at[src_row:src_row + rows, f * lanes:(f + 1) * lanes],
                out_ref.at[pl.ds(row, rows), (f * n_blk + blk) * lanes:(f * n_blk + blk + 1) * lanes],
                sem.at[len(copies)]))
    for c in copies:
        c.start()
    for c in copies:
        c.wait()


def place_call(idx, pieces, moves, shape, n_f, blk, n_blk, out):
    n_in = len(pieces)
    args = list(pieces)
    in_specs = [pl.BlockSpec(p.shape, lambda *_: (0, 0)) for p in pieces]
    aliases = {}
    if out is not None:
        args.append(out)
        in_specs.append(pl.BlockSpec(memory_space=pl.ANY))
        aliases = {n_in + 1: 0}
    return pl.pallas_call(
        functools.partial(place_kernel, n_in, moves, n_f, blk, n_blk),
        grid_spec=pltpu.PrefetchScalarGridSpec(
            num_scalar_prefetch=1, grid=(1,), in_specs=in_specs, out_specs=pl.BlockSpec(memory_space=pl.ANY),
            scratch_shapes=[pltpu.SemaphoreType.DMA((len(moves) * n_f,))]),
        out_shape=jax.ShapeDtypeStruct(shape, jnp.bfloat16),
        input_output_aliases=aliases,
        compiler_params=params(),
        cost_estimate=cost(1000000, 4 * sum(p.size for p in pieces)),
        name="place",
    )(idx, *args)


def after(val, *deps):
    return lax.optimization_barrier((val, *deps))[0]


def solution(mesh):
    n_tp = mesh.shape['tp']
    n_fs = mesh.shape['fsdp']
    mesh2 = Mesh(mesh.devices.reshape(mesh.shape['dp'], n_tp // 2, 2, n_fs), ('dp', 'ta', 'tb', 'fsdp'))
    tp = ('ta', 'tb')
    batch_axes = ('dp', 'fsdp')
    in_specs = (P(batch_axes, None, None), P(batch_axes, None), P(batch_axes),
                P('fsdp', tp), P('fsdp', tp), P('fsdp', tp), P(tp, 'fsdp'),
                P('fsdp', tp), P('fsdp', tp), P(tp, 'fsdp'), P(None), P(None))
    out_specs = (P(batch_axes, None, None), P(batch_axes, None, tp, None), P(batch_axes, None, tp, None))

    def shift(val, s):
        return lax.ppermute(val, tp, [(i, (i + s) % n_tp) for i in range(n_tp)])

    def local_layer(tokens, positions, valid_len, w_query, w_key, w_value, w_out, w_gate, w_up, w_down, norm_attn, norm_mlp):
        _, seq, d = tokens.shape
        x = tokens.reshape(seq, d)
        n_q = w_query.shape[1] // HEAD_DIM
        n_kv = w_key.shape[1] // HEAD_DIM
        sub = seq // (n_tp * N_CALLS)
        me = lax.axis_index(tp)

        w_qkv = lax.all_gather(jnp.concatenate([w_query, w_key, w_value], axis=1), 'fsdp', axis=0, tiled=True)
        rounds = []
        for s in range(1, n_tp):
            rounds.append(shift(w_out, s))
        full_o = lax.all_gather(jnp.concatenate([w_out, *rounds], axis=0), 'fsdp', axis=1, tiled=True)
        fl = w_gate.shape[1]
        n_src = 2
        swaps = []
        lead = fl * 5 // 8
        for cut in (slice(0, lead), slice(lead, fl)):
            local = jnp.concatenate([w_gate[:, cut], w_up[:, cut]], axis=1)
            swaps.append((local, shift(local, 2)))
        swaps.append((w_down, shift(w_down, 2)))

        def joined(p, axis, *deps):
            return jnp.concatenate([after(swaps[p][0], *deps), swaps[p][1]], axis=axis)

        angles = positions.reshape(seq, 1).astype(jnp.float32) * rope_freqs()[None, :]
        cos_h, sin_h = jnp.cos(angles), jnp.sin(angles)
        cos_t = jnp.concatenate([cos_h, cos_h], axis=1)
        sin_t = jnp.concatenate([-sin_h, sin_h], axis=1)
        h = norm_call(x, norm_attn.reshape(1, d))
        q, k, v, vt = qkv_call(h, w_qkv, cos_t, sin_t, n_q, n_kv)

        pieces = []
        gu_parts = []
        o = q
        for call in range(N_CALLS):
            gu_parts.append(joined(call, 1, o))
            o = att_call(after(q, gu_parts[call], o), k, vt, valid_len, call)
            got = []
            for s in range(n_tp):
                blk = lax.dynamic_slice_in_dim(o, (me + s) % n_tp * sub, sub, axis=0)
                if s:
                    blk = shift(blk, s)
                got.append(blk)
            pieces.append(got)
        d_part = joined(2, 0, o)
        gu_full = [lax.all_gather(w, 'fsdp', axis=0, tiled=True) for w in gu_parts]
        n_blk = w_down.shape[1] // HEAD_DIM
        d_full = [lax.all_gather(d_part[:, b * HEAD_DIM:(b + 1) * HEAD_DIM], 'fsdp', axis=1, tiled=True) for b in range(n_blk)]

        resid, u_own, u_prev, u_next = [], [], [], []
        order = d_part
        for call in range(N_CALLS):
            got = pieces[call]
            got[0] = after(got[0], order)
            row = (call * n_tp + me).reshape(1).astype(jnp.int32)
            r, ua, ub = out_call(row, got, full_o, x, norm_mlp.reshape(1, d))
            order = r
            resid.append(r)
            u_own += [ua, ub]
            u_prev.append(shift(ua, 1))
            u_next.append(shift(ub, -1))
        u_recv = u_prev + u_next

        rows_of = {0: u_own, 1: u_recv}
        acts = {0: [], 1: []}
        order = resid[-1]
        for p, who in ((0, 0), (0, 1), (1, 0), (1, 1)):
            us = rows_of[who]
            acts[who].append(gu_call([after(us[0], order)] + us[1:], gu_full[p], n_src))
            order = acts[who][-1]
        a_own, a_recv = acts[0], acts[1]

        order = a_recv[1]
        mine = []
        for b in range(n_blk):
            p_prev, p_next = down_call([after(a_recv[0], order), a_recv[1]], d_full[b], n_src, n_fs, b, n_blk)
            b_next = shift(p_prev, -1)
            b_prev = shift(p_next, 1)
            m = down_call([after(a_own[0], p_prev), a_own[1]], d_full[b], n_src, n_fs, b, n_blk, resid, (b_next, b_prev))
            order = m[0]
            near = {}
            for c in range(N_CALLS):
                near[0, c] = shift(m[c], 1)
            for c in reversed(range(N_CALLS)):
                near[1, c] = shift(m[c], -1)
            mine.append((m, near))
        idx = jnp.stack([(me - s) % n_tp for s in range(n_tp)] + [me]).astype(jnp.int32)
        near_moves = [(i * N_CALLS + c, 0, sub, c, who) for i, who in enumerate((0, 1, n_tp - 1)) for c in range(N_CALLS)]
        far_moves = [(0, 0, sub, 0, 2), (1, 0, sub, N_CALLS - 1, 2)]
        hidden = None
        for b in range(n_blk):
            m, near = mine[b]
            src = (near[0, 0], near[1, N_CALLS - 1])
            if b == n_blk - 1:
                src = tuple(after(v, hidden) for v in src)
            far_0 = shift(src[0], 1)
            far_1 = shift(src[1], -1)
            pieces = [*m, *(near[g, c] for g in range(2) for c in range(N_CALLS))]
            if b == 0:
                pieces[0] = after(pieces[0], order)
            hidden = place_call(idx, pieces, near_moves, (seq, d), n_fs, b, n_blk, hidden)
            hidden = place_call(idx, (far_0, far_1), far_moves, (seq, d), n_fs, b, n_blk, hidden)
        hidden = hidden.reshape(1, seq, d)
        return hidden, k.reshape(1, seq, n_kv, HEAD_DIM), v.reshape(1, seq, n_kv, HEAD_DIM)


    return jax.shard_map(local_layer, mesh=mesh2, in_specs=in_specs, out_specs=out_specs, check_vma=False)
```

```python
import functools
import math
import jax
import jax.numpy as jnp
from jax import lax
from jax.experimental import pallas as pl
from jax.experimental.pallas import tpu as pltpu
from jax.sharding import Mesh, PartitionSpec as P


HEAD_DIM = 128
ROPE_THETA = 500000.0
NORM_EPS = 1e-5
EXP2_SCALE = HEAD_DIM ** -0.5 * math.log2(math.e)
N_CALLS = 2
VMEM_LIMIT = 67043328


def rope_freqs():
    half_idx = jnp.arange(HEAD_DIM // 2, dtype=jnp.float32)
    inv_freq = jnp.power(ROPE_THETA, -2.0 * half_idx / HEAD_DIM)
    wave_len = 2.0 * math.pi / inv_freq
    smooth = (8192.0 / wave_len - 1.0) / 3.0
    blended = (1.0 - smooth) * inv_freq / 8.0 + smooth * inv_freq
    return jnp.where(wave_len < 2048.0, inv_freq, jnp.where(wave_len > 8192.0, inv_freq / 8.0, blended))


def params(**kw):
    return pltpu.CompilerParams(vmem_limit_bytes=VMEM_LIMIT, **kw)


def cost(flops, nbytes):
    return pl.CostEstimate(flops=flops, bytes_accessed=nbytes, transcendentals=0)


def norm_rows(vals_f32, gain):
    inv = lax.rsqrt(jnp.mean(vals_f32 * vals_f32, axis=-1, keepdims=True) + NORM_EPS)
    return (vals_f32 * inv * gain).astype(jnp.bfloat16)


def norm_kernel(x_ref, g_ref, h_ref):
    h_ref[...] = norm_rows(x_ref[...].astype(jnp.float32), g_ref[...].astype(jnp.float32))


def norm_call(x, gain):
    s, d = x.shape
    bm = min(256, s)
    return pl.pallas_call(
        norm_kernel,
        grid=(s // bm,),
        in_specs=[pl.BlockSpec((bm, d), lambda i: (i, 0)), pl.BlockSpec((1, d), lambda i: (0, 0))],
        out_specs=pl.BlockSpec((bm, d), lambda i: (i, 0)),
        out_shape=jax.ShapeDtypeStruct((s, d), jnp.bfloat16),
        compiler_params=params(),
        cost_estimate=cost(8 * s * d, 4 * s * d),
        name="norm",
    )(x, gain)


def qkv_kernel(n_q, n_kv, h_ref, w_ref, cos_ref, sin_ref, q_ref, k_ref, v_ref, vt_ref):
    h = h_ref[...]
    cos_t, sin_t = cos_ref[...], sin_ref[...]
    n_heads = n_q + 2 * n_kv
    for lo in range(0, n_heads, 2):
        y = jnp.dot(h, w_ref[:, lo * HEAD_DIM:(lo + 2) * HEAD_DIM], preferred_element_type=jnp.float32)
        for i in range(lo, lo + 2):
            a = y[:, (i - lo) * HEAD_DIM:(i - lo + 1) * HEAD_DIM]
            if i >= n_q + n_kv:
                cols = slice((i - n_q - n_kv) * HEAD_DIM, (i - n_q - n_kv + 1) * HEAD_DIM)
                v_ref[:, cols] = a.astype(jnp.bfloat16)
                vt_ref[cols, :] = a.T.astype(jnp.bfloat16)
                continue
            r = (a * cos_t + pltpu.roll(a, HEAD_DIM // 2, 1) * sin_t).astype(jnp.bfloat16)
            if i < n_q:
                q_ref[i] = r
            else:
                k_ref[:, (i - n_q) * HEAD_DIM:(i - n_q + 1) * HEAD_DIM] = r


def qkv_call(h, w, cos_t, sin_t, n_q, n_kv):
    s, d = h.shape
    bm = min(512, s)
    n = w.shape[1]
    row = lambda i: (i, 0)
    return pl.pallas_call(
        functools.partial(qkv_kernel, n_q, n_kv),
        grid=(s // bm,),
        in_specs=[pl.BlockSpec((bm, d), row), pl.BlockSpec((d, n), lambda i: (0, 0), pipeline_mode=pl.Buffered(1)),
                  pl.BlockSpec((bm, HEAD_DIM), row), pl.BlockSpec((bm, HEAD_DIM), row)],
        out_specs=[pl.BlockSpec((n_q, bm, HEAD_DIM), lambda i: (0, i, 0)),
                   pl.BlockSpec((bm, n_kv * HEAD_DIM), row), pl.BlockSpec((bm, n_kv * HEAD_DIM), row),
                   pl.BlockSpec((n_kv * HEAD_DIM, bm), lambda i: (0, i))],
        out_shape=[jax.ShapeDtypeStruct((n_q, s, HEAD_DIM), jnp.bfloat16),
                   jax.ShapeDtypeStruct((s, n_kv * HEAD_DIM), jnp.bfloat16),
                   jax.ShapeDtypeStruct((s, n_kv * HEAD_DIM), jnp.bfloat16),
                   jax.ShapeDtypeStruct((n_kv * HEAD_DIM, s), jnp.bfloat16)],
        compiler_params=params(),
        cost_estimate=cost(2 * s * d * n, 2 * s * d + 2 * d * n + 2 * s * n),
        name="qkv",
    )(h, w, cos_t, sin_t)


def att_kernel(bq, bk, per, first, len_ref, q_ref, k_ref, vt_ref, o_ref, s_ref, p_ref, m_ref, l_ref, alpha_ref, acc_ref):
    row0 = first + pl.program_id(1) * bq
    valid = len_ref[0]
    last = k_ref.shape[0] // bk - 1
    m_ref[...] = jnp.full_like(m_ref, -jnp.inf)
    l_ref[...] = jnp.zeros_like(l_ref)
    alpha_ref[...] = jnp.zeros_like(alpha_ref)
    acc_ref[...] = jnp.zeros_like(acc_ref)
    p_ref[...] = jnp.zeros_like(p_ref)

    def scores(j, h):
        k_blk = k_ref[pl.ds(pl.multiple_of(j * bk, bk), bk), :]
        s_ref[h] = lax.dot_general(k_blk, q_ref[h], (((1,), (1,)), ((), ())), preferred_element_type=jnp.float32)

    def values(j, h):
        vt_blk = vt_ref[:, pl.ds(pl.multiple_of(j * bk, bk), bk)]
        acc_ref[h] = acc_ref[h] * alpha_ref[h] + jnp.dot(vt_blk, p_ref[h], preferred_element_type=jnp.float32)

    tall = min(32, bk)

    def softmax(j, h, masked):
        m_old = m_ref[h]
        m8 = None
        for c in range(bk // tall):
            r = slice(c * tall, (c + 1) * tall)
            sc = s_ref[h, r, :]
            if masked:
                kid = j * bk + c * tall + lax.broadcasted_iota(jnp.int32, (tall, bq), 0)
                qid = row0 + lax.broadcasted_iota(jnp.int32, (tall, bq), 1)
                sc = jnp.where((kid <= qid) & (kid < valid), sc, -jnp.inf)
                s_ref[h, r, :] = sc
            top = jnp.max(sc.reshape(tall // 8, 8, bq), axis=0)
            m8 = top if m8 is None else jnp.maximum(m8, top)
        m_new = jnp.maximum(m_old, jnp.max(m8, axis=0, keepdims=True))
        m_rows = jnp.broadcast_to(m_new, (8, bq))[None]
        l8 = None
        for c in range(bk // tall):
            r = slice(c * tall, (c + 1) * tall)
            p = jnp.exp2((s_ref[h, r, :].reshape(tall // 8, 8, bq) - m_rows) * EXP2_SCALE)
            tot = jnp.sum(p, axis=0)
            l8 = tot if l8 is None else l8 + tot
            p_ref[h, r, :] = p.reshape(tall, bq).astype(jnp.bfloat16)
        alpha = jnp.exp2((m_old - m_new) * EXP2_SCALE)
        l_ref[h] = l_ref[h] * alpha + jnp.sum(l8, axis=0, keepdims=True)
        alpha_ref[h] = alpha
        m_ref[h] = m_new

    def step(j, masked):
        for h in range(per):
            values(jnp.maximum(j - 1, 0), h)
            softmax(j, h, masked)
            scores(jnp.minimum(j + 1, last), h)

    n_full = jnp.minimum((row0 + 1) // bk, valid // bk)
    n_end = jnp.minimum((row0 + bq + bk - 1) // bk, (valid + bk - 1) // bk)

    def full(j, _):
        step(j, False)
        return 0

    def part(j, _):
        step(j, True)
        return 0

    for h in range(per):
        scores(0, h)
    lax.fori_loop(0, n_full, full, 0)
    lax.fori_loop(n_full, n_end, part, 0)
    for h in range(per):
        values(n_end - 1, h)
        o_ref[:, h * HEAD_DIM:(h + 1) * HEAD_DIM] = (acc_ref[h] / l_ref[h]).T.astype(jnp.bfloat16)


def att_call(q, k, vt, valid_len, call):
    n_q, s, _ = q.shape
    n_kv = k.shape[1] // HEAD_DIM
    per = n_q // n_kv
    rows = s // N_CALLS
    bq = min(512, rows)
    bk = min(512, s)
    first = call * rows
    off = first // bq
    frac = (2 * call + 1) / N_CALLS ** 2
    return pl.pallas_call(
        functools.partial(att_kernel, bq, bk, per, first),
        grid=(n_kv, rows // bq),
        in_specs=[pl.BlockSpec(memory_space=pltpu.SMEM),
                  pl.BlockSpec((per, bq, HEAD_DIM), lambda g, i: (g, off + i, 0)),
                  pl.BlockSpec((s, HEAD_DIM), lambda g, i: (0, g)),
                  pl.BlockSpec((HEAD_DIM, s), lambda g, i: (g, 0))],
        out_specs=pl.BlockSpec((bq, per * HEAD_DIM), lambda g, i: (i, g)),
        out_shape=jax.ShapeDtypeStruct((rows, n_q * HEAD_DIM), jnp.bfloat16),
        scratch_shapes=[pltpu.VMEM((per, bk, bq), jnp.float32), pltpu.VMEM((per, bk, bq), jnp.bfloat16)]
        + [pltpu.VMEM((per, 1, bq), jnp.float32)] * 3 + [pltpu.VMEM((per, HEAD_DIM, bq), jnp.float32)],
        compiler_params=params(),
        cost_estimate=cost(int(8 * frac * n_q * s * s * HEAD_DIM), 4 * n_q * s * HEAD_DIM),
        name="attention",
    )(valid_len, q, k, vt)


def out_kernel(n_src, idx_ref, *refs):
    o_refs = refs[:n_src]
    w_ref, x_ref, g_ref, r_ref, ua_ref, ub_ref, o_all, y_ref = refs[n_src:]
    ko = o_refs[0].shape[1]
    n = pl.program_id(0)
    bn = w_ref.shape[1]
    half = ua_ref.shape[0]

    @pl.when(n == 0)
    def _():
        for s in range(n_src):
            o_all[:, s * ko:(s + 1) * ko] = o_refs[s][...]

    acc = jnp.dot(o_all[...], w_ref[...], preferred_element_type=jnp.float32)
    col = pl.ds(pl.multiple_of(n * bn, bn), bn)
    y_ref[:, col] = (x_ref[:, col].astype(jnp.float32) + acc).astype(jnp.bfloat16)

    @pl.when(n == pl.num_programs(0) - 1)
    def _():
        r_ref[...] = y_ref[...]
        u = norm_rows(y_ref[...].astype(jnp.float32), g_ref[...].astype(jnp.float32))
        ua_ref[...] = u[:half]
        ub_ref[...] = u[half:]


def out_call(idx, o_pieces, w, x, gain):
    n_src = len(o_pieces)
    rows, ko = o_pieces[0].shape
    d = x.shape[1]
    bn = min(512, d)
    fixed = lambda n, idx: (0, 0)
    half = jax.ShapeDtypeStruct((rows // 2, d), jnp.bfloat16)
    return pl.pallas_call(
        functools.partial(out_kernel, n_src),
        grid_spec=pltpu.PrefetchScalarGridSpec(
            num_scalar_prefetch=1,
            grid=(d // bn,),
            in_specs=[pl.BlockSpec((rows, ko), fixed)] * n_src + [
                pl.BlockSpec((n_src * ko, bn), lambda n, idx: (0, n)),
                pl.BlockSpec((rows, d), lambda n, idx: (idx[0], 0)),
                pl.BlockSpec((1, d), fixed)],
            out_specs=[pl.BlockSpec((rows, d), fixed), pl.BlockSpec((rows // 2, d), fixed), pl.BlockSpec((rows // 2, d), fixed)],
            scratch_shapes=[pltpu.VMEM((rows, n_src * ko), jnp.bfloat16), pltpu.VMEM((rows, d), jnp.bfloat16)]),
        out_shape=[jax.ShapeDtypeStruct((rows, d), jnp.bfloat16), half, half],
        compiler_params=params(),
        cost_estimate=cost(2 * rows * d * ko * n_src, 2 * w.size + 8 * rows * d),
        name="w_out",
    )(idx, *o_pieces, w, x, gain)


def gu_kernel(bm, n_u, *refs):
    u_refs = refs[:n_u]
    g_ref, up_ref, a_ref, u_all, sem = refs[n_u:]
    rows = u_all.shape[0]
    piece = rows // n_u
    first = (pl.program_id(0) == 0) & (pl.program_id(1) == 0)
    copies = [pltpu.make_async_copy(u_refs[i], u_all.at[i * piece:(i + 1) * piece, :], sem.at[i]) for i in range(n_u)]

    @pl.when(first)
    def _():
        for c in copies:
            c.start()

    @pl.loop(0, rows // bm)
    def _(m):
        r = pl.ds(pl.multiple_of(m * bm, bm), bm)
        for i in range(n_u):
            @pl.when(first & (m == i * piece // bm))
            def _():
                copies[i].wait()
        u = u_all[r, :]
        gate = jnp.dot(u, g_ref[...], preferred_element_type=jnp.float32)
        up = jnp.dot(u, up_ref[...], preferred_element_type=jnp.float32)
        a_ref[r, :] = (jax.nn.silu(gate) * up).astype(jnp.bfloat16)


def gu_call(us, w, n_src):
    n_u = len(us)
    rows, d = us[0].shape
    rows *= n_u
    half = w.shape[1] // (2 * n_src)
    bn = math.gcd(256, half)
    nb = half // bn
    bm = min(512, rows)
    return pl.pallas_call(
        functools.partial(gu_kernel, bm, n_u),
        grid=(n_src, nb),
        in_specs=[pl.BlockSpec(memory_space=pl.ANY)] * n_u + [
            pl.BlockSpec((d, bn), lambda j, n: (0, 2 * j * nb + n)),
            pl.BlockSpec((d, bn), lambda j, n: (0, (2 * j + 1) * nb + n))],
        out_specs=pl.BlockSpec((rows, bn), lambda j, n: (0, j * nb + n)),
        out_shape=jax.ShapeDtypeStruct((rows, n_src * half), jnp.bfloat16),
        scratch_shapes=[pltpu.VMEM((rows, d), jnp.bfloat16), pltpu.SemaphoreType.DMA((n_u,))],
        compiler_params=params(),
        cost_estimate=cost(4 * rows * d * n_src * half, 2 * w.size + 2 * rows * d + 2 * rows * n_src * half),
        name="gate_up",
    )(*us, w, w)


def down_kernel(bm, parts, n_src, own, meta_ref, *refs):
    a_refs = refs[:parts]
    w_ref = refs[parts]
    rest = refs[parts + 1:]
    rows = a_refs[0].shape[0]
    n = pl.program_id(0)
    steps = pl.num_programs(0)
    bn = w_ref.shape[1]
    kj = w_ref.shape[0] // n_src

    @pl.loop(0, rows // bm)
    def _(m):
        r = pl.ds(pl.multiple_of(m * bm, bm), bm)
        acc = None
        for j in range(n_src):
            k0 = j * kj
            for p in range(parts):
                kp = a_refs[p].shape[1] // n_src
                part = jnp.dot(a_refs[p][r, j * kp:(j + 1) * kp], w_ref[k0:k0 + kp, :], preferred_element_type=jnp.float32)
                acc = part if acc is None else acc + part
                k0 += kp
        out = pl.ds(pl.multiple_of(m // 2 * bm, bm), bm)
        for h in range(2):
            @pl.when(m % 2 == h)
            def _():
                if own:
                    for i in range(bn // HEAD_DIM):
                        lanes = slice(i * HEAD_DIM, (i + 1) * HEAD_DIM)
                        col = pl.ds(pl.multiple_of(meta_ref[steps + n * (bn // HEAD_DIM) + i] * HEAD_DIM, HEAD_DIM), HEAD_DIM)
                        part = acc[:, lanes] + rest[1 + h][out, lanes].astype(jnp.float32)
                        rest[3][r, lanes] = (rest[0][r, col].astype(jnp.float32) + part).astype(jnp.bfloat16)
                else:
                    rest[h][out, :] = acc.astype(jnp.bfloat16)


def down_call(a_parts, w, meta, n_src, bn, steps, resid=None, partials=()):
    parts = len(a_parts)
    rows = a_parts[0].shape[0]
    cols = steps * bn
    own = resid is not None
    fixed = lambda n, meta: (0, 0)
    step = lambda n, meta: (0, n)
    once = dict(pipeline_mode=pl.Buffered(1))
    args = [*a_parts, w]
    in_specs = [pl.BlockSpec(a.shape, fixed, **once) for a in a_parts] + [pl.BlockSpec((w.shape[0], bn), lambda n, meta: (0, meta[n]))]
    if own:
        args += [resid, *partials]
        in_specs += [pl.BlockSpec(resid.shape, fixed, **once)] + [pl.BlockSpec((rows // 2, bn), step)] * 2
    n_out = 1 if own else 2
    return pl.pallas_call(
        functools.partial(down_kernel, rows // (2 * N_CALLS), parts, n_src, own),
        grid_spec=pltpu.PrefetchScalarGridSpec(
            num_scalar_prefetch=1, grid=(steps,), in_specs=in_specs, out_specs=[pl.BlockSpec((rows // n_out, bn), step)] * n_out),
        out_shape=[jax.ShapeDtypeStruct((rows // n_out, cols), jnp.bfloat16)] * n_out,
        compiler_params=params(),
        cost_estimate=cost(2 * rows * cols * w.shape[0], 2 * w.size + 4 * rows * cols),
        name="down",
    )(meta, *args)


def place_kernel(n_in, moves, n_tp, skip, idx_ref, *refs):
    ins = refs[:n_in]
    out_ref, sem = refs[-2:]
    copies = []
    for i, src_row, rows, call, who in moves:
        row = pl.multiple_of((call * n_tp + idx_ref[who]) * rows, rows)
        for q in range(ins[i].shape[1] // HEAD_DIM):
            col = pl.multiple_of(idx_ref[n_tp + skip + q] * HEAD_DIM, HEAD_DIM)
            copies.append(pltpu.make_async_copy(
                ins[i].at[src_row:src_row + rows, q * HEAD_DIM:(q + 1) * HEAD_DIM],
                out_ref.at[pl.ds(row, rows), pl.ds(col, HEAD_DIM)],
                sem.at[len(copies)]))
    for c in copies:
        c.start()
    for c in copies:
        c.wait()


def place_call(idx, pieces, moves, shape, n_tp, skip, out):
    n_in = len(pieces)
    args = list(pieces)
    in_specs = [pl.BlockSpec(p.shape, lambda *_: (0, 0)) for p in pieces]
    aliases = {}
    if out is not None:
        args.append(out)
        in_specs.append(pl.BlockSpec(memory_space=pl.ANY))
        aliases = {n_in + 1: 0}
    n_copies = sum(pieces[m[0]].shape[1] // HEAD_DIM for m in moves)
    return pl.pallas_call(
        functools.partial(place_kernel, n_in, moves, n_tp, skip),
        grid_spec=pltpu.PrefetchScalarGridSpec(
            num_scalar_prefetch=1, grid=(1,), in_specs=in_specs, out_specs=pl.BlockSpec(memory_space=pl.ANY),
            scratch_shapes=[pltpu.SemaphoreType.DMA((n_copies,))]),
        out_shape=jax.ShapeDtypeStruct(shape, jnp.bfloat16),
        input_output_aliases=aliases,
        compiler_params=params(),
        cost_estimate=cost(1000000, 4 * sum(p.size for p in pieces)),
        name="place",
    )(idx, *args)


def after(val, *deps):
    return lax.optimization_barrier((val, *deps))[0]


def solution(mesh):
    n_tp = mesh.shape['tp']
    n_fs = mesh.shape['fsdp']
    mesh2 = Mesh(mesh.devices.reshape(mesh.shape['dp'], n_tp // 2, 2, n_fs), ('dp', 'ta', 'tb', 'fsdp'))
    tp = ('ta', 'tb')
    batch_axes = ('dp', 'fsdp')
    in_specs = (P(batch_axes, None, None), P(batch_axes, None), P(batch_axes),
                P('fsdp', tp), P('fsdp', tp), P('fsdp', tp), P(tp, 'fsdp'),
                P('fsdp', tp), P('fsdp', tp), P(tp, 'fsdp'), P(None), P(None))
    out_specs = (P(batch_axes, None, None), P(batch_axes, None, tp, None), P(batch_axes, None, tp, None))

    def shift(val, s):
        return lax.ppermute(val, tp, [(i, (i + s) % n_tp) for i in range(n_tp)])

    def local_layer(tokens, positions, valid_len, w_query, w_key, w_value, w_out, w_gate, w_up, w_down, norm_attn, norm_mlp):
        _, seq, d = tokens.shape
        x = tokens.reshape(seq, d)
        n_q = w_query.shape[1] // HEAD_DIM
        n_kv = w_key.shape[1] // HEAD_DIM
        sub = seq // (n_tp * N_CALLS)
        me = lax.axis_index(tp)

        w_qkv = lax.all_gather(jnp.concatenate([w_query, w_key, w_value], axis=1), 'fsdp', axis=0, tiled=True)
        rounds = []
        for s in range(1, n_tp):
            rounds.append(shift(w_out, s))
        full_o = lax.all_gather(jnp.concatenate([w_out, *rounds], axis=0), 'fsdp', axis=1, tiled=True)
        fl = w_gate.shape[1]
        n_src = 2
        swaps = []
        lead = fl * 5 // 8
        for cut in (slice(0, lead), slice(lead, fl)):
            local = jnp.concatenate([w_gate[:, cut], w_up[:, cut]], axis=1)
            swaps.append((local, shift(local, 2)))
        swaps.append((w_down, shift(w_down, 2)))

        def joined(p, axis, *deps):
            return jnp.concatenate([after(swaps[p][0], *deps), swaps[p][1]], axis=axis)

        angles = positions.reshape(seq, 1).astype(jnp.float32) * rope_freqs()[None, :]
        cos_h, sin_h = jnp.cos(angles), jnp.sin(angles)
        cos_t = jnp.concatenate([cos_h, cos_h], axis=1)
        sin_t = jnp.concatenate([-sin_h, sin_h], axis=1)
        h = norm_call(x, norm_attn.reshape(1, d))
        q, k, v, vt = qkv_call(h, w_qkv, cos_t, sin_t, n_q, n_kv)

        pieces = []
        gu_parts = []
        o = q
        for call in range(N_CALLS):
            gu_parts.append(joined(call, 1, o))
            o = att_call(after(q, gu_parts[call], o), k, vt, valid_len, call)
            got = []
            for s in range(n_tp):
                blk = lax.dynamic_slice_in_dim(o, (me + s) % n_tp * sub, sub, axis=0)
                if s:
                    blk = shift(blk, s)
                got.append(blk)
            pieces.append(got)
        d_part = joined(2, 0, o)
        gu_full = [lax.all_gather(w, 'fsdp', axis=0, tiled=True) for w in gu_parts]
        n_blk = w_down.shape[1] // HEAD_DIM
        d_pair = lax.ppermute(d_part, 'fsdp', [(i, i ^ 1) for i in range(n_fs)])
        d_near = jnp.concatenate([d_part, d_pair], axis=1)
        d_full = [lax.all_gather(d_part[:, b * HEAD_DIM:(b + 1) * HEAD_DIM], 'fsdp', axis=1, tiled=True) for b in range(n_blk)]

        resid, u_own, u_prev, u_next = [], [], [], []
        order = d_part
        for call in range(N_CALLS):
            got = pieces[call]
            got[0] = after(got[0], order)
            row = (call * n_tp + me).reshape(1).astype(jnp.int32)
            r, ua, ub = out_call(row, got, full_o, x, norm_mlp.reshape(1, d))
            order = r
            resid.append(r)
            u_own += [ua, ub]
            u_prev.append(shift(ua, 1))
            u_next.append(shift(ub, -1))
        u_recv = [u_prev[0], u_next[0], u_prev[1], u_next[1]]
        resid = jnp.concatenate(resid, axis=0)

        def gate_up(p, who, dep):
            us = (u_own, u_recv)[who]
            return gu_call([after(us[0], dep)] + us[1:], gu_full[p], n_src)

        a_own = [gate_up(0, 0, resid)]
        a_recv = [gate_up(0, 1, a_own[0])]
        a_recv.append(gate_up(1, 1, a_recv[0]))

        fs = lax.axis_index('fsdp')
        chip, n_chip = fs // 2, n_fs // 2
        others = [(chip + 1 + i) % n_chip for i in range(n_chip - 1)]
        bn = 2 * HEAD_DIM
        blocks = [(d_near, list(range(n_blk)), [fs * n_blk + i for i in range(n_blk)] + [(fs ^ 1) * n_blk + i for i in range(n_blk)])]
        for b in range(n_blk):
            units = sum(([2 * o_ * n_blk + b, (2 * o_ + 1) * n_blk + b] for o_ in others), [])
            blocks.append((d_full[b], others, units))
        order = a_recv[1]
        mine = []
        for b, (w, sel, units) in enumerate(blocks):
            meta = jnp.stack([jnp.asarray(v, jnp.int32) for v in [*sel, *units]])
            p_prev, p_next = down_call([after(a_recv[0], order), a_recv[1]], w, meta, n_src, bn, len(sel))
            b_next = shift(p_prev, -1)
            b_prev = shift(p_next, 1)
            if b == 0:
                a_own.append(gate_up(1, 0, p_prev))
            m, = down_call([after(a_own[0], p_prev), a_own[1]], w, meta, n_src, bn, len(sel), resid, (b_next, b_prev))
            order = m
            near = {}
            for g, by in enumerate((1, -1)):
                near[g] = shift(m, by)
            mine.append((m, near))
        idx = jnp.stack([jnp.asarray(v, jnp.int32) for v in [(me - s) % n_tp for s in range(n_tp)] + sum((u for _, _, u in blocks), [])])
        near_moves = [(i, c * sub, sub, c, who) for i, who in enumerate((0, 1, n_tp - 1)) for c in range(N_CALLS)]
        far_moves = [(0, 0, sub, 0, 2), (1, 0, sub, N_CALLS - 1, 2)]
        hidden = None
        skip = 0
        last = len(blocks) - 1
        for b in range(len(blocks)):
            m, near = mine[b]
            src = (near[0], near[1]) if b < last else (after(near[0], hidden), after(near[1], hidden))
            far_0 = shift(src[0][:sub], 1)
            far_1 = shift(src[1][sub:], -1)
            pieces = [after(m, order) if b == 0 else m, near[0], near[1]]
            hidden = place_call(idx, pieces, near_moves, (seq, d), n_tp, skip, hidden)
            hidden = place_call(idx, (far_0, far_1), far_moves, (seq, d), n_tp, skip, hidden)
            skip += len(blocks[b][2])
        hidden = hidden.reshape(1, seq, d)
        return hidden, k.reshape(1, seq, n_kv, HEAD_DIM), v.reshape(1, seq, n_kv, HEAD_DIM)


    return jax.shard_map(local_layer, mesh=mesh2, in_specs=in_specs, out_specs=out_specs, check_vma=False)
```

```python
import functools
import math
import jax
import jax.numpy as jnp
from jax import lax
from jax.experimental import pallas as pl
from jax.experimental.pallas import tpu as pltpu
from jax.sharding import Mesh, PartitionSpec as P


HEAD_DIM = 128
ROPE_THETA = 500000.0
NORM_EPS = 1e-5
EXP2_SCALE = HEAD_DIM ** -0.5 * math.log2(math.e)
N_CALLS = 2
VMEM_LIMIT = 67043328


def rope_freqs():
    half_idx = jnp.arange(HEAD_DIM // 2, dtype=jnp.float32)
    inv_freq = jnp.power(ROPE_THETA, -2.0 * half_idx / HEAD_DIM)
    wave_len = 2.0 * math.pi / inv_freq
    smooth = (8192.0 / wave_len - 1.0) / 3.0
    blended = (1.0 - smooth) * inv_freq / 8.0 + smooth * inv_freq
    return jnp.where(wave_len < 2048.0, inv_freq, jnp.where(wave_len > 8192.0, inv_freq / 8.0, blended))


def params(**kw):
    return pltpu.CompilerParams(vmem_limit_bytes=VMEM_LIMIT, **kw)


def cost(flops, nbytes):
    return pl.CostEstimate(flops=flops, bytes_accessed=nbytes, transcendentals=0)


def norm_rows(vals_f32, gain):
    inv = lax.rsqrt(jnp.mean(vals_f32 * vals_f32, axis=-1, keepdims=True) + NORM_EPS)
    return (vals_f32 * inv * gain).astype(jnp.bfloat16)


def norm_kernel(x_ref, g_ref, h_ref):
    h_ref[...] = norm_rows(x_ref[...].astype(jnp.float32), g_ref[...].astype(jnp.float32))


def norm_call(x, gain):
    s, d = x.shape
    bm = min(512, s)
    return pl.pallas_call(
        norm_kernel,
        grid=(s // bm,),
        in_specs=[pl.BlockSpec((bm, d), lambda i: (i, 0)), pl.BlockSpec((1, d), lambda i: (0, 0))],
        out_specs=pl.BlockSpec((bm, d), lambda i: (i, 0)),
        out_shape=jax.ShapeDtypeStruct((s, d), jnp.bfloat16),
        compiler_params=params(),
        cost_estimate=cost(8 * s * d, 4 * s * d),
        name="norm",
    )(x, gain)


def qkv_kernel(n_q, n_kv, h_ref, w_ref, cos_ref, sin_ref, q_ref, k_ref, v_ref, vt_ref):
    h = h_ref[...]
    cos_t, sin_t = cos_ref[...], sin_ref[...]
    n_heads = n_q + 2 * n_kv
    for lo in range(0, n_heads, 2):
        y = jnp.dot(h, w_ref[:, lo * HEAD_DIM:(lo + 2) * HEAD_DIM], preferred_element_type=jnp.float32)
        for i in range(lo, lo + 2):
            a = y[:, (i - lo) * HEAD_DIM:(i - lo + 1) * HEAD_DIM]
            if i >= n_q + n_kv:
                cols = slice((i - n_q - n_kv) * HEAD_DIM, (i - n_q - n_kv + 1) * HEAD_DIM)
                v_ref[:, cols] = a.astype(jnp.bfloat16)
                vt_ref[cols, :] = a.T.astype(jnp.bfloat16)
                continue
            r = (a * cos_t + pltpu.roll(a, HEAD_DIM // 2, 1) * sin_t).astype(jnp.bfloat16)
            if i < n_q:
                q_ref[i] = r
            else:
                k_ref[:, (i - n_q) * HEAD_DIM:(i - n_q + 1) * HEAD_DIM] = r


def qkv_call(h, w, cos_t, sin_t, n_q, n_kv):
    s, d = h.shape
    bm = min(512, s)
    n = w.shape[1]
    row = lambda i: (i, 0)
    return pl.pallas_call(
        functools.partial(qkv_kernel, n_q, n_kv),
        grid=(s // bm,),
        in_specs=[pl.BlockSpec((bm, d), row), pl.BlockSpec((d, n), lambda i: (0, 0), pipeline_mode=pl.Buffered(1)),
                  pl.BlockSpec((bm, HEAD_DIM), row), pl.BlockSpec((bm, HEAD_DIM), row)],
        out_specs=[pl.BlockSpec((n_q, bm, HEAD_DIM), lambda i: (0, i, 0)),
                   pl.BlockSpec((bm, n_kv * HEAD_DIM), row), pl.BlockSpec((bm, n_kv * HEAD_DIM), row),
                   pl.BlockSpec((n_kv * HEAD_DIM, bm), lambda i: (0, i))],
        out_shape=[jax.ShapeDtypeStruct((n_q, s, HEAD_DIM), jnp.bfloat16),
                   jax.ShapeDtypeStruct((s, n_kv * HEAD_DIM), jnp.bfloat16),
                   jax.ShapeDtypeStruct((s, n_kv * HEAD_DIM), jnp.bfloat16),
                   jax.ShapeDtypeStruct((n_kv * HEAD_DIM, s), jnp.bfloat16)],
        compiler_params=params(),
        cost_estimate=cost(2 * s * d * n, 2 * s * d + 2 * d * n + 2 * s * n),
        name="qkv",
    )(h, w, cos_t, sin_t)


def att_kernel(bq, bk, per, first, len_ref, q_ref, k_ref, vt_ref, o_ref, s_ref, p_ref, m_ref, l_ref, alpha_ref, acc_ref):
    row0 = first + pl.program_id(1) * bq
    valid = len_ref[0]
    last = k_ref.shape[0] // bk - 1
    m_ref[...] = jnp.full_like(m_ref, -jnp.inf)
    l_ref[...] = jnp.zeros_like(l_ref)
    alpha_ref[...] = jnp.zeros_like(alpha_ref)
    acc_ref[...] = jnp.zeros_like(acc_ref)
    p_ref[...] = jnp.zeros_like(p_ref)

    def scores(j, h):
        k_blk = k_ref[pl.ds(pl.multiple_of(j * bk, bk), bk), :]
        s_ref[h] = lax.dot_general(k_blk, q_ref[h], (((1,), (1,)), ((), ())), preferred_element_type=jnp.float32)

    def values(j, h):
        vt_blk = vt_ref[:, pl.ds(pl.multiple_of(j * bk, bk), bk)]
        acc_ref[h] = acc_ref[h] * alpha_ref[h] + jnp.dot(vt_blk, p_ref[h], preferred_element_type=jnp.float32)

    tall = min(32, bk)

    def softmax(j, h, masked):
        m_old = m_ref[h]
        m8 = None
        for c in range(bk // tall):
            r = slice(c * tall, (c + 1) * tall)
            sc = s_ref[h, r, :]
            if masked:
                kid = j * bk + c * tall + lax.broadcasted_iota(jnp.int32, (tall, bq), 0)
                qid = row0 + lax.broadcasted_iota(jnp.int32, (tall, bq), 1)
                sc = jnp.where((kid <= qid) & (kid < valid), sc, -jnp.inf)
                s_ref[h, r, :] = sc
            top = jnp.max(sc.reshape(tall // 8, 8, bq), axis=0)
            m8 = top if m8 is None else jnp.maximum(m8, top)
        m_new = jnp.maximum(m_old, jnp.max(m8, axis=0, keepdims=True))
        m_rows = jnp.broadcast_to(m_new, (8, bq))[None]
        l8 = None
        for c in range(bk // tall):
            r = slice(c * tall, (c + 1) * tall)
            p = jnp.exp2((s_ref[h, r, :].reshape(tall // 8, 8, bq) - m_rows) * EXP2_SCALE)
            tot = jnp.sum(p, axis=0)
            l8 = tot if l8 is None else l8 + tot
            p_ref[h, r, :] = p.reshape(tall, bq).astype(jnp.bfloat16)
        alpha = jnp.exp2((m_old - m_new) * EXP2_SCALE)
        l_ref[h] = l_ref[h] * alpha + jnp.sum(l8, axis=0, keepdims=True)
        alpha_ref[h] = alpha
        m_ref[h] = m_new

    def step(j, masked):
        for h in range(per):
            values(jnp.maximum(j - 1, 0), h)
            softmax(j, h, masked)
            scores(jnp.minimum(j + 1, last), h)

    n_full = jnp.minimum((row0 + 1) // bk, valid // bk)
    n_end = jnp.minimum((row0 + bq + bk - 1) // bk, (valid + bk - 1) // bk)

    def full(j, _):
        step(j, False)
        return 0

    def part(j, _):
        step(j, True)
        return 0

    for h in range(per):
        scores(0, h)
    lax.fori_loop(0, n_full, full, 0)
    lax.fori_loop(n_full, n_end, part, 0)
    for h in range(per):
        values(n_end - 1, h)
        o_ref[:, h * HEAD_DIM:(h + 1) * HEAD_DIM] = (acc_ref[h] / l_ref[h]).T.astype(jnp.bfloat16)


def att_call(q, k, vt, valid_len, call):
    n_q, s, _ = q.shape
    n_kv = k.shape[1] // HEAD_DIM
    per = n_q // n_kv
    rows = s // N_CALLS
    bq = min(512, rows)
    bk = min(512, s)
    first = call * rows
    off = first // bq
    frac = (2 * call + 1) / N_CALLS ** 2
    return pl.pallas_call(
        functools.partial(att_kernel, bq, bk, per, first),
        grid=(n_kv, rows // bq),
        in_specs=[pl.BlockSpec(memory_space=pltpu.SMEM),
                  pl.BlockSpec((per, bq, HEAD_DIM), lambda g, i: (g, off + i, 0)),
                  pl.BlockSpec((s, HEAD_DIM), lambda g, i: (0, g)),
                  pl.BlockSpec((HEAD_DIM, s), lambda g, i: (g, 0))],
        out_specs=pl.BlockSpec((bq, per * HEAD_DIM), lambda g, i: (i, g)),
        out_shape=jax.ShapeDtypeStruct((rows, n_q * HEAD_DIM), jnp.bfloat16),
        scratch_shapes=[pltpu.VMEM((per, bk, bq), jnp.float32), pltpu.VMEM((per, bk, bq), jnp.bfloat16)]
        + [pltpu.VMEM((per, 1, bq), jnp.float32)] * 3 + [pltpu.VMEM((per, HEAD_DIM, bq), jnp.float32)],
        compiler_params=params(),
        cost_estimate=cost(int(8 * frac * n_q * s * s * HEAD_DIM), 4 * n_q * s * HEAD_DIM),
        name="attention",
    )(valid_len, q, k, vt)


def out_kernel(n_src, idx_ref, *refs):
    o_refs = refs[:n_src]
    w_ref, x_ref, g_ref, r_ref, ua_ref, ub_ref, o_all, y_ref = refs[n_src:]
    ko = o_refs[0].shape[1]
    n = pl.program_id(0)
    bn = w_ref.shape[1]
    half = ua_ref.shape[0]

    @pl.when(n == 0)
    def _():
        for s in range(n_src):
            o_all[:, s * ko:(s + 1) * ko] = o_refs[s][...]

    acc = jnp.dot(o_all[...], w_ref[...], preferred_element_type=jnp.float32)
    col = pl.ds(pl.multiple_of(n * bn, bn), bn)
    y_ref[:, col] = (x_ref[:, col].astype(jnp.float32) + acc).astype(jnp.bfloat16)

    @pl.when(n == pl.num_programs(0) - 1)
    def _():
        r_ref[...] = y_ref[...]
        u = norm_rows(y_ref[...].astype(jnp.float32), g_ref[...].astype(jnp.float32))
        ua_ref[...] = u[:half]
        ub_ref[...] = u[half:]


def out_call(idx, o_pieces, w, x, gain):
    n_src = len(o_pieces)
    rows, ko = o_pieces[0].shape
    d = x.shape[1]
    bn = min(512, d)
    fixed = lambda n, idx: (0, 0)
    half = jax.ShapeDtypeStruct((rows // 2, d), jnp.bfloat16)
    return pl.pallas_call(
        functools.partial(out_kernel, n_src),
        grid_spec=pltpu.PrefetchScalarGridSpec(
            num_scalar_prefetch=1,
            grid=(d // bn,),
            in_specs=[pl.BlockSpec((rows, ko), fixed)] * n_src + [
                pl.BlockSpec((n_src * ko, bn), lambda n, idx: (0, n)),
                pl.BlockSpec((rows, d), lambda n, idx: (idx[0], 0)),
                pl.BlockSpec((1, d), fixed)],
            out_specs=[pl.BlockSpec((rows, d), fixed), pl.BlockSpec((rows // 2, d), fixed), pl.BlockSpec((rows // 2, d), fixed)],
            scratch_shapes=[pltpu.VMEM((rows, n_src * ko), jnp.bfloat16), pltpu.VMEM((rows, d), jnp.bfloat16)]),
        out_shape=[jax.ShapeDtypeStruct((rows, d), jnp.bfloat16), half, half],
        compiler_params=params(),
        cost_estimate=cost(2 * rows * d * ko * n_src, 2 * w.size + 8 * rows * d),
        name="w_out",
    )(idx, *o_pieces, w, x, gain)


def gu_kernel(bm, n_u, *refs):
    u_refs = refs[:n_u]
    g_ref, up_ref, a_ref, u_all, sem = refs[n_u:]
    rows = u_all.shape[0]
    piece = rows // n_u
    first = (pl.program_id(0) == 0) & (pl.program_id(1) == 0)
    copies = [pltpu.make_async_copy(u_refs[i], u_all.at[i * piece:(i + 1) * piece, :], sem.at[i]) for i in range(n_u)]

    @pl.when(first)
    def _():
        for c in copies:
            c.start()

    @pl.loop(0, rows // bm)
    def _(m):
        r = pl.ds(pl.multiple_of(m * bm, bm), bm)
        for i in range(n_u):
            @pl.when(first & (m == i * piece // bm))
            def _():
                copies[i].wait()
        u = u_all[r, :]
        gate = jnp.dot(u, g_ref[...], preferred_element_type=jnp.float32)
        up = jnp.dot(u, up_ref[...], preferred_element_type=jnp.float32)
        a_ref[r, :] = (jax.nn.silu(gate) * up).astype(jnp.bfloat16)


def gu_call(us, w, n_src):
    n_u = len(us)
    rows, d = us[0].shape
    rows *= n_u
    half = w.shape[1] // (2 * n_src)
    bn = math.gcd(256, half)
    nb = half // bn
    bm = min(512, rows)
    return pl.pallas_call(
        functools.partial(gu_kernel, bm, n_u),
        grid=(n_src, nb),
        in_specs=[pl.BlockSpec(memory_space=pl.ANY)] * n_u + [
            pl.BlockSpec((d, bn), lambda j, n: (0, 2 * j * nb + n)),
            pl.BlockSpec((d, bn), lambda j, n: (0, (2 * j + 1) * nb + n))],
        out_specs=pl.BlockSpec((rows, bn), lambda j, n: (0, j * nb + n)),
        out_shape=jax.ShapeDtypeStruct((rows, n_src * half), jnp.bfloat16),
        scratch_shapes=[pltpu.VMEM((rows, d), jnp.bfloat16), pltpu.SemaphoreType.DMA((n_u,))],
        compiler_params=params(),
        cost_estimate=cost(4 * rows * d * n_src * half, 2 * w.size + 2 * rows * d + 2 * rows * n_src * half),
        name="gate_up",
    )(*us, w, w)


def down_kernel(bm, parts, n_src, own, meta_ref, *refs):
    a_refs = refs[:parts]
    w_ref = refs[parts]
    rest = refs[parts + 1:]
    rows = a_refs[0].shape[0]
    n = pl.program_id(0)
    steps = pl.num_programs(0)
    bn = w_ref.shape[1]
    kj = w_ref.shape[0] // n_src

    @pl.loop(0, rows // bm)
    def _(m):
        r = pl.ds(pl.multiple_of(m * bm, bm), bm)
        acc = None
        for j in range(n_src):
            k0 = j * kj
            for p in range(parts):
                kp = a_refs[p].shape[1] // n_src
                part = jnp.dot(a_refs[p][r, j * kp:(j + 1) * kp], w_ref[k0:k0 + kp, :], preferred_element_type=jnp.float32)
                acc = part if acc is None else acc + part
                k0 += kp
        out = pl.ds(pl.multiple_of(m // 2 * bm, bm), bm)
        for h in range(2):
            @pl.when(m % 2 == h)
            def _():
                if own:
                    for i in range(bn // HEAD_DIM):
                        lanes = slice(i * HEAD_DIM, (i + 1) * HEAD_DIM)
                        col = pl.ds(pl.multiple_of(meta_ref[steps + n * (bn // HEAD_DIM) + i] * HEAD_DIM, HEAD_DIM), HEAD_DIM)
                        part = acc[:, lanes] + rest[1 + h][out, lanes].astype(jnp.float32)
                        rest[3][r, lanes] = (rest[0][r, col].astype(jnp.float32) + part).astype(jnp.bfloat16)
                else:
                    rest[h][out, :] = acc.astype(jnp.bfloat16)


def down_call(a_parts, w, meta, n_src, bn, steps, rows, call=0, resid=None, partials=()):
    parts = len(a_parts)
    cols = steps * bn
    own = resid is not None
    half = rows // 2
    step = lambda n, meta: (0, n)
    once = dict(pipeline_mode=pl.Buffered(1))
    args = [*a_parts, w]
    in_specs = [pl.BlockSpec((rows, a.shape[1]), lambda n, meta, b=(call if a.shape[0] > rows else 0): (b, 0), **once) for a in a_parts]
    in_specs += [pl.BlockSpec((w.shape[0], bn), lambda n, meta: (0, meta[n]))]
    if own:
        args += [resid, *partials]
        in_specs += [pl.BlockSpec(resid.shape, lambda n, meta: (0, 0), **once)] + [pl.BlockSpec((half, bn), lambda n, meta: (call, n))] * 2
    n_out = 1 if own else 2
    return pl.pallas_call(
        functools.partial(down_kernel, half if own else half // N_CALLS, parts, n_src, own),
        grid_spec=pltpu.PrefetchScalarGridSpec(
            num_scalar_prefetch=1, grid=(steps,), in_specs=in_specs, out_specs=[pl.BlockSpec((rows // n_out, bn), step)] * n_out),
        out_shape=[jax.ShapeDtypeStruct((rows // n_out, cols), jnp.bfloat16)] * n_out,
        compiler_params=params(),
        cost_estimate=cost(2 * rows * cols * w.shape[0], 2 * w.size + 4 * rows * cols),
        name="down",
    )(meta, *args)


def place_kernel(n_in, moves, n_tp, skip, idx_ref, *refs):
    ins = refs[:n_in]
    out_ref, sem = refs[-2:]
    copies = []
    for i, src_row, rows, call, who in moves:
        row = pl.multiple_of((call * n_tp + idx_ref[who]) * rows, rows)
        for q in range(ins[i].shape[1] // HEAD_DIM):
            col = pl.multiple_of(idx_ref[n_tp + skip + q] * HEAD_DIM, HEAD_DIM)
            copies.append(pltpu.make_async_copy(
                ins[i].at[src_row:src_row + rows, q * HEAD_DIM:(q + 1) * HEAD_DIM],
                out_ref.at[pl.ds(row, rows), pl.ds(col, HEAD_DIM)],
                sem.at[len(copies)]))
    for c in copies:
        c.start()
    for c in copies:
        c.wait()


def place_call(idx, pieces, moves, shape, n_tp, skip, out):
    n_in = len(pieces)
    args = list(pieces)
    in_specs = [pl.BlockSpec(p.shape, lambda *_: (0, 0)) for p in pieces]
    aliases = {}
    if out is not None:
        args.append(out)
        in_specs.append(pl.BlockSpec(memory_space=pl.ANY))
        aliases = {n_in + 1: 0}
    n_copies = sum(pieces[m[0]].shape[1] // HEAD_DIM for m in moves)
    return pl.pallas_call(
        functools.partial(place_kernel, n_in, moves, n_tp, skip),
        grid_spec=pltpu.PrefetchScalarGridSpec(
            num_scalar_prefetch=1, grid=(1,), in_specs=in_specs, out_specs=pl.BlockSpec(memory_space=pl.ANY),
            scratch_shapes=[pltpu.SemaphoreType.DMA((n_copies,))]),
        out_shape=jax.ShapeDtypeStruct(shape, jnp.bfloat16),
        input_output_aliases=aliases,
        compiler_params=params(),
        cost_estimate=cost(1000000, 4 * sum(p.size for p in pieces)),
        name="place",
    )(idx, *args)


def after(val, *deps):
    return lax.optimization_barrier((val, *deps))[0]


def solution(mesh):
    n_tp = mesh.shape['tp']
    n_fs = mesh.shape['fsdp']
    mesh2 = Mesh(mesh.devices.reshape(mesh.shape['dp'], n_tp // 2, 2, n_fs), ('dp', 'ta', 'tb', 'fsdp'))
    tp = ('ta', 'tb')
    batch_axes = ('dp', 'fsdp')
    in_specs = (P(batch_axes, None, None), P(batch_axes, None), P(batch_axes),
                P('fsdp', tp), P('fsdp', tp), P('fsdp', tp), P(tp, 'fsdp'),
                P('fsdp', tp), P('fsdp', tp), P(tp, 'fsdp'), P(None), P(None))
    out_specs = (P(batch_axes, None, None), P(batch_axes, None, tp, None), P(batch_axes, None, tp, None))

    def shift(val, s):
        return lax.ppermute(val, tp, [(i, (i + s) % n_tp) for i in range(n_tp)])

    def local_layer(tokens, positions, valid_len, w_query, w_key, w_value, w_out, w_gate, w_up, w_down, norm_attn, norm_mlp):
        _, seq, d = tokens.shape
        x = tokens.reshape(seq, d)
        n_q = w_query.shape[1] // HEAD_DIM
        n_kv = w_key.shape[1] // HEAD_DIM
        sub = seq // (n_tp * N_CALLS)
        me = lax.axis_index(tp)

        w_qkv = lax.all_gather(jnp.concatenate([w_query, w_key, w_value], axis=1), 'fsdp', axis=0, tiled=True)
        rounds = []
        for s in range(1, n_tp):
            rounds.append(shift(w_out, s))
        full_o = lax.all_gather(jnp.concatenate([w_out, *rounds], axis=0), 'fsdp', axis=1, tiled=True)
        fl = w_gate.shape[1]
        n_src = 2
        swaps = []
        lead = fl * 5 // 8
        for cut in (slice(0, lead), slice(lead, fl)):
            local = jnp.concatenate([w_gate[:, cut], w_up[:, cut]], axis=1)
            swaps.append((local, shift(local, 2)))
        swaps.append((w_down, shift(w_down, 2)))

        def joined(p, axis, *deps):
            return jnp.concatenate([after(swaps[p][0], *deps), swaps[p][1]], axis=axis)

        angles = positions.reshape(seq, 1).astype(jnp.float32) * rope_freqs()[None, :]
        cos_h, sin_h = jnp.cos(angles), jnp.sin(angles)
        cos_t = jnp.concatenate([cos_h, cos_h], axis=1)
        sin_t = jnp.concatenate([-sin_h, sin_h], axis=1)
        h = norm_call(x, norm_attn.reshape(1, d))
        q, k, v, vt = qkv_call(h, w_qkv, cos_t, sin_t, n_q, n_kv)

        pieces = []
        gu_parts = []
        o = q
        for call in range(N_CALLS):
            gu_parts.append(joined(call, 1, o))
            o = att_call(after(q, gu_parts[call], o), k, vt, valid_len, call)
            got = []
            for s in range(n_tp):
                blk = lax.dynamic_slice_in_dim(o, (me + s) % n_tp * sub, sub, axis=0)
                if s:
                    blk = shift(blk, s)
                got.append(blk)
            pieces.append(got)
        d_part = joined(2, 0, o)
        gu_full = [lax.all_gather(w, 'fsdp', axis=0, tiled=True) for w in gu_parts]
        n_blk = w_down.shape[1] // HEAD_DIM
        d_pair = lax.ppermute(d_part, 'fsdp', [(i, i ^ 1) for i in range(n_fs)])
        d_near = jnp.concatenate([d_part, d_pair], axis=1)
        d_full = [lax.all_gather(d_part[:, b * HEAD_DIM:(b + 1) * HEAD_DIM], 'fsdp', axis=1, tiled=True) for b in range(n_blk)]

        resid, u_own, u_prev, u_next = [], [], [], []
        order = d_part
        for call in range(N_CALLS):
            got = pieces[call]
            got[0] = after(got[0], order)
            row = (call * n_tp + me).reshape(1).astype(jnp.int32)
            r, ua, ub = out_call(row, got, full_o, x, norm_mlp.reshape(1, d))
            order = r
            resid.append(r)
            u_own += [ua, ub]
            u_prev.append(shift(ua, 1))
            u_next.append(shift(ub, -1))
        u_recv = [u_prev[0], u_next[0], u_prev[1], u_next[1]]

        def gate_up(p, us, dep):
            return gu_call([after(us[0], dep)] + us[1:], gu_full[p], n_src)

        a_own = gate_up(0, u_own, resid[-1])
        a_recv = [gate_up(0, u_recv, a_own)]
        a_recv.append(gate_up(1, u_recv, a_recv[0]))
        a_late = []

        fs = lax.axis_index('fsdp')
        chip, n_chip = fs // 2, n_fs // 2
        others = [(chip + 1 + i) % n_chip for i in range(n_chip - 1)]
        bn = 2 * HEAD_DIM
        blocks = [(d_near, list(range(n_blk)), [fs * n_blk + i for i in range(n_blk)] + [(fs ^ 1) * n_blk + i for i in range(n_blk)])]
        for b in range(n_blk):
            units = sum(([2 * o_ * n_blk + b, (2 * o_ + 1) * n_blk + b] for o_ in others), [])
            blocks.append((d_full[b], others, units))
        order = a_recv[1]
        mine = []
        for b, (w, sel, units) in enumerate(blocks):
            meta = jnp.stack([jnp.asarray(v, jnp.int32) for v in [*sel, *units]])
            p_prev, p_next = down_call([after(a_recv[0], order), a_recv[1]], w, meta, n_src, bn, len(sel), N_CALLS * sub)
            b_next = shift(p_prev, -1)
            b_prev = shift(p_next, 1)
            order = p_prev
            m, near = [], {}
            for c in range(N_CALLS):
                if b == 0:
                    a_late.append(gate_up(1, u_own[2 * c:2 * c + 2], order))
                    order = a_late[c]
                m += down_call([after(a_own, order), a_late[c]], w, meta, n_src, bn, len(sel), sub, c, resid[c], (b_next, b_prev))
                order = m[c]
                for g, by in enumerate((1, -1)):
                    near[g, c] = shift(m[c], by)
            mine.append((m, near))
        idx = jnp.stack([jnp.asarray(v, jnp.int32) for v in [(me - s) % n_tp for s in range(n_tp)] + sum((u for _, _, u in blocks), [])])
        near_moves = [(i * N_CALLS + c, 0, sub, c, who) for i, who in enumerate((0, 1, n_tp - 1)) for c in range(N_CALLS)]
        far_moves = [(0, 0, sub, 0, 2), (1, 0, sub, N_CALLS - 1, 2)]
        hidden = None
        skip = 0
        last = len(blocks) - 1
        for b in range(len(blocks)):
            m, near = mine[b]
            src = (near[0, 0], near[1, N_CALLS - 1])
            if b == last:
                src = tuple(after(v, hidden) for v in src)
            far_0 = shift(src[0], 1)
            far_1 = shift(src[1], -1)
            pieces = [*m, *(near[g, c] for g in range(2) for c in range(N_CALLS))]
            if b == 0:
                pieces[0] = after(pieces[0], order)
            hidden = place_call(idx, pieces, near_moves, (seq, d), n_tp, skip, hidden)
            hidden = place_call(idx, (far_0, far_1), far_moves, (seq, d), n_tp, skip, hidden)
            skip += len(blocks[b][2])
        hidden = hidden.reshape(1, seq, d)
        return hidden, k.reshape(1, seq, n_kv, HEAD_DIM), v.reshape(1, seq, n_kv, HEAD_DIM)


    return jax.shard_map(local_layer, mesh=mesh2, in_specs=in_specs, out_specs=out_specs, check_vma=False)
```

```python
import functools
import math
import jax
import jax.numpy as jnp
from jax import lax
from jax.experimental import pallas as pl
from jax.experimental.pallas import tpu as pltpu
from jax.sharding import Mesh, PartitionSpec as P


HEAD_DIM = 128
ROPE_THETA = 500000.0
NORM_EPS = 1e-5
EXP2_SCALE = HEAD_DIM ** -0.5 * math.log2(math.e)
N_CALLS = 2
VMEM_LIMIT = 67043328


def rope_freqs():
    half_idx = jnp.arange(HEAD_DIM // 2, dtype=jnp.float32)
    inv_freq = jnp.power(ROPE_THETA, -2.0 * half_idx / HEAD_DIM)
    wave_len = 2.0 * math.pi / inv_freq
    smooth = (8192.0 / wave_len - 1.0) / 3.0
    blended = (1.0 - smooth) * inv_freq / 8.0 + smooth * inv_freq
    return jnp.where(wave_len < 2048.0, inv_freq, jnp.where(wave_len > 8192.0, inv_freq / 8.0, blended))


def params(**kw):
    return pltpu.CompilerParams(vmem_limit_bytes=VMEM_LIMIT, **kw)


def cost(flops, nbytes):
    return pl.CostEstimate(flops=flops, bytes_accessed=nbytes, transcendentals=0)


def norm_rows(vals_f32, gain):
    inv = lax.rsqrt(jnp.mean(vals_f32 * vals_f32, axis=-1, keepdims=True) + NORM_EPS)
    return (vals_f32 * inv * gain).astype(jnp.bfloat16)


def norm_into(x_ref, gain, store):
    rows = min(16, x_ref.shape[0])

    @pl.loop(0, x_ref.shape[0] // rows)
    def _(i):
        r = pl.ds(pl.multiple_of(i * rows, rows), rows)
        store(r, norm_rows(x_ref[r, :].astype(jnp.float32), gain))


def norm_kernel(x_ref, g_ref, h_ref):
    def store(r, val):
        h_ref[r, :] = val

    norm_into(x_ref, g_ref[...].astype(jnp.float32), store)


def norm_call(x, gain):
    s, d = x.shape
    bm = min(512, s)
    return pl.pallas_call(
        norm_kernel,
        grid=(s // bm,),
        in_specs=[pl.BlockSpec((bm, d), lambda i: (i, 0)), pl.BlockSpec((1, d), lambda i: (0, 0))],
        out_specs=pl.BlockSpec((bm, d), lambda i: (i, 0)),
        out_shape=jax.ShapeDtypeStruct((s, d), jnp.bfloat16),
        compiler_params=params(),
        cost_estimate=cost(8 * s * d, 4 * s * d),
        name="norm",
    )(x, gain)


def qkv_kernel(n_q, n_kv, h_ref, w_ref, cos_ref, sin_ref, q_ref, k_ref, v_ref, vt_ref):
    h = h_ref[...]
    cos_t, sin_t = cos_ref[...], sin_ref[...]
    n_heads = n_q + 2 * n_kv
    for lo in range(0, n_heads, 2):
        y = jnp.dot(h, w_ref[:, lo * HEAD_DIM:(lo + 2) * HEAD_DIM], preferred_element_type=jnp.float32)
        for i in range(lo, lo + 2):
            a = y[:, (i - lo) * HEAD_DIM:(i - lo + 1) * HEAD_DIM]
            if i >= n_q + n_kv:
                cols = slice((i - n_q - n_kv) * HEAD_DIM, (i - n_q - n_kv + 1) * HEAD_DIM)
                v_ref[:, cols] = a.astype(jnp.bfloat16)
                vt_ref[cols, :] = a.T.astype(jnp.bfloat16)
                continue
            r = (a * cos_t + pltpu.roll(a, HEAD_DIM // 2, 1) * sin_t).astype(jnp.bfloat16)
            if i < n_q:
                q_ref[i] = r
            else:
                k_ref[:, (i - n_q) * HEAD_DIM:(i - n_q + 1) * HEAD_DIM] = r


def qkv_call(h, w, cos_t, sin_t, n_q, n_kv):
    s, d = h.shape
    bm = min(512, s)
    n = w.shape[1]
    row = lambda i: (i, 0)
    return pl.pallas_call(
        functools.partial(qkv_kernel, n_q, n_kv),
        grid=(s // bm,),
        in_specs=[pl.BlockSpec((bm, d), row), pl.BlockSpec((d, n), lambda i: (0, 0), pipeline_mode=pl.Buffered(1)),
                  pl.BlockSpec((bm, HEAD_DIM), row), pl.BlockSpec((bm, HEAD_DIM), row)],
        out_specs=[pl.BlockSpec((n_q, bm, HEAD_DIM), lambda i: (0, i, 0)),
                   pl.BlockSpec((bm, n_kv * HEAD_DIM), row), pl.BlockSpec((bm, n_kv * HEAD_DIM), row),
                   pl.BlockSpec((n_kv * HEAD_DIM, bm), lambda i: (0, i))],
        out_shape=[jax.ShapeDtypeStruct((n_q, s, HEAD_DIM), jnp.bfloat16),
                   jax.ShapeDtypeStruct((s, n_kv * HEAD_DIM), jnp.bfloat16),
                   jax.ShapeDtypeStruct((s, n_kv * HEAD_DIM), jnp.bfloat16),
                   jax.ShapeDtypeStruct((n_kv * HEAD_DIM, s), jnp.bfloat16)],
        compiler_params=params(),
        cost_estimate=cost(2 * s * d * n, 2 * s * d + 2 * d * n + 2 * s * n),
        name="qkv",
    )(h, w, cos_t, sin_t)


def att_kernel(bq, bk, per, first, len_ref, q_ref, k_ref, vt_ref, o_ref, s_ref, p_ref, m_ref, l_ref, alpha_ref, acc_ref):
    row0 = first + pl.program_id(1) * bq
    valid = len_ref[0]
    last = k_ref.shape[0] // bk - 1
    m_ref[...] = jnp.full_like(m_ref, -jnp.inf)
    l_ref[...] = jnp.zeros_like(l_ref)
    alpha_ref[...] = jnp.zeros_like(alpha_ref)
    acc_ref[...] = jnp.zeros_like(acc_ref)
    p_ref[...] = jnp.zeros_like(p_ref)

    def scores(j, h):
        k_blk = k_ref[pl.ds(pl.multiple_of(j * bk, bk), bk), :]
        s_ref[h] = lax.dot_general(k_blk, q_ref[h], (((1,), (1,)), ((), ())), preferred_element_type=jnp.float32)

    def values(j, h):
        vt_blk = vt_ref[:, pl.ds(pl.multiple_of(j * bk, bk), bk)]
        acc_ref[h] = acc_ref[h] * alpha_ref[h] + jnp.dot(vt_blk, p_ref[h], preferred_element_type=jnp.float32)

    tall = min(32, bk)

    def softmax(j, h, masked):
        m_old = m_ref[h]
        m8 = None
        for c in range(bk // tall):
            r = slice(c * tall, (c + 1) * tall)
            sc = s_ref[h, r, :]
            if masked:
                kid = j * bk + c * tall + lax.broadcasted_iota(jnp.int32, (tall, bq), 0)
                qid = row0 + lax.broadcasted_iota(jnp.int32, (tall, bq), 1)
                sc = jnp.where((kid <= qid) & (kid < valid), sc, -jnp.inf)
                s_ref[h, r, :] = sc
            top = jnp.max(sc.reshape(tall // 8, 8, bq), axis=0)
            m8 = top if m8 is None else jnp.maximum(m8, top)
        m_new = jnp.maximum(m_old, jnp.max(m8, axis=0, keepdims=True))
        m_rows = jnp.broadcast_to(m_new, (8, bq))[None]
        l8 = None
        for c in range(bk // tall):
            r = slice(c * tall, (c + 1) * tall)
            p = jnp.exp2((s_ref[h, r, :].reshape(tall // 8, 8, bq) - m_rows) * EXP2_SCALE)
            tot = jnp.sum(p, axis=0)
            l8 = tot if l8 is None else l8 + tot
            p_ref[h, r, :] = p.reshape(tall, bq).astype(jnp.bfloat16)
        alpha = jnp.exp2((m_old - m_new) * EXP2_SCALE)
        l_ref[h] = l_ref[h] * alpha + jnp.sum(l8, axis=0, keepdims=True)
        alpha_ref[h] = alpha
        m_ref[h] = m_new

    def step(j, masked):
        for h in range(per):
            values(jnp.maximum(j - 1, 0), h)
            softmax(j, h, masked)
            scores(jnp.minimum(j + 1, last), h)

    n_full = jnp.minimum((row0 + 1) // bk, valid // bk)
    n_end = jnp.minimum((row0 + bq + bk - 1) // bk, (valid + bk - 1) // bk)

    def full(j, _):
        step(j, False)
        return 0

    def part(j, _):
        step(j, True)
        return 0

    for h in range(per):
        scores(0, h)
    lax.fori_loop(0, n_full, full, 0)
    lax.fori_loop(n_full, n_end, part, 0)
    for h in range(per):
        values(n_end - 1, h)
        o_ref[:, h * HEAD_DIM:(h + 1) * HEAD_DIM] = (acc_ref[h] / l_ref[h]).T.astype(jnp.bfloat16)


def att_call(q, k, vt, valid_len, call):
    n_q, s, _ = q.shape
    n_kv = k.shape[1] // HEAD_DIM
    per = n_q // n_kv
    rows = s // N_CALLS
    bq = min(512, rows)
    bk = min(512, s)
    first = call * rows
    off = first // bq
    frac = (2 * call + 1) / N_CALLS ** 2
    return pl.pallas_call(
        functools.partial(att_kernel, bq, bk, per, first),
        grid=(n_kv, rows // bq),
        in_specs=[pl.BlockSpec(memory_space=pltpu.SMEM),
                  pl.BlockSpec((per, bq, HEAD_DIM), lambda g, i: (g, off + i, 0)),
                  pl.BlockSpec((s, HEAD_DIM), lambda g, i: (0, g)),
                  pl.BlockSpec((HEAD_DIM, s), lambda g, i: (g, 0))],
        out_specs=pl.BlockSpec((bq, per * HEAD_DIM), lambda g, i: (i, g)),
        out_shape=jax.ShapeDtypeStruct((rows, n_q * HEAD_DIM), jnp.bfloat16),
        scratch_shapes=[pltpu.VMEM((per, bk, bq), jnp.float32), pltpu.VMEM((per, bk, bq), jnp.bfloat16)]
        + [pltpu.VMEM((per, 1, bq), jnp.float32)] * 3 + [pltpu.VMEM((per, HEAD_DIM, bq), jnp.float32)],
        compiler_params=params(),
        cost_estimate=cost(int(8 * frac * n_q * s * s * HEAD_DIM), 4 * n_q * s * HEAD_DIM),
        name="attention",
    )(valid_len, q, k, vt)


def out_kernel(n_src, idx_ref, *refs):
    o_refs = refs[:n_src]
    w_ref, x_ref, g_ref, r_ref, ua_ref, ub_ref, o_all, y_ref = refs[n_src:]
    ko = o_refs[0].shape[1]
    n = pl.program_id(0)
    bn = w_ref.shape[1]
    half = ua_ref.shape[0]

    @pl.when(n == 0)
    def _():
        for s in range(n_src):
            o_all[:, s * ko:(s + 1) * ko] = o_refs[s][...]

    acc = jnp.dot(o_all[...], w_ref[...], preferred_element_type=jnp.float32)
    col = pl.ds(pl.multiple_of(n * bn, bn), bn)
    y_ref[:, col] = (x_ref[:, col].astype(jnp.float32) + acc).astype(jnp.bfloat16)

    @pl.when(n == pl.num_programs(0) - 1)
    def _():
        r_ref[...] = y_ref[...]
        gain = g_ref[...].astype(jnp.float32)
        for part, u_ref in enumerate((ua_ref, ub_ref)):
            def store(r, val, u_ref=u_ref):
                u_ref[r, :] = val

            norm_into(y_ref.at[part * half:(part + 1) * half, :], gain, store)


def out_call(idx, o_pieces, w, x, gain):
    n_src = len(o_pieces)
    rows, ko = o_pieces[0].shape
    d = x.shape[1]
    bn = min(512, d)
    fixed = lambda n, idx: (0, 0)
    half = jax.ShapeDtypeStruct((rows // 2, d), jnp.bfloat16)
    return pl.pallas_call(
        functools.partial(out_kernel, n_src),
        grid_spec=pltpu.PrefetchScalarGridSpec(
            num_scalar_prefetch=1,
            grid=(d // bn,),
            in_specs=[pl.BlockSpec((rows, ko), fixed)] * n_src + [
                pl.BlockSpec((n_src * ko, bn), lambda n, idx: (0, n)),
                pl.BlockSpec((rows, d), lambda n, idx: (idx[0], 0)),
                pl.BlockSpec((1, d), fixed)],
            out_specs=[pl.BlockSpec((rows, d), fixed), pl.BlockSpec((rows // 2, d), fixed), pl.BlockSpec((rows // 2, d), fixed)],
            scratch_shapes=[pltpu.VMEM((rows, n_src * ko), jnp.bfloat16), pltpu.VMEM((rows, d), jnp.bfloat16)]),
        out_shape=[jax.ShapeDtypeStruct((rows, d), jnp.bfloat16), half, half],
        compiler_params=params(),
        cost_estimate=cost(2 * rows * d * ko * n_src, 2 * w.size + 8 * rows * d),
        name="w_out",
    )(idx, *o_pieces, w, x, gain)


def gu_kernel(bm, n_u, *refs):
    u_refs = refs[:n_u]
    g_ref, up_ref, a_ref, u_all, sem = refs[n_u:]
    rows = u_all.shape[0]
    piece = rows // n_u
    first = (pl.program_id(0) == 0) & (pl.program_id(1) == 0)
    copies = [pltpu.make_async_copy(u_refs[i], u_all.at[i * piece:(i + 1) * piece, :], sem.at[i]) for i in range(n_u)]

    @pl.when(first)
    def _():
        for c in copies:
            c.start()

    @pl.loop(0, rows // bm)
    def _(m):
        r = pl.ds(pl.multiple_of(m * bm, bm), bm)
        for i in range(n_u):
            @pl.when(first & (m == i * piece // bm))
            def _():
                copies[i].wait()
        u = u_all[r, :]
        gate = jnp.dot(u, g_ref[...], preferred_element_type=jnp.float32)
        up = jnp.dot(u, up_ref[...], preferred_element_type=jnp.float32)
        a_ref[r, :] = (jax.nn.silu(gate) * up).astype(jnp.bfloat16)


def gu_call(us, w, n_src):
    n_u = len(us)
    rows, d = us[0].shape
    rows *= n_u
    half = w.shape[1] // (2 * n_src)
    bn = math.gcd(256, half)
    nb = half // bn
    bm = min(512, rows)
    return pl.pallas_call(
        functools.partial(gu_kernel, bm, n_u),
        grid=(n_src, nb),
        in_specs=[pl.BlockSpec(memory_space=pl.ANY)] * n_u + [
            pl.BlockSpec((d, bn), lambda j, n: (0, 2 * j * nb + n)),
            pl.BlockSpec((d, bn), lambda j, n: (0, (2 * j + 1) * nb + n))],
        out_specs=pl.BlockSpec((rows, bn), lambda j, n: (0, j * nb + n)),
        out_shape=jax.ShapeDtypeStruct((rows, n_src * half), jnp.bfloat16),
        scratch_shapes=[pltpu.VMEM((rows, d), jnp.bfloat16), pltpu.SemaphoreType.DMA((n_u,))],
        compiler_params=params(),
        cost_estimate=cost(4 * rows * d * n_src * half, 2 * w.size + 2 * rows * d + 2 * rows * n_src * half),
        name="gate_up",
    )(*us, w, w)


def down_kernel(bm, parts, n_src, own, row0, meta_ref, *refs):
    a_any = refs[:parts]
    w_ref = refs[parts]
    rest = refs[parts + 1:]
    resid_any = rest[0] if own else None
    partials = rest[1:3] if own else ()
    outs = rest[3:4] if own else rest[:2]
    scratch = rest[4:] if own else rest[2:]
    a_refs, sem = scratch[:parts], scratch[parts]
    rows = a_refs[0].shape[0]
    n = pl.program_id(0)
    bn = w_ref.shape[1]
    kj = w_ref.shape[0] // n_src
    n_m = rows // bm
    copies = [[pltpu.make_async_copy(a_any[p].at[row0[p] + i * bm:row0[p] + (i + 1) * bm, :], a_refs[p].at[i * bm:(i + 1) * bm, :], sem.at[p, i])
               for p in range(parts)] for i in range(n_m)]
    more = []
    if own:
        r_ref, r_sem = scratch[parts + 1:]
        for q in range(r_ref.shape[1] // HEAD_DIM):
            col = pl.multiple_of(meta_ref[r_ref.shape[1] // bn + q] * HEAD_DIM, HEAD_DIM)
            more.append(pltpu.make_async_copy(resid_any.at[:, pl.ds(col, HEAD_DIM)], r_ref.at[:, q * HEAD_DIM:(q + 1) * HEAD_DIM], r_sem.at[q]))

    @pl.when(n == 0)
    def _():
        for c in sum(copies, []) + more:
            c.start()

    @pl.loop(0, n_m)
    def _(m):
        for i in range(n_m):
            @pl.when((n == 0) & (m == i))
            def _():
                for c in copies[i]:
                    c.wait()
        r = pl.ds(pl.multiple_of(m * bm, bm), bm)
        acc = None
        for j in range(n_src):
            k0 = j * kj
            for p in range(parts):
                kp = a_refs[p].shape[1] // n_src
                part = jnp.dot(a_refs[p][r, j * kp:(j + 1) * kp], w_ref[k0:k0 + kp, :], preferred_element_type=jnp.float32)
                acc = part if acc is None else acc + part
                k0 += kp
        if own:
            @pl.when((n == 0) & (m == 0))
            def _():
                for c in more:
                    c.wait()

            for h in range(2):
                @pl.when(m == h)
                def _():
                    base = r_ref[r, pl.ds(pl.multiple_of(n * bn, bn), bn)].astype(jnp.float32)
                    outs[0][r, :] = (base + (acc + partials[h][...].astype(jnp.float32))).astype(jnp.bfloat16)
        else:
            out = pl.ds(pl.multiple_of(m // 2 * bm, bm), bm)
            for h in range(2):
                @pl.when(m % 2 == h)
                def _():
                    outs[h][out, :] = acc.astype(jnp.bfloat16)


def down_call(a_parts, w, meta, n_src, bn, steps, rows, call=0, resid=None, partials=()):
    parts = len(a_parts)
    cols = steps * bn
    own = resid is not None
    half = rows // 2
    bm = half if own else half // N_CALLS
    step = lambda n, meta: (0, n)
    anywhere = pl.BlockSpec(memory_space=pl.ANY)
    args = [*a_parts, w]
    in_specs = [anywhere] * parts + [pl.BlockSpec((w.shape[0], bn), lambda n, meta: (0, meta[n]))]
    scratch = [pltpu.VMEM((rows, a.shape[1]), jnp.bfloat16) for a in a_parts] + [pltpu.SemaphoreType.DMA((parts, rows // bm))]
    if own:
        args += [resid, *partials]
        in_specs += [anywhere] + [pl.BlockSpec((half, bn), lambda n, meta: (call, n))] * 2
        scratch += [pltpu.VMEM((rows, cols), jnp.bfloat16), pltpu.SemaphoreType.DMA((cols // HEAD_DIM,))]
    n_out = 1 if own else 2
    row0 = tuple(call * rows if a.shape[0] > rows else 0 for a in a_parts)
    return pl.pallas_call(
        functools.partial(down_kernel, bm, parts, n_src, own, row0),
        grid_spec=pltpu.PrefetchScalarGridSpec(
            num_scalar_prefetch=1, grid=(steps,), in_specs=in_specs, out_specs=[pl.BlockSpec((rows // n_out, bn), step)] * n_out,
            scratch_shapes=scratch),
        out_shape=[jax.ShapeDtypeStruct((rows // n_out, cols), jnp.bfloat16)] * n_out,
        compiler_params=params(),
        cost_estimate=cost(2 * rows * cols * w.shape[0], 2 * w.size + 4 * rows * cols),
        name="down",
    )(meta, *args)


def place_kernel(n_in, moves, n_tp, skip, idx_ref, *refs):
    ins = refs[:n_in]
    out_ref, sem = refs[-2:]
    copies = []
    for i, src_row, rows, call, who in moves:
        row = pl.multiple_of((call * n_tp + idx_ref[who]) * rows, rows)
        for q in range(ins[i].shape[1] // HEAD_DIM):
            col = pl.multiple_of(idx_ref[n_tp + skip + q] * HEAD_DIM, HEAD_DIM)
            copies.append(pltpu.make_async_copy(
                ins[i].at[src_row:src_row + rows, q * HEAD_DIM:(q + 1) * HEAD_DIM],
                out_ref.at[pl.ds(row, rows), pl.ds(col, HEAD_DIM)],
                sem.at[len(copies)]))
    for c in copies:
        c.start()
    for c in copies:
        c.wait()


def place_call(idx, pieces, moves, shape, n_tp, skip, out):
    n_in = len(pieces)
    args = list(pieces)
    in_specs = [pl.BlockSpec(p.shape, lambda *_: (0, 0)) for p in pieces]
    aliases = {}
    if out is not None:
        args.append(out)
        in_specs.append(pl.BlockSpec(memory_space=pl.ANY))
        aliases = {n_in + 1: 0}
    n_copies = sum(pieces[m[0]].shape[1] // HEAD_DIM for m in moves)
    return pl.pallas_call(
        functools.partial(place_kernel, n_in, moves, n_tp, skip),
        grid_spec=pltpu.PrefetchScalarGridSpec(
            num_scalar_prefetch=1, grid=(1,), in_specs=in_specs, out_specs=pl.BlockSpec(memory_space=pl.ANY),
            scratch_shapes=[pltpu.SemaphoreType.DMA((n_copies,))]),
        out_shape=jax.ShapeDtypeStruct(shape, jnp.bfloat16),
        input_output_aliases=aliases,
        compiler_params=params(),
        cost_estimate=cost(1000000, 4 * sum(p.size for p in pieces)),
        name="place",
    )(idx, *args)


def after(val, *deps):
    return lax.optimization_barrier((val, *deps))[0]


def solution(mesh):
    n_tp = mesh.shape['tp']
    n_fs = mesh.shape['fsdp']
    mesh2 = Mesh(mesh.devices.reshape(mesh.shape['dp'], n_tp // 2, 2, n_fs), ('dp', 'ta', 'tb', 'fsdp'))
    tp = ('ta', 'tb')
    batch_axes = ('dp', 'fsdp')
    in_specs = (P(batch_axes, None, None), P(batch_axes, None), P(batch_axes),
                P('fsdp', tp), P('fsdp', tp), P('fsdp', tp), P(tp, 'fsdp'),
                P('fsdp', tp), P('fsdp', tp), P(tp, 'fsdp'), P(None), P(None))
    out_specs = (P(batch_axes, None, None), P(batch_axes, None, tp, None), P(batch_axes, None, tp, None))

    def shift(val, s):
        return lax.ppermute(val, tp, [(i, (i + s) % n_tp) for i in range(n_tp)])

    def local_layer(tokens, positions, valid_len, w_query, w_key, w_value, w_out, w_gate, w_up, w_down, norm_attn, norm_mlp):
        _, seq, d = tokens.shape
        x = tokens.reshape(seq, d)
        n_q = w_query.shape[1] // HEAD_DIM
        n_kv = w_key.shape[1] // HEAD_DIM
        sub = seq // (n_tp * N_CALLS)
        me = lax.axis_index(tp)

        w_qkv = lax.all_gather(jnp.concatenate([w_query, w_key, w_value], axis=1), 'fsdp', axis=0, tiled=True)
        rounds = []
        for s in range(1, n_tp):
            rounds.append(shift(w_out, s))
        full_o = lax.all_gather(jnp.concatenate([w_out, *rounds], axis=0), 'fsdp', axis=1, tiled=True)
        fl = w_gate.shape[1]
        n_src = 2
        swaps = []
        lead = fl * 5 // 8
        for cut in (slice(0, lead), slice(lead, fl)):
            local = jnp.concatenate([w_gate[:, cut], w_up[:, cut]], axis=1)
            swaps.append((local, shift(local, 2)))
        swaps.append((w_down, shift(w_down, 2)))

        def joined(p, axis, *deps):
            return jnp.concatenate([after(swaps[p][0], *deps), swaps[p][1]], axis=axis)

        angles = positions.reshape(seq, 1).astype(jnp.float32) * rope_freqs()[None, :]
        cos_h, sin_h = jnp.cos(angles), jnp.sin(angles)
        cos_t = jnp.concatenate([cos_h, cos_h], axis=1)
        sin_t = jnp.concatenate([-sin_h, sin_h], axis=1)
        h = norm_call(x, norm_attn.reshape(1, d))
        q, k, v, vt = qkv_call(h, w_qkv, cos_t, sin_t, n_q, n_kv)

        pieces = []
        gu_parts = []
        o = q
        for call in range(N_CALLS):
            gu_parts.append(joined(call, 1, o))
            o = att_call(after(q, gu_parts[call], o), k, vt, valid_len, call)
            got = []
            for s in range(n_tp):
                blk = lax.dynamic_slice_in_dim(o, (me + s) % n_tp * sub, sub, axis=0)
                if s:
                    blk = shift(blk, s)
                got.append(blk)
            pieces.append(got)
        d_part = joined(2, 0, o)
        gu_full = [lax.all_gather(w, 'fsdp', axis=0, tiled=True) for w in gu_parts]
        n_blk = w_down.shape[1] // HEAD_DIM
        d_pair = lax.ppermute(d_part, 'fsdp', [(i, i ^ 1) for i in range(n_fs)])
        d_near = jnp.concatenate([d_part, d_pair], axis=1)
        d_full = [lax.all_gather(d_part[:, b * HEAD_DIM:(b + 1) * HEAD_DIM], 'fsdp', axis=1, tiled=True) for b in range(n_blk)]

        resid, u_own, u_prev, u_next = [], [], [], []
        order = d_part
        for call in range(N_CALLS):
            got = pieces[call]
            got[0] = after(got[0], order)
            row = (call * n_tp + me).reshape(1).astype(jnp.int32)
            r, ua, ub = out_call(row, got, full_o, x, norm_mlp.reshape(1, d))
            order = r
            resid.append(r)
            u_own += [ua, ub]
            u_prev.append(shift(ua, 1))
            u_next.append(shift(ub, -1))
        u_recv = [u_prev[0], u_next[0], u_prev[1], u_next[1]]

        def gate_up(p, us, dep):
            return gu_call([after(us[0], dep)] + us[1:], gu_full[p], n_src)

        a_own = gate_up(0, u_own, resid[-1])
        a_recv = [gate_up(0, u_recv, a_own)]
        a_recv.append(gate_up(1, u_recv, a_recv[0]))
        a_late = []

        fs = lax.axis_index('fsdp')
        chip, n_chip = fs // 2, n_fs // 2
        others = [(chip + 1 + i) % n_chip for i in range(n_chip - 1)]
        bn = 2 * HEAD_DIM
        blocks = [(d_near, list(range(n_blk)), [fs * n_blk + i for i in range(n_blk)] + [(fs ^ 1) * n_blk + i for i in range(n_blk)])]
        for b in range(n_blk):
            units = sum(([2 * o_ * n_blk + b, (2 * o_ + 1) * n_blk + b] for o_ in others), [])
            blocks.append((d_full[b], others, units))
        idx = jnp.stack([jnp.asarray(v, jnp.int32) for v in [(me - s) % n_tp for s in range(n_tp)] + sum((u for _, _, u in blocks), [])])
        near_moves = [(i * N_CALLS + c, 0, sub, c, who) for i, who in enumerate((0, 1, n_tp - 1)) for c in range(N_CALLS)]
        far_moves = [(0, 0, sub, 0, 2), (1, 0, sub, N_CALLS - 1, 2)]
        skip = [sum(len(u) for _, _, u in blocks[:b]) for b in range(len(blocks))]
        last = len(blocks) - 1
        mine, far = [], []

        def place_near(b, out, *deps):
            m, near = mine[b]
            pieces = [*m, *(near[g, c] for g in range(2) for c in range(N_CALLS))]
            pieces[0] = after(pieces[0], *deps)
            return place_call(idx, pieces, near_moves, (seq, d), n_tp, skip[b], out)

        def place_far(b, out):
            return place_call(idx, far[b], far_moves, (seq, d), n_tp, skip[b], out)

        def relay(b, *deps):
            near = mine[b][1]
            far_0 = shift(after(near[0, 0], *deps), 1)
            far_1 = shift(after(near[1, N_CALLS - 1], *deps), -1)
            far.append((far_0, far_1))

        order = a_recv[1]
        hidden = None
        for b, (w, sel, units) in enumerate(blocks):
            meta = jnp.stack([jnp.asarray(v, jnp.int32) for v in [*sel, *units]])
            p_prev, p_next = down_call([after(a_recv[0], order), a_recv[1]], w, meta, n_src, bn, len(sel), N_CALLS * sub)
            b_next = shift(p_prev, -1)
            b_prev = shift(p_next, 1)
            order = p_prev
            if b >= 1:
                relay(b - 1)
            if b >= 2:
                hidden = place_far(b - 2, place_near(b - 2, hidden, order))
                order = hidden
            m, near = [], {}
            for c in range(N_CALLS):
                if b == 0:
                    a_late.append(gate_up(1, u_own[2 * c:2 * c + 2], order))
                    order = a_late[c]
                m += down_call([after(a_own, order), a_late[c]], w, meta, n_src, bn, len(sel), sub, c, resid[c], (b_next, b_prev))
                order = m[c]
                for g, by in enumerate((1, -1)):
                    near[g, c] = shift(m[c], by)
            mine.append((m, near))
        hidden = place_far(last - 1, place_near(last - 1, hidden, order))
        relay(last, hidden)
        hidden = place_far(last, place_near(last, hidden))
        hidden = hidden.reshape(1, seq, d)
        return hidden, k.reshape(1, seq, n_kv, HEAD_DIM), v.reshape(1, seq, n_kv, HEAD_DIM)


    return jax.shard_map(local_layer, mesh=mesh2, in_specs=in_specs, out_specs=out_specs, check_vma=False)
```

```python
import functools
import math
import jax
import jax.numpy as jnp
from jax import lax
from jax.experimental import pallas as pl
from jax.experimental.pallas import tpu as pltpu
from jax.sharding import Mesh, PartitionSpec as P


HEAD_DIM = 128
ROPE_THETA = 500000.0
NORM_EPS = 1e-5
EXP2_SCALE = HEAD_DIM ** -0.5 * math.log2(math.e)
N_CALLS = 2
VMEM_LIMIT = 67043328


def rope_freqs():
    half_idx = jnp.arange(HEAD_DIM // 2, dtype=jnp.float32)
    inv_freq = jnp.power(ROPE_THETA, -2.0 * half_idx / HEAD_DIM)
    wave_len = 2.0 * math.pi / inv_freq
    smooth = (8192.0 / wave_len - 1.0) / 3.0
    blended = (1.0 - smooth) * inv_freq / 8.0 + smooth * inv_freq
    return jnp.where(wave_len < 2048.0, inv_freq, jnp.where(wave_len > 8192.0, inv_freq / 8.0, blended))


def params(**kw):
    return pltpu.CompilerParams(vmem_limit_bytes=VMEM_LIMIT, **kw)


def cost(flops, nbytes):
    return pl.CostEstimate(flops=flops, bytes_accessed=nbytes, transcendentals=0)


def norm_rows(vals_f32, gain):
    inv = lax.rsqrt(jnp.mean(vals_f32 * vals_f32, axis=-1, keepdims=True) + NORM_EPS)
    return (vals_f32 * inv * gain).astype(jnp.bfloat16)


def norm_kernel(x_ref, g_ref, h_ref):
    h_ref[...] = norm_rows(x_ref[...].astype(jnp.float32), g_ref[...].astype(jnp.float32))


def norm_call(x, gain):
    s, d = x.shape
    bm = min(512, s)
    return pl.pallas_call(
        norm_kernel,
        grid=(s // bm,),
        in_specs=[pl.BlockSpec((bm, d), lambda i: (i, 0)), pl.BlockSpec((1, d), lambda i: (0, 0))],
        out_specs=pl.BlockSpec((bm, d), lambda i: (i, 0)),
        out_shape=jax.ShapeDtypeStruct((s, d), jnp.bfloat16),
        compiler_params=params(),
        cost_estimate=cost(8 * s * d, 4 * s * d),
        name="norm",
    )(x, gain)


def qkv_kernel(n_q, n_kv, h_ref, w_ref, cos_ref, sin_ref, q_ref, k_ref, v_ref, vt_ref):
    h = h_ref[...]
    cos_t, sin_t = cos_ref[...], sin_ref[...]
    n_heads = n_q + 2 * n_kv
    for lo in range(0, n_heads, 2):
        y = jnp.dot(h, w_ref[:, lo * HEAD_DIM:(lo + 2) * HEAD_DIM], preferred_element_type=jnp.float32)
        for i in range(lo, lo + 2):
            a = y[:, (i - lo) * HEAD_DIM:(i - lo + 1) * HEAD_DIM]
            if i >= n_q + n_kv:
                cols = slice((i - n_q - n_kv) * HEAD_DIM, (i - n_q - n_kv + 1) * HEAD_DIM)
                v_ref[:, cols] = a.astype(jnp.bfloat16)
                vt_ref[cols, :] = a.T.astype(jnp.bfloat16)
                continue
            r = (a * cos_t + pltpu.roll(a, HEAD_DIM // 2, 1) * sin_t).astype(jnp.bfloat16)
            if i < n_q:
                q_ref[i] = r
            else:
                k_ref[:, (i - n_q) * HEAD_DIM:(i - n_q + 1) * HEAD_DIM] = r


def qkv_call(h, w, cos_t, sin_t, n_q, n_kv):
    s, d = h.shape
    bm = min(512, s)
    n = w.shape[1]
    row = lambda i: (i, 0)
    return pl.pallas_call(
        functools.partial(qkv_kernel, n_q, n_kv),
        grid=(s // bm,),
        in_specs=[pl.BlockSpec((bm, d), row), pl.BlockSpec((d, n), lambda i: (0, 0), pipeline_mode=pl.Buffered(1)),
                  pl.BlockSpec((bm, HEAD_DIM), row), pl.BlockSpec((bm, HEAD_DIM), row)],
        out_specs=[pl.BlockSpec((n_q, bm, HEAD_DIM), lambda i: (0, i, 0)),
                   pl.BlockSpec((bm, n_kv * HEAD_DIM), row), pl.BlockSpec((bm, n_kv * HEAD_DIM), row),
                   pl.BlockSpec((n_kv * HEAD_DIM, bm), lambda i: (0, i))],
        out_shape=[jax.ShapeDtypeStruct((n_q, s, HEAD_DIM), jnp.bfloat16),
                   jax.ShapeDtypeStruct((s, n_kv * HEAD_DIM), jnp.bfloat16),
                   jax.ShapeDtypeStruct((s, n_kv * HEAD_DIM), jnp.bfloat16),
                   jax.ShapeDtypeStruct((n_kv * HEAD_DIM, s), jnp.bfloat16)],
        compiler_params=params(),
        cost_estimate=cost(2 * s * d * n, 2 * s * d + 2 * d * n + 2 * s * n),
        name="qkv",
    )(h, w, cos_t, sin_t)


def att_kernel(bq, bk, per, first, len_ref, q_ref, k_ref, vt_ref, o_ref, s_ref, p_ref, m_ref, l_ref, alpha_ref, acc_ref):
    row0 = first + pl.program_id(1) * bq
    valid = len_ref[0]
    last = k_ref.shape[0] // bk - 1
    m_ref[...] = jnp.full_like(m_ref, -jnp.inf)
    l_ref[...] = jnp.zeros_like(l_ref)
    alpha_ref[...] = jnp.zeros_like(alpha_ref)
    acc_ref[...] = jnp.zeros_like(acc_ref)
    p_ref[...] = jnp.zeros_like(p_ref)

    def scores(j, h):
        k_blk = k_ref[pl.ds(pl.multiple_of(j * bk, bk), bk), :]
        s_ref[h] = lax.dot_general(k_blk, q_ref[h], (((1,), (1,)), ((), ())), preferred_element_type=jnp.float32)

    def values(j, h):
        vt_blk = vt_ref[:, pl.ds(pl.multiple_of(j * bk, bk), bk)]
        acc_ref[h] = acc_ref[h] * alpha_ref[h] + jnp.dot(vt_blk, p_ref[h], preferred_element_type=jnp.float32)

    tall = min(32, bk)

    def softmax(j, h, masked):
        m_old = m_ref[h]
        m8 = None
        for c in range(bk // tall):
            r = slice(c * tall, (c + 1) * tall)
            sc = s_ref[h, r, :]
            if masked:
                kid = j * bk + c * tall + lax.broadcasted_iota(jnp.int32, (tall, bq), 0)
                qid = row0 + lax.broadcasted_iota(jnp.int32, (tall, bq), 1)
                sc = jnp.where((kid <= qid) & (kid < valid), sc, -jnp.inf)
                s_ref[h, r, :] = sc
            top = jnp.max(sc.reshape(tall // 8, 8, bq), axis=0)
            m8 = top if m8 is None else jnp.maximum(m8, top)
        m_new = jnp.maximum(m_old, jnp.max(m8, axis=0, keepdims=True))
        m_rows = jnp.broadcast_to(m_new, (8, bq))[None]
        l8 = None
        for c in range(bk // tall):
            r = slice(c * tall, (c + 1) * tall)
            p = jnp.exp2((s_ref[h, r, :].reshape(tall // 8, 8, bq) - m_rows) * EXP2_SCALE)
            tot = jnp.sum(p, axis=0)
            l8 = tot if l8 is None else l8 + tot
            p_ref[h, r, :] = p.reshape(tall, bq).astype(jnp.bfloat16)
        alpha = jnp.exp2((m_old - m_new) * EXP2_SCALE)
        l_ref[h] = l_ref[h] * alpha + jnp.sum(l8, axis=0, keepdims=True)
        alpha_ref[h] = alpha
        m_ref[h] = m_new

    def step(j, masked):
        for h in range(per):
            values(jnp.maximum(j - 1, 0), h)
            softmax(j, h, masked)
            scores(jnp.minimum(j + 1, last), h)

    n_full = jnp.minimum((row0 + 1) // bk, valid // bk)
    n_end = jnp.minimum((row0 + bq + bk - 1) // bk, (valid + bk - 1) // bk)

    def full(j, _):
        step(j, False)
        return 0

    def part(j, _):
        step(j, True)
        return 0

    for h in range(per):
        scores(0, h)
    lax.fori_loop(0, n_full, full, 0)
    lax.fori_loop(n_full, n_end, part, 0)
    for h in range(per):
        values(n_end - 1, h)
        o_ref[:, h * HEAD_DIM:(h + 1) * HEAD_DIM] = (acc_ref[h] / l_ref[h]).T.astype(jnp.bfloat16)


def att_call(q, k, vt, valid_len, call):
    n_q, s, _ = q.shape
    n_kv = k.shape[1] // HEAD_DIM
    per = n_q // n_kv
    rows = s // N_CALLS
    bq = min(512, rows)
    bk = min(512, s)
    first = call * rows
    off = first // bq
    frac = (2 * call + 1) / N_CALLS ** 2
    return pl.pallas_call(
        functools.partial(att_kernel, bq, bk, per, first),
        grid=(n_kv, rows // bq),
        in_specs=[pl.BlockSpec(memory_space=pltpu.SMEM),
                  pl.BlockSpec((per, bq, HEAD_DIM), lambda g, i: (g, off + i, 0)),
                  pl.BlockSpec((s, HEAD_DIM), lambda g, i: (0, g)),
                  pl.BlockSpec((HEAD_DIM, s), lambda g, i: (g, 0))],
        out_specs=pl.BlockSpec((bq, per * HEAD_DIM), lambda g, i: (i, g)),
        out_shape=jax.ShapeDtypeStruct((rows, n_q * HEAD_DIM), jnp.bfloat16),
        scratch_shapes=[pltpu.VMEM((per, bk, bq), jnp.float32), pltpu.VMEM((per, bk, bq), jnp.bfloat16)]
        + [pltpu.VMEM((per, 1, bq), jnp.float32)] * 3 + [pltpu.VMEM((per, HEAD_DIM, bq), jnp.float32)],
        compiler_params=params(),
        cost_estimate=cost(int(8 * frac * n_q * s * s * HEAD_DIM), 4 * n_q * s * HEAD_DIM),
        name="attention",
    )(valid_len, q, k, vt)


def out_kernel(n_src, idx_ref, *refs):
    o_refs = refs[:n_src]
    w_ref, x_ref, g_ref, r_ref, ua_ref, ub_ref, o_all, y_ref = refs[n_src:]
    ko = o_refs[0].shape[1]
    n = pl.program_id(0)
    bn = w_ref.shape[1]
    half = ua_ref.shape[0]

    @pl.when(n == 0)
    def _():
        for s in range(n_src):
            o_all[:, s * ko:(s + 1) * ko] = o_refs[s][...]

    acc = jnp.dot(o_all[...], w_ref[...], preferred_element_type=jnp.float32)
    col = pl.ds(pl.multiple_of(n * bn, bn), bn)
    y_ref[:, col] = (x_ref[:, col].astype(jnp.float32) + acc).astype(jnp.bfloat16)

    @pl.when(n == pl.num_programs(0) - 1)
    def _():
        r_ref[...] = y_ref[...]
        u = norm_rows(y_ref[...].astype(jnp.float32), g_ref[...].astype(jnp.float32))
        ua_ref[...] = u[:half]
        ub_ref[...] = u[half:]


def out_call(idx, o_pieces, w, x, gain):
    n_src = len(o_pieces)
    rows, ko = o_pieces[0].shape
    d = x.shape[1]
    bn = min(512, d)
    fixed = lambda n, idx: (0, 0)
    half = jax.ShapeDtypeStruct((rows // 2, d), jnp.bfloat16)
    return pl.pallas_call(
        functools.partial(out_kernel, n_src),
        grid_spec=pltpu.PrefetchScalarGridSpec(
            num_scalar_prefetch=1,
            grid=(d // bn,),
            in_specs=[pl.BlockSpec((rows, ko), fixed)] * n_src + [
                pl.BlockSpec((n_src * ko, bn), lambda n, idx: (0, n)),
                pl.BlockSpec((rows, d), lambda n, idx: (idx[0], 0)),
                pl.BlockSpec((1, d), fixed)],
            out_specs=[pl.BlockSpec((rows, d), fixed), pl.BlockSpec((rows // 2, d), fixed), pl.BlockSpec((rows // 2, d), fixed)],
            scratch_shapes=[pltpu.VMEM((rows, n_src * ko), jnp.bfloat16), pltpu.VMEM((rows, d), jnp.bfloat16)]),
        out_shape=[jax.ShapeDtypeStruct((rows, d), jnp.bfloat16), half, half],
        compiler_params=params(),
        cost_estimate=cost(2 * rows * d * ko * n_src, 2 * w.size + 8 * rows * d),
        name="w_out",
    )(idx, *o_pieces, w, x, gain)


def gu_kernel(bm, n_u, *refs):
    u_refs = refs[:n_u]
    g_ref, up_ref, a_ref, u_all, sem = refs[n_u:]
    rows = u_all.shape[0]
    piece = rows // n_u
    first = (pl.program_id(0) == 0) & (pl.program_id(1) == 0)
    copies = [pltpu.make_async_copy(u_refs[i], u_all.at[i * piece:(i + 1) * piece, :], sem.at[i]) for i in range(n_u)]

    @pl.when(first)
    def _():
        for c in copies:
            c.start()

    @pl.loop(0, rows // bm)
    def _(m):
        r = pl.ds(pl.multiple_of(m * bm, bm), bm)
        for i in range(n_u):
            @pl.when(first & (m == i * piece // bm))
            def _():
                copies[i].wait()
        u = u_all[r, :]
        gate = jnp.dot(u, g_ref[...], preferred_element_type=jnp.float32)
        up = jnp.dot(u, up_ref[...], preferred_element_type=jnp.float32)
        a_ref[r, :] = (jax.nn.silu(gate) * up).astype(jnp.bfloat16)


def gu_call(us, w, n_src):
    n_u = len(us)
    rows, d = us[0].shape
    rows *= n_u
    half = w.shape[1] // (2 * n_src)
    bn = math.gcd(256, half)
    nb = half // bn
    bm = min(512, rows)
    return pl.pallas_call(
        functools.partial(gu_kernel, bm, n_u),
        grid=(n_src, nb),
        in_specs=[pl.BlockSpec(memory_space=pl.ANY)] * n_u + [
            pl.BlockSpec((d, bn), lambda j, n: (0, 2 * j * nb + n)),
            pl.BlockSpec((d, bn), lambda j, n: (0, (2 * j + 1) * nb + n))],
        out_specs=pl.BlockSpec((rows, bn), lambda j, n: (0, j * nb + n)),
        out_shape=jax.ShapeDtypeStruct((rows, n_src * half), jnp.bfloat16),
        scratch_shapes=[pltpu.VMEM((rows, d), jnp.bfloat16), pltpu.SemaphoreType.DMA((n_u,))],
        compiler_params=params(),
        cost_estimate=cost(4 * rows * d * n_src * half, 2 * w.size + 2 * rows * d + 2 * rows * n_src * half),
        name="gate_up",
    )(*us, w, w)


def down_kernel(bm, parts, n_src, own, row0, meta_ref, *refs):
    a_any = refs[:parts]
    w_ref = refs[parts]
    rest = refs[parts + 1:]
    resid_any = rest[0] if own else None
    partials = rest[1:3] if own else ()
    outs = rest[3:4] if own else rest[:2]
    scratch = rest[4:] if own else rest[2:]
    a_refs, sem = scratch[:parts], scratch[parts]
    rows = a_refs[0].shape[0]
    n = pl.program_id(0)
    bn = w_ref.shape[1]
    kj = w_ref.shape[0] // n_src
    n_m = rows // bm
    copies = [[pltpu.make_async_copy(a_any[p].at[row0[p] + i * bm:row0[p] + (i + 1) * bm, :], a_refs[p].at[i * bm:(i + 1) * bm, :], sem.at[p, i])
               for p in range(parts)] for i in range(n_m)]
    more = []
    if own:
        r_ref, r_sem = scratch[parts + 1:]
        for q in range(r_ref.shape[1] // HEAD_DIM):
            col = pl.multiple_of(meta_ref[r_ref.shape[1] // bn + q] * HEAD_DIM, HEAD_DIM)
            more.append(pltpu.make_async_copy(resid_any.at[:, pl.ds(col, HEAD_DIM)], r_ref.at[:, q * HEAD_DIM:(q + 1) * HEAD_DIM], r_sem.at[q]))

    @pl.when(n == 0)
    def _():
        for c in sum(copies, []) + more:
            c.start()

    @pl.loop(0, n_m)
    def _(m):
        for i in range(n_m):
            @pl.when((n == 0) & (m == i))
            def _():
                for c in copies[i]:
                    c.wait()
        r = pl.ds(pl.multiple_of(m * bm, bm), bm)
        acc = None
        for j in range(n_src):
            k0 = j * kj
            for p in range(parts):
                kp = a_refs[p].shape[1] // n_src
                part = jnp.dot(a_refs[p][r, j * kp:(j + 1) * kp], w_ref[k0:k0 + kp, :], preferred_element_type=jnp.float32)
                acc = part if acc is None else acc + part
                k0 += kp
        half = bm // 2
        if own:
            @pl.when((n == 0) & (m == 0))
            def _():
                for c in more:
                    c.wait()

            cols = pl.ds(pl.multiple_of(n * bn, bn), bn)
            for h in range(2):
                rr = slice(h * half, (h + 1) * half)
                part = acc[rr] + partials[h][...].astype(jnp.float32)
                outs[0][rr, :] = (r_ref[rr, cols].astype(jnp.float32) + part).astype(jnp.bfloat16)
        else:
            out = pl.ds(pl.multiple_of(m * half, half), half)
            for h in range(2):
                outs[h][out, :] = acc[h * half:(h + 1) * half].astype(jnp.bfloat16)


def down_call(a_parts, w, meta, n_src, bn, steps, rows, call=0, resid=None, partials=()):
    parts = len(a_parts)
    cols = steps * bn
    own = resid is not None
    half = rows // 2
    bm = rows if own else rows // N_CALLS
    step = lambda n, meta: (0, n)
    anywhere = pl.BlockSpec(memory_space=pl.ANY)
    args = [*a_parts, w]
    in_specs = [anywhere] * parts + [pl.BlockSpec((w.shape[0], bn), lambda n, meta: (0, meta[n]))]
    scratch = [pltpu.VMEM((rows, a.shape[1]), jnp.bfloat16) for a in a_parts] + [pltpu.SemaphoreType.DMA((parts, rows // bm))]
    if own:
        args += [resid, *partials]
        in_specs += [anywhere] + [pl.BlockSpec((half, bn), lambda n, meta: (call, n))] * 2
        scratch += [pltpu.VMEM((rows, cols), jnp.bfloat16), pltpu.SemaphoreType.DMA((cols // HEAD_DIM,))]
    n_out = 1 if own else 2
    row0 = tuple(call * rows if a.shape[0] > rows else 0 for a in a_parts)
    return pl.pallas_call(
        functools.partial(down_kernel, bm, parts, n_src, own, row0),
        grid_spec=pltpu.PrefetchScalarGridSpec(
            num_scalar_prefetch=1, grid=(steps,), in_specs=in_specs, out_specs=[pl.BlockSpec((rows // n_out, bn), step)] * n_out,
            scratch_shapes=scratch),
        out_shape=[jax.ShapeDtypeStruct((rows // n_out, cols), jnp.bfloat16)] * n_out,
        compiler_params=params(),
        cost_estimate=cost(2 * rows * cols * w.shape[0], 2 * w.size + 4 * rows * cols),
        name="down",
    )(meta, *args)


def place_kernel(n_in, moves, n_tp, skip, idx_ref, *refs):
    ins = refs[:n_in]
    out_ref, sem = refs[-2:]
    copies = []
    for i, src_row, rows, call, who in moves:
        row = pl.multiple_of((call * n_tp + idx_ref[who]) * rows, rows)
        for q in range(ins[i].shape[1] // HEAD_DIM):
            col = pl.multiple_of(idx_ref[n_tp + skip + q] * HEAD_DIM, HEAD_DIM)
            copies.append(pltpu.make_async_copy(
                ins[i].at[src_row:src_row + rows, q * HEAD_DIM:(q + 1) * HEAD_DIM],
                out_ref.at[pl.ds(row, rows), pl.ds(col, HEAD_DIM)],
                sem.at[len(copies)]))
    for c in copies:
        c.start()
    for c in copies:
        c.wait()


def place_call(idx, pieces, moves, shape, n_tp, skip, out):
    n_in = len(pieces)
    args = list(pieces)
    in_specs = [pl.BlockSpec(p.shape, lambda *_: (0, 0)) for p in pieces]
    aliases = {}
    if out is not None:
        args.append(out)
        in_specs.append(pl.BlockSpec(memory_space=pl.ANY))
        aliases = {n_in + 1: 0}
    n_copies = sum(pieces[m[0]].shape[1] // HEAD_DIM for m in moves)
    return pl.pallas_call(
        functools.partial(place_kernel, n_in, moves, n_tp, skip),
        grid_spec=pltpu.PrefetchScalarGridSpec(
            num_scalar_prefetch=1, grid=(1,), in_specs=in_specs, out_specs=pl.BlockSpec(memory_space=pl.ANY),
            scratch_shapes=[pltpu.SemaphoreType.DMA((n_copies,))]),
        out_shape=jax.ShapeDtypeStruct(shape, jnp.bfloat16),
        input_output_aliases=aliases,
        compiler_params=params(),
        cost_estimate=cost(1000000, 4 * sum(p.size for p in pieces)),
        name="place",
    )(idx, *args)


def after(val, *deps):
    return lax.optimization_barrier((val, *deps))[0]


def solution(mesh):
    n_tp = mesh.shape['tp']
    n_fs = mesh.shape['fsdp']
    mesh2 = Mesh(mesh.devices.reshape(mesh.shape['dp'], n_tp // 2, 2, n_fs), ('dp', 'ta', 'tb', 'fsdp'))
    tp = ('ta', 'tb')
    batch_axes = ('dp', 'fsdp')
    in_specs = (P(batch_axes, None, None), P(batch_axes, None), P(batch_axes),
                P('fsdp', tp), P('fsdp', tp), P('fsdp', tp), P(tp, 'fsdp'),
                P('fsdp', tp), P('fsdp', tp), P(tp, 'fsdp'), P(None), P(None))
    out_specs = (P(batch_axes, None, None), P(batch_axes, None, tp, None), P(batch_axes, None, tp, None))

    def shift(val, s):
        return lax.ppermute(val, tp, [(i, (i + s) % n_tp) for i in range(n_tp)])

    def local_layer(tokens, positions, valid_len, w_query, w_key, w_value, w_out, w_gate, w_up, w_down, norm_attn, norm_mlp):
        _, seq, d = tokens.shape
        x = tokens.reshape(seq, d)
        n_q = w_query.shape[1] // HEAD_DIM
        n_kv = w_key.shape[1] // HEAD_DIM
        sub = seq // (n_tp * N_CALLS)
        me = lax.axis_index(tp)

        w_qkv = lax.all_gather(jnp.concatenate([w_query, w_key, w_value], axis=1), 'fsdp', axis=0, tiled=True)
        rounds = []
        for s in range(1, n_tp):
            rounds.append(shift(w_out, s))
        full_o = lax.all_gather(jnp.concatenate([w_out, *rounds], axis=0), 'fsdp', axis=1, tiled=True)
        fl = w_gate.shape[1]
        n_src = 2
        swaps = []
        lead = fl * 5 // 8
        for cut in (slice(0, lead), slice(lead, fl)):
            local = jnp.concatenate([w_gate[:, cut], w_up[:, cut]], axis=1)
            swaps.append((local, shift(local, 2)))
        swaps.append((w_down, shift(w_down, 2)))

        def joined(p, axis, *deps):
            return jnp.concatenate([after(swaps[p][0], *deps), swaps[p][1]], axis=axis)

        angles = positions.reshape(seq, 1).astype(jnp.float32) * rope_freqs()[None, :]
        cos_h, sin_h = jnp.cos(angles), jnp.sin(angles)
        cos_t = jnp.concatenate([cos_h, cos_h], axis=1)
        sin_t = jnp.concatenate([-sin_h, sin_h], axis=1)
        h = norm_call(x, norm_attn.reshape(1, d))
        q, k, v, vt = qkv_call(h, w_qkv, cos_t, sin_t, n_q, n_kv)

        pieces = []
        gu_parts = []
        o = q
        for call in range(N_CALLS):
            gu_parts.append(joined(call, 1, o))
            o = att_call(after(q, gu_parts[call], o), k, vt, valid_len, call)
            got = []
            for s in range(n_tp):
                blk = lax.dynamic_slice_in_dim(o, (me + s) % n_tp * sub, sub, axis=0)
                if s:
                    blk = shift(blk, s)
                got.append(blk)
            pieces.append(got)
        d_part = joined(2, 0, o)
        gu_full = [lax.all_gather(w, 'fsdp', axis=0, tiled=True) for w in gu_parts]
        n_blk = w_down.shape[1] // HEAD_DIM
        d_pair = lax.ppermute(d_part, 'fsdp', [(i, i ^ 1) for i in range(n_fs)])
        d_near = jnp.concatenate([d_part, d_pair], axis=1)
        d_full = [lax.all_gather(d_part[:, b * HEAD_DIM:(b + 1) * HEAD_DIM], 'fsdp', axis=1, tiled=True) for b in range(n_blk)]

        resid, u_own, u_prev, u_next = [], [], [], []
        order = d_part
        for call in range(N_CALLS):
            got = pieces[call]
            got[0] = after(got[0], order)
            row = (call * n_tp + me).reshape(1).astype(jnp.int32)
            r, ua, ub = out_call(row, got, full_o, x, norm_mlp.reshape(1, d))
            order = r
            resid.append(r)
            u_own += [ua, ub]
            u_prev.append(shift(ua, 1))
            u_next.append(shift(ub, -1))
        u_recv = [u_prev[0], u_next[0], u_prev[1], u_next[1]]

        def gate_up(p, us, dep):
            return gu_call([after(us[0], dep)] + us[1:], gu_full[p], n_src)

        a_own = gate_up(0, u_own, resid[-1])
        a_recv = [gate_up(0, u_recv, a_own)]
        a_recv.append(gate_up(1, u_recv, a_recv[0]))
        a_late = []

        fs = lax.axis_index('fsdp')
        chip, n_chip = fs // 2, n_fs // 2
        others = [(chip + 1 + i) % n_chip for i in range(n_chip - 1)]
        bn = 2 * HEAD_DIM
        blocks = [(d_near, list(range(n_blk)), [fs * n_blk + i for i in range(n_blk)] + [(fs ^ 1) * n_blk + i for i in range(n_blk)])]
        for b in range(n_blk):
            units = sum(([2 * o_ * n_blk + b, (2 * o_ + 1) * n_blk + b] for o_ in others), [])
            blocks.append((d_full[b], others, units))
        idx = jnp.stack([jnp.asarray(v, jnp.int32) for v in [(me - s) % n_tp for s in range(n_tp)] + sum((u for _, _, u in blocks), [])])
        near_moves = [(i * N_CALLS + c, 0, sub, c, who) for i, who in enumerate((0, 1, n_tp - 1)) for c in range(N_CALLS)]
        far_moves = [(0, 0, sub, 0, 2), (1, 0, sub, N_CALLS - 1, 2)]
        skip = [sum(len(u) for _, _, u in blocks[:b]) for b in range(len(blocks))]
        last = len(blocks) - 1
        mine, far = [], []

        def place_near(b, out, *deps):
            m, near = mine[b]
            pieces = [*m, *(near[g, c] for g in range(2) for c in range(N_CALLS))]
            pieces[0] = after(pieces[0], *deps)
            return place_call(idx, pieces, near_moves, (seq, d), n_tp, skip[b], out)

        def place_far(b, out):
            return place_call(idx, far[b], far_moves, (seq, d), n_tp, skip[b], out)

        def relay(b, *deps):
            near = mine[b][1]
            far_0 = shift(after(near[0, 0], *deps), 1)
            far_1 = shift(after(near[1, N_CALLS - 1], *deps), -1)
            far.append((far_0, far_1))

        order = a_recv[1]
        hidden = None
        for b, (w, sel, units) in enumerate(blocks):
            meta = jnp.stack([jnp.asarray(v, jnp.int32) for v in [*sel, *units]])
            p_prev, p_next = down_call([after(a_recv[0], order), a_recv[1]], w, meta, n_src, bn, len(sel), N_CALLS * sub)
            b_next = shift(p_prev, -1)
            b_prev = shift(p_next, 1)
            order = p_prev
            if b >= 1:
                relay(b - 1)
            if b >= 2:
                hidden = place_far(b - 2, place_near(b - 2, hidden, order))
                order = hidden
            m, near = [], {}
            for c in range(N_CALLS):
                if b == 0:
                    a_late.append(gate_up(1, u_own[2 * c:2 * c + 2], order))
                    order = a_late[c]
                m += down_call([after(a_own, order), a_late[c]], w, meta, n_src, bn, len(sel), sub, c, resid[c], (b_next, b_prev))
                order = m[c]
                for g, by in enumerate((1, -1)):
                    near[g, c] = shift(m[c], by)
            mine.append((m, near))
        hidden = place_far(last - 1, place_near(last - 1, hidden, order))
        relay(last, hidden)
        hidden = place_far(last, place_near(last, hidden))
        hidden = hidden.reshape(1, seq, d)
        return hidden, k.reshape(1, seq, n_kv, HEAD_DIM), v.reshape(1, seq, n_kv, HEAD_DIM)


    return jax.shard_map(local_layer, mesh=mesh2, in_specs=in_specs, out_specs=out_specs, check_vma=False)
```

```python
import functools
import math
import jax
import jax.numpy as jnp
from jax import lax
from jax.experimental import pallas as pl
from jax.experimental.pallas import tpu as pltpu
from jax.sharding import Mesh, PartitionSpec as P


HEAD_DIM = 128
ROPE_THETA = 500000.0
NORM_EPS = 1e-5
EXP2_SCALE = HEAD_DIM ** -0.5 * math.log2(math.e)
N_CALLS = 2
VMEM_LIMIT = 67043328


def rope_freqs():
    half_idx = jnp.arange(HEAD_DIM // 2, dtype=jnp.float32)
    inv_freq = jnp.power(ROPE_THETA, -2.0 * half_idx / HEAD_DIM)
    wave_len = 2.0 * math.pi / inv_freq
    smooth = (8192.0 / wave_len - 1.0) / 3.0
    blended = (1.0 - smooth) * inv_freq / 8.0 + smooth * inv_freq
    return jnp.where(wave_len < 2048.0, inv_freq, jnp.where(wave_len > 8192.0, inv_freq / 8.0, blended))


def params(**kw):
    return pltpu.CompilerParams(vmem_limit_bytes=VMEM_LIMIT, **kw)


def cost(flops, nbytes):
    return pl.CostEstimate(flops=flops, bytes_accessed=nbytes, transcendentals=0)


def norm_rows(vals_f32, gain):
    inv = lax.rsqrt(jnp.mean(vals_f32 * vals_f32, axis=-1, keepdims=True) + NORM_EPS)
    return (vals_f32 * inv * gain).astype(jnp.bfloat16)


def norm_kernel(x_ref, g_ref, h_ref):
    h_ref[...] = norm_rows(x_ref[...].astype(jnp.float32), g_ref[...].astype(jnp.float32))


def norm_call(x, gain):
    s, d = x.shape
    bm = min(512, s)
    return pl.pallas_call(
        norm_kernel,
        grid=(s // bm,),
        in_specs=[pl.BlockSpec((bm, d), lambda i: (i, 0)), pl.BlockSpec((1, d), lambda i: (0, 0))],
        out_specs=pl.BlockSpec((bm, d), lambda i: (i, 0)),
        out_shape=jax.ShapeDtypeStruct((s, d), jnp.bfloat16),
        compiler_params=params(),
        cost_estimate=cost(8 * s * d, 4 * s * d),
        name="norm",
    )(x, gain)


def qkv_kernel(n_q, n_kv, h_ref, w_ref, cos_ref, sin_ref, q_ref, k_ref, v_ref, vt_ref):
    h = h_ref[...]
    cos_t, sin_t = cos_ref[...], sin_ref[...]
    n_heads = n_q + 2 * n_kv
    for lo in range(0, n_heads, 2):
        y = jnp.dot(h, w_ref[:, lo * HEAD_DIM:(lo + 2) * HEAD_DIM], preferred_element_type=jnp.float32)
        for i in range(lo, lo + 2):
            a = y[:, (i - lo) * HEAD_DIM:(i - lo + 1) * HEAD_DIM]
            if i >= n_q + n_kv:
                cols = slice((i - n_q - n_kv) * HEAD_DIM, (i - n_q - n_kv + 1) * HEAD_DIM)
                v_ref[:, cols] = a.astype(jnp.bfloat16)
                vt_ref[cols, :] = a.T.astype(jnp.bfloat16)
                continue
            r = (a * cos_t + pltpu.roll(a, HEAD_DIM // 2, 1) * sin_t).astype(jnp.bfloat16)
            if i < n_q:
                q_ref[i] = r
            else:
                k_ref[:, (i - n_q) * HEAD_DIM:(i - n_q + 1) * HEAD_DIM] = r


def qkv_call(h, w, cos_t, sin_t, n_q, n_kv):
    s, d = h.shape
    bm = min(512, s)
    n = w.shape[1]
    row = lambda i: (i, 0)
    return pl.pallas_call(
        functools.partial(qkv_kernel, n_q, n_kv),
        grid=(s // bm,),
        in_specs=[pl.BlockSpec((bm, d), row), pl.BlockSpec((d, n), lambda i: (0, 0), pipeline_mode=pl.Buffered(1)),
                  pl.BlockSpec((bm, HEAD_DIM), row), pl.BlockSpec((bm, HEAD_DIM), row)],
        out_specs=[pl.BlockSpec((n_q, bm, HEAD_DIM), lambda i: (0, i, 0)),
                   pl.BlockSpec((bm, n_kv * HEAD_DIM), row), pl.BlockSpec((bm, n_kv * HEAD_DIM), row),
                   pl.BlockSpec((n_kv * HEAD_DIM, bm), lambda i: (0, i))],
        out_shape=[jax.ShapeDtypeStruct((n_q, s, HEAD_DIM), jnp.bfloat16),
                   jax.ShapeDtypeStruct((s, n_kv * HEAD_DIM), jnp.bfloat16),
                   jax.ShapeDtypeStruct((s, n_kv * HEAD_DIM), jnp.bfloat16),
                   jax.ShapeDtypeStruct((n_kv * HEAD_DIM, s), jnp.bfloat16)],
        compiler_params=params(),
        cost_estimate=cost(2 * s * d * n, 2 * s * d + 2 * d * n + 2 * s * n),
        name="qkv",
    )(h, w, cos_t, sin_t)


def att_kernel(bq, bk, per, first, len_ref, q_ref, k_ref, vt_ref, o_ref, s_ref, p_ref, m_ref, l_ref, alpha_ref, acc_ref):
    row0 = first + pl.program_id(1) * bq
    valid = len_ref[0]
    last = k_ref.shape[0] // bk - 1
    m_ref[...] = jnp.full_like(m_ref, -jnp.inf)
    l_ref[...] = jnp.zeros_like(l_ref)
    alpha_ref[...] = jnp.zeros_like(alpha_ref)
    acc_ref[...] = jnp.zeros_like(acc_ref)
    p_ref[...] = jnp.zeros_like(p_ref)

    def scores(j, h):
        k_blk = k_ref[pl.ds(pl.multiple_of(j * bk, bk), bk), :]
        s_ref[h] = lax.dot_general(k_blk, q_ref[h], (((1,), (1,)), ((), ())), preferred_element_type=jnp.float32)

    def values(j, h):
        vt_blk = vt_ref[:, pl.ds(pl.multiple_of(j * bk, bk), bk)]
        acc_ref[h] = acc_ref[h] * alpha_ref[h] + jnp.dot(vt_blk, p_ref[h], preferred_element_type=jnp.float32)

    tall = min(32, bk)

    def softmax(j, h, masked):
        m_old = m_ref[h]
        m8 = None
        for c in range(bk // tall):
            r = slice(c * tall, (c + 1) * tall)
            sc = s_ref[h, r, :]
            if masked:
                kid = j * bk + c * tall + lax.broadcasted_iota(jnp.int32, (tall, bq), 0)
                qid = row0 + lax.broadcasted_iota(jnp.int32, (tall, bq), 1)
                sc = jnp.where((kid <= qid) & (kid < valid), sc, -jnp.inf)
                s_ref[h, r, :] = sc
            top = jnp.max(sc.reshape(tall // 8, 8, bq), axis=0)
            m8 = top if m8 is None else jnp.maximum(m8, top)
        m_new = jnp.maximum(m_old, jnp.max(m8, axis=0, keepdims=True))
        m_rows = jnp.broadcast_to(m_new, (8, bq))[None]
        l8 = None
        for c in range(bk // tall):
            r = slice(c * tall, (c + 1) * tall)
            p = jnp.exp2((s_ref[h, r, :].reshape(tall // 8, 8, bq) - m_rows) * EXP2_SCALE)
            tot = jnp.sum(p, axis=0)
            l8 = tot if l8 is None else l8 + tot
            p_ref[h, r, :] = p.reshape(tall, bq).astype(jnp.bfloat16)
        alpha = jnp.exp2((m_old - m_new) * EXP2_SCALE)
        l_ref[h] = l_ref[h] * alpha + jnp.sum(l8, axis=0, keepdims=True)
        alpha_ref[h] = alpha
        m_ref[h] = m_new

    def step(j, masked):
        for h in range(per):
            values(jnp.maximum(j - 1, 0), h)
            softmax(j, h, masked)
            scores(jnp.minimum(j + 1, last), h)

    n_full = jnp.minimum((row0 + 1) // bk, valid // bk)
    n_end = jnp.minimum((row0 + bq + bk - 1) // bk, (valid + bk - 1) // bk)

    def full(j, _):
        step(j, False)
        return 0

    def part(j, _):
        step(j, True)
        return 0

    for h in range(per):
        scores(0, h)
    lax.fori_loop(0, n_full, full, 0)
    lax.fori_loop(n_full, n_end, part, 0)
    for h in range(per):
        values(n_end - 1, h)
        o_ref[:, h * HEAD_DIM:(h + 1) * HEAD_DIM] = (acc_ref[h] / l_ref[h]).T.astype(jnp.bfloat16)


def att_call(q, k, vt, valid_len, call):
    n_q, s, _ = q.shape
    n_kv = k.shape[1] // HEAD_DIM
    per = n_q // n_kv
    rows = s // N_CALLS
    bq = min(512, rows)
    bk = min(512, s)
    first = call * rows
    off = first // bq
    frac = (2 * call + 1) / N_CALLS ** 2
    return pl.pallas_call(
        functools.partial(att_kernel, bq, bk, per, first),
        grid=(n_kv, rows // bq),
        in_specs=[pl.BlockSpec(memory_space=pltpu.SMEM),
                  pl.BlockSpec((per, bq, HEAD_DIM), lambda g, i: (g, off + i, 0)),
                  pl.BlockSpec((s, HEAD_DIM), lambda g, i: (0, g)),
                  pl.BlockSpec((HEAD_DIM, s), lambda g, i: (g, 0))],
        out_specs=pl.BlockSpec((bq, per * HEAD_DIM), lambda g, i: (i, g)),
        out_shape=jax.ShapeDtypeStruct((rows, n_q * HEAD_DIM), jnp.bfloat16),
        scratch_shapes=[pltpu.VMEM((per, bk, bq), jnp.float32), pltpu.VMEM((per, bk, bq), jnp.bfloat16)]
        + [pltpu.VMEM((per, 1, bq), jnp.float32)] * 3 + [pltpu.VMEM((per, HEAD_DIM, bq), jnp.float32)],
        compiler_params=params(),
        cost_estimate=cost(int(8 * frac * n_q * s * s * HEAD_DIM), 4 * n_q * s * HEAD_DIM),
        name="attention",
    )(valid_len, q, k, vt)


def out_kernel(n_src, idx_ref, *refs):
    o_refs = refs[:n_src]
    w_ref, x_ref, g_ref, r_ref, ua_ref, ub_ref, o_all, y_ref = refs[n_src:]
    ko = o_refs[0].shape[1]
    n = pl.program_id(0)
    bn = w_ref.shape[1]
    half = ua_ref.shape[0]

    @pl.when(n == 0)
    def _():
        for s in range(n_src):
            o_all[:, s * ko:(s + 1) * ko] = o_refs[s][...]

    acc = jnp.dot(o_all[...], w_ref[...], preferred_element_type=jnp.float32)
    col = pl.ds(pl.multiple_of(n * bn, bn), bn)
    y_ref[:, col] = (x_ref[:, col].astype(jnp.float32) + acc).astype(jnp.bfloat16)

    @pl.when(n == pl.num_programs(0) - 1)
    def _():
        r_ref[...] = y_ref[...]
        u = norm_rows(y_ref[...].astype(jnp.float32), g_ref[...].astype(jnp.float32))
        ua_ref[...] = u[:half]
        ub_ref[...] = u[half:]


def out_call(idx, o_pieces, w, x, gain):
    n_src = len(o_pieces)
    rows, ko = o_pieces[0].shape
    d = x.shape[1]
    bn = min(512, d)
    fixed = lambda n, idx: (0, 0)
    half = jax.ShapeDtypeStruct((rows // 2, d), jnp.bfloat16)
    return pl.pallas_call(
        functools.partial(out_kernel, n_src),
        grid_spec=pltpu.PrefetchScalarGridSpec(
            num_scalar_prefetch=1,
            grid=(d // bn,),
            in_specs=[pl.BlockSpec((rows, ko), fixed)] * n_src + [
                pl.BlockSpec((n_src * ko, bn), lambda n, idx: (0, n)),
                pl.BlockSpec((rows, d), lambda n, idx: (idx[0], 0)),
                pl.BlockSpec((1, d), fixed)],
            out_specs=[pl.BlockSpec((rows, d), fixed), pl.BlockSpec((rows // 2, d), fixed), pl.BlockSpec((rows // 2, d), fixed)],
            scratch_shapes=[pltpu.VMEM((rows, n_src * ko), jnp.bfloat16), pltpu.VMEM((rows, d), jnp.bfloat16)]),
        out_shape=[jax.ShapeDtypeStruct((rows, d), jnp.bfloat16), half, half],
        compiler_params=params(),
        cost_estimate=cost(2 * rows * d * ko * n_src, 2 * w.size + 8 * rows * d),
        name="w_out",
    )(idx, *o_pieces, w, x, gain)


def gu_kernel(bm, n_u, *refs):
    u_refs = refs[:n_u]
    g_ref, up_ref, a_ref, u_all, sem = refs[n_u:]
    rows = u_all.shape[0]
    piece = rows // n_u
    first = (pl.program_id(0) == 0) & (pl.program_id(1) == 0)
    copies = [pltpu.make_async_copy(u_refs[i], u_all.at[i * piece:(i + 1) * piece, :], sem.at[i]) for i in range(n_u)]

    @pl.when(first)
    def _():
        for c in copies:
            c.start()

    @pl.loop(0, rows // bm)
    def _(m):
        r = pl.ds(pl.multiple_of(m * bm, bm), bm)
        for i in range(n_u):
            @pl.when(first & (m == i * piece // bm))
            def _():
                copies[i].wait()
        u = u_all[r, :]
        gate = jnp.dot(u, g_ref[...], preferred_element_type=jnp.float32)
        up = jnp.dot(u, up_ref[...], preferred_element_type=jnp.float32)
        a_ref[r, :] = (jax.nn.silu(gate) * up).astype(jnp.bfloat16)


def gu_call(us, w, n_src):
    n_u = len(us)
    rows, d = us[0].shape
    rows *= n_u
    half = w.shape[1] // (2 * n_src)
    bn = math.gcd(256, half)
    nb = half // bn
    bm = min(512, rows)
    return pl.pallas_call(
        functools.partial(gu_kernel, bm, n_u),
        grid=(n_src, nb),
        in_specs=[pl.BlockSpec(memory_space=pl.ANY)] * n_u + [
            pl.BlockSpec((d, bn), lambda j, n: (0, 2 * j * nb + n)),
            pl.BlockSpec((d, bn), lambda j, n: (0, (2 * j + 1) * nb + n))],
        out_specs=pl.BlockSpec((rows, bn), lambda j, n: (0, j * nb + n)),
        out_shape=jax.ShapeDtypeStruct((rows, n_src * half), jnp.bfloat16),
        scratch_shapes=[pltpu.VMEM((rows, d), jnp.bfloat16), pltpu.SemaphoreType.DMA((n_u,))],
        compiler_params=params(),
        cost_estimate=cost(4 * rows * d * n_src * half, 2 * w.size + 2 * rows * d + 2 * rows * n_src * half),
        name="gate_up",
    )(*us, w, w)


def down_kernel(bm, parts, n_src, own, row0, meta_ref, *refs):
    a_any = refs[:parts]
    w_ref = refs[parts]
    rest = refs[parts + 1:]
    resid_any = rest[0] if own else None
    partials = rest[1:3] if own else ()
    outs = rest[3:4] if own else rest[:2]
    scratch = rest[4:] if own else rest[2:]
    a_refs, sem = scratch[:parts], scratch[parts]
    rows = a_refs[0].shape[0]
    n = pl.program_id(0)
    bn = w_ref.shape[1]
    kj = w_ref.shape[0] // n_src
    n_m = rows // bm
    copies = [[pltpu.make_async_copy(a_any[p].at[row0[p] + i * bm:row0[p] + (i + 1) * bm, :], a_refs[p].at[i * bm:(i + 1) * bm, :], sem.at[p, i])
               for p in range(parts)] for i in range(n_m)]
    more = []
    if own:
        r_ref, r_sem = scratch[parts + 1:]
        for q in range(r_ref.shape[1] // HEAD_DIM):
            col = pl.multiple_of(meta_ref[r_ref.shape[1] // bn + q] * HEAD_DIM, HEAD_DIM)
            more.append(pltpu.make_async_copy(resid_any.at[:, pl.ds(col, HEAD_DIM)], r_ref.at[:, q * HEAD_DIM:(q + 1) * HEAD_DIM], r_sem.at[q]))

    @pl.when(n == 0)
    def _():
        for c in sum(copies, []) + more:
            c.start()

    @pl.loop(0, n_m)
    def _(m):
        for i in range(n_m):
            @pl.when((n == 0) & (m == i))
            def _():
                for c in copies[i]:
                    c.wait()
        r = pl.ds(pl.multiple_of(m * bm, bm), bm)
        acc = None
        for j in range(n_src):
            k0 = j * kj
            for p in range(parts):
                kp = a_refs[p].shape[1] // n_src
                part = jnp.dot(a_refs[p][r, j * kp:(j + 1) * kp], w_ref[k0:k0 + kp, :], preferred_element_type=jnp.float32)
                acc = part if acc is None else acc + part
                k0 += kp
        half = bm // 2
        if own:
            @pl.when((n == 0) & (m == 0))
            def _():
                for c in more:
                    c.wait()

            cols = pl.ds(pl.multiple_of(n * bn, bn), bn)
            for h in range(2):
                rr = slice(h * half, (h + 1) * half)
                part = acc[rr] + partials[h][...].astype(jnp.float32)
                outs[0][rr, :] = (r_ref[rr, cols].astype(jnp.float32) + part).astype(jnp.bfloat16)
        else:
            out = pl.ds(pl.multiple_of(m * half, half), half)
            for h in range(2):
                outs[h][out, :] = acc[h * half:(h + 1) * half].astype(jnp.bfloat16)


def down_call(a_parts, w, meta, n_src, bn, steps, rows, call=0, resid=None, partials=()):
    parts = len(a_parts)
    cols = steps * bn
    own = resid is not None
    half = rows // 2
    bm = rows if own else rows // N_CALLS
    step = lambda n, meta: (0, n)
    anywhere = pl.BlockSpec(memory_space=pl.ANY)
    args = [*a_parts, w]
    in_specs = [anywhere] * parts + [pl.BlockSpec((w.shape[0], bn), lambda n, meta: (0, meta[n]))]
    scratch = [pltpu.VMEM((rows, a.shape[1]), jnp.bfloat16) for a in a_parts] + [pltpu.SemaphoreType.DMA((parts, rows // bm))]
    if own:
        args += [resid, *partials]
        in_specs += [anywhere] + [pl.BlockSpec((half, bn), lambda n, meta: (call, n))] * 2
        scratch += [pltpu.VMEM((rows, cols), jnp.bfloat16), pltpu.SemaphoreType.DMA((cols // HEAD_DIM,))]
    n_out = 1 if own else 2
    row0 = tuple(call * rows if a.shape[0] > rows else 0 for a in a_parts)
    return pl.pallas_call(
        functools.partial(down_kernel, bm, parts, n_src, own, row0),
        grid_spec=pltpu.PrefetchScalarGridSpec(
            num_scalar_prefetch=1, grid=(steps,), in_specs=in_specs, out_specs=[pl.BlockSpec((rows // n_out, bn), step)] * n_out,
            scratch_shapes=scratch),
        out_shape=[jax.ShapeDtypeStruct((rows // n_out, cols), jnp.bfloat16)] * n_out,
        compiler_params=params(),
        cost_estimate=cost(2 * rows * cols * w.shape[0], 2 * w.size + 4 * rows * cols),
        name="down",
    )(meta, *args)


def place_kernel(n_in, moves, n_tp, skip, idx_ref, *refs):
    ins = refs[:n_in]
    out_ref, sem = refs[-2:]
    copies = []
    for i, src_row, rows, call, who in moves:
        row = pl.multiple_of((call * n_tp + idx_ref[who]) * rows, rows)
        for q in range(ins[i].shape[1] // HEAD_DIM):
            col = pl.multiple_of(idx_ref[n_tp + skip + q] * HEAD_DIM, HEAD_DIM)
            copies.append(pltpu.make_async_copy(
                ins[i].at[src_row:src_row + rows, q * HEAD_DIM:(q + 1) * HEAD_DIM],
                out_ref.at[pl.ds(row, rows), pl.ds(col, HEAD_DIM)],
                sem.at[len(copies)]))
    for c in copies:
        c.start()
    for c in copies:
        c.wait()


def place_call(idx, pieces, moves, shape, n_tp, skip, out):
    n_in = len(pieces)
    args = list(pieces)
    in_specs = [pl.BlockSpec(p.shape, lambda *_: (0, 0)) for p in pieces]
    aliases = {}
    if out is not None:
        args.append(out)
        in_specs.append(pl.BlockSpec(memory_space=pl.ANY))
        aliases = {n_in + 1: 0}
    n_copies = sum(pieces[m[0]].shape[1] // HEAD_DIM for m in moves)
    return pl.pallas_call(
        functools.partial(place_kernel, n_in, moves, n_tp, skip),
        grid_spec=pltpu.PrefetchScalarGridSpec(
            num_scalar_prefetch=1, grid=(1,), in_specs=in_specs, out_specs=pl.BlockSpec(memory_space=pl.ANY),
            scratch_shapes=[pltpu.SemaphoreType.DMA((n_copies,))]),
        out_shape=jax.ShapeDtypeStruct(shape, jnp.bfloat16),
        input_output_aliases=aliases,
        compiler_params=params(),
        cost_estimate=cost(1000000, 4 * sum(p.size for p in pieces)),
        name="place",
    )(idx, *args)


def after(val, *deps):
    return lax.optimization_barrier((val, *deps))[0]


def solution(mesh):
    n_tp = mesh.shape['tp']
    n_fs = mesh.shape['fsdp']
    mesh2 = Mesh(mesh.devices.reshape(mesh.shape['dp'], n_tp // 2, 2, n_fs), ('dp', 'ta', 'tb', 'fsdp'))
    tp = ('ta', 'tb')
    batch_axes = ('dp', 'fsdp')
    in_specs = (P(batch_axes, None, None), P(batch_axes, None), P(batch_axes),
                P('fsdp', tp), P('fsdp', tp), P('fsdp', tp), P(tp, 'fsdp'),
                P('fsdp', tp), P('fsdp', tp), P(tp, 'fsdp'), P(None), P(None))
    out_specs = (P(batch_axes, None, None), P(batch_axes, None, tp, None), P(batch_axes, None, tp, None))

    def shift(val, s):
        return lax.ppermute(val, tp, [(i, (i + s) % n_tp) for i in range(n_tp)])

    def local_layer(tokens, positions, valid_len, w_query, w_key, w_value, w_out, w_gate, w_up, w_down, norm_attn, norm_mlp):
        _, seq, d = tokens.shape
        x = tokens.reshape(seq, d)
        n_q = w_query.shape[1] // HEAD_DIM
        n_kv = w_key.shape[1] // HEAD_DIM
        sub = seq // (n_tp * N_CALLS)
        me = lax.axis_index(tp)

        w_qkv = lax.all_gather(jnp.concatenate([w_query, w_key, w_value], axis=1), 'fsdp', axis=0, tiled=True)
        rounds = []
        for s in range(1, n_tp):
            rounds.append(shift(w_out, s))
        full_o = lax.all_gather(jnp.concatenate([w_out, *rounds], axis=0), 'fsdp', axis=1, tiled=True)
        fl = w_gate.shape[1]
        n_src = 2
        swaps = []
        lead = fl * 5 // 8
        for cut in (slice(0, lead), slice(lead, fl)):
            local = jnp.concatenate([w_gate[:, cut], w_up[:, cut]], axis=1)
            swaps.append((local, shift(local, 2)))
        swaps.append((w_down, shift(w_down, 2)))

        def joined(p, axis, *deps):
            return jnp.concatenate([after(swaps[p][0], *deps), swaps[p][1]], axis=axis)

        angles = positions.reshape(seq, 1).astype(jnp.float32) * rope_freqs()[None, :]
        cos_h, sin_h = jnp.cos(angles), jnp.sin(angles)
        cos_t = jnp.concatenate([cos_h, cos_h], axis=1)
        sin_t = jnp.concatenate([-sin_h, sin_h], axis=1)
        h = norm_call(x, norm_attn.reshape(1, d))
        q, k, v, vt = qkv_call(h, w_qkv, cos_t, sin_t, n_q, n_kv)

        pieces = []
        gu_parts = []
        o = q
        for call in range(N_CALLS):
            gu_parts.append(joined(call, 1, o))
            o = att_call(after(q, gu_parts[call], o), k, vt, valid_len, call)
            got = []
            for s in range(n_tp):
                blk = lax.dynamic_slice_in_dim(o, (me + s) % n_tp * sub, sub, axis=0)
                if s:
                    blk = shift(blk, s)
                got.append(blk)
            pieces.append(got)
        d_part = joined(2, 0, o)
        gu_full = [lax.all_gather(w, 'fsdp', axis=0, tiled=True) for w in gu_parts]
        n_blk = w_down.shape[1] // HEAD_DIM
        d_pair = lax.ppermute(d_part, 'fsdp', [(i, i ^ 1) for i in range(n_fs)])
        d_near = jnp.concatenate([d_part, d_pair], axis=1)
        d_full = [lax.all_gather(d_part[:, b * HEAD_DIM:(b + 1) * HEAD_DIM], 'fsdp', axis=1, tiled=True) for b in range(n_blk)]

        resid, u_own, u_prev, u_next = [], [], [], []
        order = d_part
        for call in range(N_CALLS):
            got = pieces[call]
            got[0] = after(got[0], order)
            row = (call * n_tp + me).reshape(1).astype(jnp.int32)
            r, ua, ub = out_call(row, got, full_o, x, norm_mlp.reshape(1, d))
            order = r
            resid.append(r)
            u_own += [ua, ub]
            u_prev.append(shift(ua, 1))
            u_next.append(shift(ub, -1))
        u_recv = [u_prev[0], u_next[0], u_prev[1], u_next[1]]

        def gate_up(p, us, dep):
            return gu_call([after(us[0], dep)] + us[1:], gu_full[p], n_src)

        a_own = gate_up(0, u_own, resid[-1])
        a_recv = [gate_up(0, u_recv, a_own)]
        a_recv.append(gate_up(1, u_recv, a_recv[0]))
        a_late = []

        fs = lax.axis_index('fsdp')
        chip, n_chip = fs // 2, n_fs // 2
        others = [(chip + 1 + i) % n_chip for i in range(n_chip - 1)]
        bn = 2 * HEAD_DIM
        blocks = [(d_near, list(range(n_blk)), [fs * n_blk + i for i in range(n_blk)] + [(fs ^ 1) * n_blk + i for i in range(n_blk)])]
        for b in range(n_blk):
            units = sum(([2 * o_ * n_blk + b, (2 * o_ + 1) * n_blk + b] for o_ in others), [])
            blocks.append((d_full[b], others, units))
        idx = jnp.stack([jnp.asarray(v, jnp.int32) for v in [(me - s) % n_tp for s in range(n_tp)] + sum((u for _, _, u in blocks), [])])
        near_moves = [(i * N_CALLS + c, 0, sub, c, who) for i, who in enumerate((0, 1, n_tp - 1)) for c in range(N_CALLS)]
        far_moves = [(0, 0, sub, 0, 2), (1, 0, sub, N_CALLS - 1, 2)]
        skip = [sum(len(u) for _, _, u in blocks[:b]) for b in range(len(blocks))]
        last = len(blocks) - 1
        mine, far = [], []

        def place_near(b, out, *deps):
            m, near = mine[b]
            pieces = [*m, *(near[g, c] for g in range(2) for c in range(N_CALLS))]
            pieces[0] = after(pieces[0], *deps)
            return place_call(idx, pieces, near_moves, (seq, d), n_tp, skip[b], out)

        def place_far(b, out):
            return place_call(idx, far[b], far_moves, (seq, d), n_tp, skip[b], out)

        def relay(b, *deps):
            near = mine[b][1]
            far_0 = shift(after(near[0, 0], *deps), 1)
            far_1 = shift(after(near[1, N_CALLS - 1], *deps), -1)
            far.append((far_0, far_1))

        order = a_recv[1]
        hidden = None
        asked = []

        def ask(b, dep):
            w, sel, units = blocks[b]
            meta = jnp.stack([jnp.asarray(v, jnp.int32) for v in [*sel, *units]])
            p_prev, p_next = down_call([after(a_recv[0], dep), a_recv[1]], w, meta, n_src, bn, len(sel), N_CALLS * sub)
            b_next = shift(p_prev, -1)
            b_prev = shift(p_next, 1)
            asked.append((meta, b_next, b_prev))
            return p_prev

        for b, (w, sel, units) in enumerate(blocks):
            if b < last:
                order = ask(b, order)
            if b == last - 1:
                order = ask(last, order)
            meta, b_next, b_prev = asked[b]
            if b >= 1:
                relay(b - 1)
            if b >= 2:
                hidden = place_far(b - 2, place_near(b - 2, hidden, order))
                order = hidden
            m, near = [], {}
            for c in range(N_CALLS):
                if b == 0:
                    a_late.append(gate_up(1, u_own[2 * c:2 * c + 2], order))
                    order = a_late[c]
                m += down_call([after(a_own, order), a_late[c]], w, meta, n_src, bn, len(sel), sub, c, resid[c], (b_next, b_prev))
                order = m[c]
                for g, by in enumerate((1, -1)):
                    near[g, c] = shift(m[c], by)
            mine.append((m, near))
        hidden = place_far(last - 1, place_near(last - 1, hidden, order))
        relay(last, hidden)
        hidden = place_far(last, place_near(last, hidden))
        hidden = hidden.reshape(1, seq, d)
        return hidden, k.reshape(1, seq, n_kv, HEAD_DIM), v.reshape(1, seq, n_kv, HEAD_DIM)


    return jax.shard_map(local_layer, mesh=mesh2, in_specs=in_specs, out_specs=out_specs, check_vma=False)
```
